8 devices in a mesh: data: 8 (over z, y, x, core).
Axes of the slice: x: 2, y: 2, z: 1, core: 2. Of those that a mesh axis runs over, the one named last changes fastest.
Arguments:
- h_a: bfloat16 [4096, 512], P('data')
- h_b: bfloat16 [4096, 512], P('data')
- w_one: bfloat16 [512, 2048], replicated
- w_two: bfloat16 [2048, 2048], replicated
- w_three: bfloat16 [2048, 2048], replicated
- gain_one: float32 [2048], replicated
- shift_one: float32 [2048], replicated
- gain_two: float32 [2048], replicated
- shift_two: float32 [2048], replicated
- lam_off: float32 [], replicated
Outputs:
- output 1: float32 [], replicated
- output 2: float32 [512, 2048], P('data')
- output 3: float32 [2048, 2048], P('data')
- output 4: float32 [2048, 2048], P('data')
- output 5: float32 [2048], replicated
- output 6: float32 [2048], replicated
- output 7: float32 [2048], replicated
- output 8: float32 [2048], replicated
All inputs are finite; a program needn't handle non-finite values.
Results may differ from the reference program's by a relative error of at most 0.00520155.
Values are sent between devices in bfloat16 or wider.
A program may use at most 1 GiB of HBM per device.

```python
import jax
import jax.numpy as jnp
from jax import lax

FEAT_DIM = 512
PROJ_DIM = 2048
ROWS_DEV = 512
SHARDS = 8
TOTAL_ROWS = ROWS_DEV * SHARDS
NORM_EPS = 1e-5


def setup_inputs(seed: int = 0) -> dict:
    key_list = jax.random.split(jax.random.key(seed), 14)
    common = jax.random.normal(key_list[0], (TOTAL_ROWS, FEAT_DIM), jnp.float32)
    shard_shift = 0.6 * jax.random.normal(key_list[1], (SHARDS, 1, FEAT_DIM), jnp.float32)
    shard_scale = jnp.exp(0.3 * jax.random.normal(key_list[2], (SHARDS, 1, FEAT_DIM), jnp.float32))

    def make_view(view_key):
        noise_vals = jax.random.normal(view_key, (TOTAL_ROWS, FEAT_DIM), jnp.float32)
        mixed_rows = (0.77 * common + 0.64 * noise_vals).reshape(SHARDS, ROWS_DEV, FEAT_DIM)
        return (mixed_rows * shard_scale + shard_shift).reshape(TOTAL_ROWS, FEAT_DIM).astype(jnp.bfloat16)

    def make_weight(weight_key, fan_in, fan_out):
        weight_scale = fan_in ** -0.5
        return (jax.random.normal(weight_key, (fan_in, fan_out), jnp.float32) * weight_scale).astype(jnp.bfloat16)

    def make_vector(vec_key, center):
        return center + 0.25 * jax.random.normal(vec_key, (PROJ_DIM,), jnp.float32)

    lam_off = (0.1 + 0.2 * jax.random.uniform(key_list[12], (), jnp.float32)) * TOTAL_ROWS / PROJ_DIM
    return {
        "h_a": make_view(key_list[3]),
        "h_b": make_view(key_list[4]),
        "w_one": make_weight(key_list[5], FEAT_DIM, PROJ_DIM),
        "w_two": make_weight(key_list[6], PROJ_DIM, PROJ_DIM),
        "w_three": make_weight(key_list[7], PROJ_DIM, PROJ_DIM),
        "gain_one": make_vector(key_list[8], 1.0),
        "shift_one": make_vector(key_list[9], 0.0),
        "gain_two": make_vector(key_list[10], 1.0),
        "shift_two": make_vector(key_list[11], 0.0),
        "lam_off": lam_off,
    }


def batch_norm(values):
    col_mean = jnp.sum(values, axis=0) / TOTAL_ROWS
    col_var = jnp.sum(values * values, axis=0) / TOTAL_ROWS - col_mean * col_mean
    return (values - col_mean) * lax.rsqrt(col_var + NORM_EPS)


def project(feat_rows, params):
    w_one, w_two, w_three, gain_one, shift_one, gain_two, shift_two = params
    hidden_one = jnp.dot(feat_rows.astype(jnp.float32), w_one, preferred_element_type=jnp.float32)
    act_one = jax.nn.relu(gain_one * batch_norm(hidden_one) + shift_one).astype(jnp.bfloat16)
    hidden_two = jnp.dot(act_one.astype(jnp.float32), w_two, preferred_element_type=jnp.float32)
    act_two = jax.nn.relu(gain_two * batch_norm(hidden_two) + shift_two).astype(jnp.bfloat16)
    proj_out = jnp.dot(act_two.astype(jnp.float32), w_three, preferred_element_type=jnp.float32)
    return batch_norm(proj_out).astype(jnp.bfloat16)


def barlow_loss(params, h_a, h_b, lam_off):
    embed_a = project(h_a, params).astype(jnp.float32)
    embed_b = project(h_b, params).astype(jnp.float32)
    corr_mat = jnp.dot(embed_a.T, embed_b, preferred_element_type=jnp.float32) / TOTAL_ROWS
    feat_index = jnp.arange(PROJ_DIM)
    diag_mask = feat_index[:, None] == feat_index[None, :]
    diag_gap = 1.0 - jnp.diagonal(corr_mat)
    off_square = jnp.sum(jnp.where(diag_mask, 0.0, corr_mat * corr_mat))
    return jnp.sum(diag_gap * diag_gap) + lam_off * off_square


def reference(h_a, h_b, w_one, w_two, w_three, gain_one, shift_one, gain_two, shift_two, lam_off):
    params = (w_one.astype(jnp.float32), w_two.astype(jnp.float32), w_three.astype(jnp.float32),
              gain_one, shift_one, gain_two, shift_two)
    loss_total, grad_list = jax.value_and_grad(barlow_loss)(params, h_a, h_b, lam_off)
    return (loss_total, grad_list[0], grad_list[1], grad_list[2],
            grad_list[3], grad_list[4], grad_list[5], grad_list[6])
```

```python
import functools

import jax
import jax.numpy as jnp
from jax import lax
from jax.experimental import pallas as pl
from jax.experimental.pallas import tpu as pltpu
from jax.sharding import PartitionSpec as P

NORM_EPS = 1e-5
MESH = pl.DeviceIdType.MESH


def exchange_kernel(src, dst, slots, send_sem, recv_sem):
    me = lax.axis_index("data")
    barrier = pltpu.get_barrier_semaphore()
    for mask in range(1, 8):
        pl.semaphore_signal(barrier, inc=1, device_id=(me ^ mask,), device_id_type=MESH)
    pl.semaphore_wait(barrier, 7)
    copies = []
    for mask in (6, 2, 4, 7, 3, 5, 1):
        copy = pltpu.make_async_remote_copy(
            src_ref=src, dst_ref=slots.at[me], send_sem=send_sem.at[mask], recv_sem=recv_sem.at[mask],
            device_id=(me ^ mask,), device_id_type=MESH)
        copy.start()
        copies.append(copy)
    slots[me] = src[...]
    for copy in copies:
        copy.wait()
    total = slots[0]
    for k in range(1, 8):
        total = total + slots[k]
    dst[...] = total


def sum_devices(values, cid):
    return pl.pallas_call(
        exchange_kernel,
        out_shape=jax.ShapeDtypeStruct(values.shape, jnp.float32),
        in_specs=[pl.BlockSpec(memory_space=pltpu.VMEM)],
        out_specs=pl.BlockSpec(memory_space=pltpu.VMEM),
        scratch_shapes=[pltpu.VMEM((8,) + values.shape, jnp.float32),
                        pltpu.SemaphoreType.DMA((8,)), pltpu.SemaphoreType.DMA((8,))],
        compiler_params=pltpu.CompilerParams(collective_id=cid, has_side_effects=True),
        name="sum_devices_%d" % cid,
    )(values)


def swap(value, mask):
    return lax.ppermute(value, "data", [(k, k ^ mask) for k in range(8)])


def pair_columns(rows, me, width):
    return [lax.dynamic_slice_in_dim(rows, (me ^ m) * width, width, axis=1) for m in (0, 2, 4, 6)]


def give_columns(rows, me, width):
    mine = jnp.concatenate([lax.dynamic_slice_in_dim(rows, (me ^ m) * width, width, axis=1)
                            for m in (1, 3, 5, 7)], axis=1)
    got = swap(mine, 1)
    return [got[:, j * width:(j + 1) * width] for j in range(4)]


def tdot(lhs, rhs):
    return lax.dot_general(lhs, rhs, (((0,), (0,)), ((), ())), preferred_element_type=jnp.float32)


def scatter_product(own_cols, partner_cols, own_rows, partner_rows):
    half = own_rows.shape[1] // 2

    def part(j, lo):
        return (tdot(own_cols[j], own_rows[:, lo:lo + half])
                + tdot(partner_cols[j], partner_rows[:, lo:lo + half]))

    x_first = [part(j, 0) for j in (1, 3, 0, 2)]
    y_first = [part(j, half) for j in (2, 3, 0, 1)]
    got_a = [swap(x_first[0], 2), swap(x_first[1], 2)]
    got_b = [swap(y_first[0], 4), swap(y_first[1], 4)]
    relay_a = swap(x_first[3] + got_a[1], 4)
    relay_b = swap(y_first[3] + got_b[1], 2)
    return jnp.concatenate([x_first[2] + got_a[0] + relay_a, y_first[2] + got_b[0] + relay_b], axis=1)


def gather_blocks(block, me):
    rows = block.shape[0]
    from_x, from_y = swap(block, 2), swap(block, 4)
    top = swap(from_x[:rows // 2], 4)
    bottom = swap(from_y[rows // 2:], 2)
    diag = jnp.concatenate([top, bottom], axis=0)
    mine = [block, from_x, from_y, diag]
    whole = jnp.zeros((8 * rows, block.shape[1]), block.dtype)
    for m, piece in zip((0, 2, 4, 6), mine):
        other = swap(piece, 1)
        whole = lax.dynamic_update_slice_in_dim(whole, piece, (me ^ m) * rows, axis=0)
        whole = lax.dynamic_update_slice_in_dim(whole, other, (me ^ m ^ 1) * rows, axis=0)
    return whole


def norm_forward(values, total_rows, cid):
    feats = values.shape[-1]
    col_sums = jnp.stack([jnp.sum(values, axis=1), jnp.sum(values * values, axis=1)])
    col_sums = sum_devices(col_sums.reshape(4, feats), cid).reshape(2, 2, feats)
    col_mean = col_sums[0] / total_rows
    inv_std = lax.rsqrt(col_sums[1] / total_rows - col_mean * col_mean + NORM_EPS)
    return (values - col_mean[:, None, :]) * inv_std[:, None, :], inv_std


def norm_backward(grad_out, normed, inv_std, total_rows, cid):
    feats = grad_out.shape[-1]
    col_sums = jnp.stack([jnp.sum(grad_out, axis=1), jnp.sum(grad_out * normed, axis=1)])
    col_sums = sum_devices(col_sums.reshape(4, feats), cid).reshape(2, 2, feats)
    grad_in = inv_std[:, None, :] * (grad_out - (col_sums[0][:, None, :] + normed * col_sums[1][:, None, :]) / total_rows)
    return grad_in, col_sums


def solution(mesh):
    shards = mesh.shape["data"]

    def local_step(h_a, h_b, w_one, w_two, w_three, gain_one, shift_one, gain_two, shift_two, lam_off):
        me = lax.axis_index("data")
        rows_dev = h_a.shape[0]
        feats = w_two.shape[0]
        total_rows = rows_dev * shards
        feat_rows = jnp.concatenate([h_a, h_b], axis=0)
        hidden_one = jnp.dot(feat_rows, w_one, preferred_element_type=jnp.float32).reshape(2, rows_dev, -1)
        normed_one, inv_one = norm_forward(hidden_one, total_rows, 0)
        pre_one = gain_one * normed_one + shift_one
        act_one = jax.nn.relu(pre_one).astype(jnp.bfloat16)
        hidden_two = jnp.dot(act_one, w_two, preferred_element_type=jnp.float32)
        normed_two, inv_two = norm_forward(hidden_two, total_rows, 1)
        pre_two = gain_two * normed_two + shift_two
        act_two = jax.nn.relu(pre_two).astype(jnp.bfloat16)
        proj_out = jnp.dot(act_two, w_three, preferred_element_type=jnp.float32)
        normed_out, inv_out = norm_forward(proj_out, total_rows, 2)
        embed_pair = normed_out.astype(jnp.bfloat16)
        blk = feats // shards
        act_one_rows = act_one.reshape(2 * rows_dev, feats)
        act_two_rows = act_two.reshape(2 * rows_dev, feats)
        pair_one, pair_two = give_columns(act_one_rows, me, blk), give_columns(act_two_rows, me, blk)
        pair_h = give_columns(feat_rows, me, feat_rows.shape[1] // shards)

        corr_block = scatter_product(pair_columns(embed_pair[0], me, blk), give_columns(embed_pair[0], me, blk),
                                     embed_pair[1], swap(embed_pair[1], 1)) / total_rows
        row_index = me * blk + jnp.arange(blk)
        diag_mask = row_index[:, None] == jnp.arange(feats)[None, :]
        diag_gap = 1.0 - corr_block
        loss_part = jnp.sum(jnp.where(diag_mask, diag_gap * diag_gap, lam_off * corr_block * corr_block))
        grad_corr = jnp.where(diag_mask, -2.0 * diag_gap, 2.0 * lam_off * corr_block)
        grad_scaled = gather_blocks((grad_corr / total_rows).astype(jnp.bfloat16), me)
        loss_total = sum_devices(jnp.full((8, 128), loss_part, jnp.float32), 6)[0, 0]

        grad_embed_a = lax.dot_general(embed_pair[1], grad_scaled, (((1,), (1,)), ((), ())),
                                       preferred_element_type=jnp.float32)
        grad_embed_b = jnp.dot(embed_pair[0], grad_scaled, preferred_element_type=jnp.float32)
        grad_embed = jnp.stack([grad_embed_a, grad_embed_b])
        grad_proj = norm_backward(grad_embed, normed_out, inv_out, total_rows, 3)[0].astype(jnp.bfloat16)

        def weight_grad(rows, pair, grads):
            grad_rows = grads.reshape(2 * rows_dev, feats)
            return scatter_product(pair_columns(rows, me, rows.shape[1] // shards), pair, grad_rows, swap(grad_rows, 1))

        grad_w_three = weight_grad(act_two_rows, pair_two, grad_proj)
        last_dims = (((2,), (1,)), ((), ()))
        grad_act_two = lax.dot_general(grad_proj, w_three, last_dims, preferred_element_type=jnp.float32)
        grad_pre_two = jnp.where(pre_two > 0, grad_act_two, 0.0)
        grad_hidden_two, sums_two = norm_backward(grad_pre_two, normed_two, inv_two, total_rows, 4)
        grad_hidden_two = (gain_two * grad_hidden_two).astype(jnp.bfloat16)
        grad_w_two = weight_grad(act_one_rows, pair_one, grad_hidden_two)
        grad_act_one = lax.dot_general(grad_hidden_two, w_two, last_dims, preferred_element_type=jnp.float32)
        grad_pre_one = jnp.where(pre_one > 0, grad_act_one, 0.0)
        grad_hidden_one, sums_one = norm_backward(grad_pre_one, normed_one, inv_one, total_rows, 5)
        grad_hidden_one = (gain_one * grad_hidden_one).astype(jnp.bfloat16)
        grad_w_one = weight_grad(feat_rows, pair_h, grad_hidden_one)
        return (loss_total, grad_w_one, grad_w_two, grad_w_three,
                jnp.sum(sums_one[1], axis=0), jnp.sum(sums_one[0], axis=0),
                jnp.sum(sums_two[1], axis=0), jnp.sum(sums_two[0], axis=0))

    row_spec = P("data", None)
    whole_mat = P(None, None)
    whole_vec = P(None)
    return jax.shard_map(
        local_step, mesh=mesh,
        in_specs=(row_spec, row_spec, whole_mat, whole_mat, whole_mat,
                  whole_vec, whole_vec, whole_vec, whole_vec, P()),
        out_specs=(P(), row_spec, row_spec, row_spec, whole_vec, whole_vec, whole_vec, whole_vec),
        check_vma=False)
```

```python
import functools

import jax
import jax.numpy as jnp
from jax import lax
from jax.experimental import pallas as pl
from jax.experimental.pallas import tpu as pltpu
from jax.sharding import PartitionSpec as P

NORM_EPS = 1e-5
MESH = pl.DeviceIdType.MESH


def exchange_kernel(src, dst, slots, send_sem, recv_sem):
    me = lax.axis_index("data")
    barrier = pltpu.get_barrier_semaphore()
    for mask in range(1, 8):
        pl.semaphore_signal(barrier, inc=1, device_id=(me ^ mask,), device_id_type=MESH)
    pl.semaphore_wait(barrier, 7)
    copies = []
    for mask in (6, 2, 4, 7, 3, 5, 1):
        copy = pltpu.make_async_remote_copy(
            src_ref=src, dst_ref=slots.at[me], send_sem=send_sem.at[mask], recv_sem=recv_sem.at[mask],
            device_id=(me ^ mask,), device_id_type=MESH)
        copy.start()
        copies.append(copy)
    slots[me] = src[...]
    for copy in copies:
        copy.wait()
    total = slots[0]
    for k in range(1, 8):
        total = total + slots[k]
    dst[...] = total


def sum_devices(values, cid):
    return pl.pallas_call(
        exchange_kernel,
        out_shape=jax.ShapeDtypeStruct(values.shape, jnp.float32),
        in_specs=[pl.BlockSpec(memory_space=pltpu.VMEM)],
        out_specs=pl.BlockSpec(memory_space=pltpu.VMEM),
        scratch_shapes=[pltpu.VMEM((8,) + values.shape, jnp.float32),
                        pltpu.SemaphoreType.DMA((8,)), pltpu.SemaphoreType.DMA((8,))],
        compiler_params=pltpu.CompilerParams(collective_id=cid, has_side_effects=True),
        name="sum_devices_%d" % cid,
    )(values)


def swap(value, mask):
    return lax.ppermute(value, "data", [(k, k ^ mask) for k in range(8)])


def pair_columns(rows, me, width):
    return [lax.dynamic_slice_in_dim(rows, (me ^ m) * width, width, axis=1) for m in (0, 2, 4, 6)]


def give_columns(rows, me, width):
    mine = jnp.concatenate([lax.dynamic_slice_in_dim(rows, (me ^ m) * width, width, axis=1)
                            for m in (1, 3, 5, 7)], axis=1)
    got = swap(mine, 1)
    return [got[:, j * width:(j + 1) * width] for j in range(4)]


def tdot(lhs, rhs):
    return lax.dot_general(lhs, rhs, (((0,), (0,)), ((), ())), preferred_element_type=jnp.float32)


def scatter_product(own_cols, partner_cols, own_rows, partner_rows):
    half = own_rows.shape[1] // 2

    def part(j, lo):
        return (tdot(own_cols[j], own_rows[:, lo:lo + half])
                + tdot(partner_cols[j], partner_rows[:, lo:lo + half]))

    x_first = [part(j, 0) for j in (1, 3, 0, 2)]
    y_first = [part(j, half) for j in (2, 3, 0, 1)]
    got_a = [swap(x_first[0], 2), swap(x_first[1], 2)]
    got_b = [swap(y_first[0], 4), swap(y_first[1], 4)]
    relay_a = swap(x_first[3] + got_a[1], 4)
    relay_b = swap(y_first[3] + got_b[1], 2)
    return jnp.concatenate([x_first[2] + got_a[0] + relay_a, y_first[2] + got_b[0] + relay_b], axis=1)


def gather_blocks(block, me):
    rows = block.shape[0]
    from_x, from_y = swap(block, 2), swap(block, 4)
    top = swap(from_x[:rows // 2], 4)
    bottom = swap(from_y[rows // 2:], 2)
    diag = jnp.concatenate([top, bottom], axis=0)
    mine = [block, from_x, from_y, diag]
    whole = jnp.zeros((8 * rows, block.shape[1]), block.dtype)
    for m, piece in zip((0, 2, 4, 6), mine):
        other = swap(piece, 1)
        whole = lax.dynamic_update_slice_in_dim(whole, piece, (me ^ m) * rows, axis=0)
        whole = lax.dynamic_update_slice_in_dim(whole, other, (me ^ m ^ 1) * rows, axis=0)
    return whole


TILE = 256
TILES = 8


def backward_kernel(rows_total, dz, x2_own, x2_pair, x1_own, x1_pair, h_own, h_pair, w3, w2, n2, n1, vec2, vec1,
                    gw3, gw2, gw1, sums2, sums1,
                    d, pd, xt, ht, dpre, wbuf, nbuf, acc3, acc2, acc1, near3, near2, near1, far3, far2, far1,
                    mine, slots, load_sem, pair_send, pair_recv, hop_send, hop_recv, far_send, far_recv,
                    sum_send, sum_recv, out_sem, w_sem, n_sem, free_sem):
    me = lax.axis_index("data")
    half = d.shape[0] // 2
    barrier = pltpu.get_barrier_semaphore()
    for mask in range(1, 8):
        pl.semaphore_signal(barrier, inc=1, device_id=(me ^ mask,), device_id_type=MESH)
    pl.semaphore_wait(barrier, 7)

    def cols(n):
        return pl.ds(pl.multiple_of(n * TILE, TILE), TILE)

    def remote(src, dst, send, recv, mask):
        return pltpu.make_async_remote_copy(src_ref=src, dst_ref=dst, send_sem=send, recv_sem=recv,
                                            device_id=(me ^ mask,), device_id_type=MESH)

    def pair_copy(src, n):
        return remote(src.at[:, cols(n)], pd.at[:, cols(n)], pair_send.at[n], pair_recv.at[n], 1)

    def first_hop(w, acc, near, blk, n, colour):
        start, mask = ((blk, 2), (2 * blk, 4))[colour]
        return remote(acc.at[n, pl.ds(start, 2 * blk)], near.at[n], hop_send.at[w, n], hop_recv.at[w, n], mask)

    def second_hop(w, acc, far, blk, n, colour):
        start, mask = ((3 * blk, 4), (blk, 2))[colour]
        return remote(acc.at[n, pl.ds(start, blk)], far.at[n], far_send.at[w, n], far_recv.at[w, n], mask)

    def load(src, dst, k):
        return pltpu.make_async_copy(src, dst, load_sem.at[k])

    def products(w, lhs, acc, near, blk, src):
        def body(i, carry):
            for colour in (0, 1):
                n = colour * 4 + i
                pair_copy(src, n).wait()
                acc[n] = (jnp.dot(lhs[:, :2 * half], d[:, cols(n)], preferred_element_type=jnp.float32)
                          + jnp.dot(lhs[:, 2 * half:], pd[:, cols(n)], preferred_element_type=jnp.float32))
                first_hop(w, acc, near, blk, n, colour).start()
            return carry
        lax.fori_loop(0, 4, body, 0)

    def relay(w, acc, near, far, blk):
        def body(i, carry):
            for colour in (0, 1):
                n = colour * 4 + i
                own, other = (pl.ds(0, blk), pl.ds(blk, blk)) if colour == 0 else (pl.ds(blk, blk), pl.ds(0, blk))
                dest = pl.ds(3 * blk, blk) if colour == 0 else pl.ds(blk, blk)
                first_hop(w, acc, near, blk, n, colour).wait_recv()
                acc[n, dest] = acc[n, dest] + near[n, other]
                second_hop(w, acc, far, blk, n, colour).start()
                acc[n, pl.ds(0, blk)] = acc[n, pl.ds(0, blk)] + near[n, own]
            return carry
        lax.fori_loop(0, 4, body, 0)

    def out_copy(w, acc, out, blk, n):
        return pltpu.make_async_copy(acc.at[n, pl.ds(0, blk)], out.at[:, cols(n)], out_sem.at[w, n])

    def finish(w, acc, near, far, out, blk):
        def body(i, carry):
            for colour in (0, 1):
                n = colour * 4 + i
                second_hop(w, acc, far, blk, n, colour).wait_recv()
                acc[n, pl.ds(0, blk)] = acc[n, pl.ds(0, blk)] + far[n]
                out_copy(w, acc, out, blk, n).start()
            return carry
        lax.fori_loop(0, 4, body, 0)

    def drain(w, acc, near, far, out, blk):
        def body(i, carry):
            for colour in (0, 1):
                n = colour * 4 + i
                first_hop(w, acc, near, blk, n, colour).wait_send()
                second_hop(w, acc, far, blk, n, colour).wait_send()
                out_copy(w, acc, out, blk, n).wait()
            return carry
        lax.fori_loop(0, 4, body, 0)

    def w_tile(src, i):
        return pltpu.make_async_copy(src.at[pl.ds(pl.multiple_of(i * TILE, TILE), TILE)], wbuf.at[i % 2],
                                     w_sem.at[i % 2])

    def n_tile(src, i):
        return pltpu.make_async_copy(src.at[:, cols(i)], nbuf.at[i % 2], n_sem.at[i % 2])

    def back_product(w_src, n_src, vec, which):
        w_tile(w_src, 0).start()
        n_tile(n_src, 0).start()

        def body(i, carry):
            slot = i % 2

            @pl.when(i < TILES - 1)
            def _():
                w_tile(w_src, i + 1).start()
                n_tile(n_src, i + 1).start()
            w_tile(w_src, i).wait()
            n_tile(n_src, i).wait()
            gain, shift = vec[0:1, cols(i)], vec[1:2, cols(i)]
            for v in (0, 1):
                rows = pl.ds(v * half, half)
                grad = lax.dot_general(d[rows, :], wbuf[slot], (((1,), (1,)), ((), ())),
                                       preferred_element_type=jnp.float32)
                normed = nbuf[slot, rows, :]
                grad = jnp.where(gain * normed + shift > 0, grad, 0.0)
                dpre[rows, cols(i)] = grad
                mine[which, v:v + 1, cols(i)] = jnp.sum(grad, axis=0, keepdims=True)
                mine[which, 2 + v:3 + v, cols(i)] = jnp.sum(grad * normed, axis=0, keepdims=True)
            return carry
        lax.fori_loop(0, TILES, body, 0)

    def sum_copy(which, mask):
        return remote(mine.at[which], slots.at[which, me], sum_send.at[which, mask], sum_recv.at[which, mask], mask)

    def send_sums(which):
        for mask in (6, 7, 2, 3, 4, 5, 1):
            sum_copy(which, mask).start()
        slots[which, me] = mine[which]

    def take_sums(which, out):
        for mask in range(1, 8):
            sum_copy(which, mask).wait()
        total = slots[which, 0]
        for k in range(1, 8):
            total = total + slots[which, k]
        out[...] = total

    def norm_grad(n_src, vec, sums):
        n_tile(n_src, 0).start()

        def body(i, carry):
            slot = i % 2

            @pl.when(i < TILES - 1)
            def _():
                n_tile(n_src, i + 1).start()
            n_tile(n_src, i).wait()
            for v in (0, 1):
                rows = pl.ds(v * half, half)
                scale = vec[0:1, cols(i)] * vec[2 + v:3 + v, cols(i)]
                mean = sums[v:v + 1, cols(i)] / rows_total
                slope = sums[2 + v:3 + v, cols(i)] / rows_total
                grad = scale * (dpre[rows, cols(i)] - (mean + nbuf[slot, rows, :] * slope))
                d[rows, cols(i)] = grad.astype(jnp.bfloat16)
            pair_copy(d, i).start()
            return carry
        lax.fori_loop(0, TILES, body, 0)

    for i in (0, 4, 1, 5, 2, 6, 3, 7):
        pair_copy(dz, i).start()
    first = [load(dz, d, 0), load(x2_own, xt.at[:, pl.ds(0, 2 * half)], 1),
             load(x2_pair, xt.at[:, pl.ds(2 * half, 2 * half)], 2),
             load(h_own, ht.at[:, pl.ds(0, 2 * half)], 3), load(h_pair, ht.at[:, pl.ds(2 * half, 2 * half)], 4)]
    for copy in first:
        copy.start()
    for copy in first:
        copy.wait()
    blk3, blk1 = gw3.shape[0], gw1.shape[0]
    products(0, xt, acc3, near3, blk3, dz)
    second = [load(x1_own, xt.at[:, pl.ds(0, 2 * half)], 1), load(x1_pair, xt.at[:, pl.ds(2 * half, 2 * half)], 2)]
    for copy in second:
        copy.start()
    back_product(w3, n2, vec2, 0)
    send_sums(0)
    relay(0, acc3, near3, far3, blk3)
    take_sums(0, sums2)
    norm_grad(n2, vec2, sums2)
    back_product(w2, n1, vec1, 1)
    send_sums(1)
    for copy in second:
        copy.wait()
    products(1, xt, acc2, near2, blk3, d)
    pl.semaphore_signal(free_sem, inc=1, device_id=(me ^ 1,), device_id_type=MESH)
    take_sums(1, sums1)
    pl.semaphore_wait(free_sem, 1)
    norm_grad(n1, vec1, sums1)
    products(2, ht, acc1, near1, blk1, d)
    finish(0, acc3, near3, far3, gw3, blk3)
    relay(1, acc2, near2, far2, blk3)
    relay(2, acc1, near1, far1, blk1)
    finish(1, acc2, near2, far2, gw2, blk3)
    finish(2, acc1, near1, far1, gw1, blk1)
    drain(0, acc3, near3, far3, gw3, blk3)
    drain(1, acc2, near2, far2, gw2, blk3)
    drain(2, acc1, near1, far1, gw1, blk1)


def backward(rows_total, dz, x2, x1, h, w3, w2, n2, n1, vec2, vec1, cid):
    rows, feats = dz.shape
    blk3, blk1 = x2[0].shape[0] // 4, h[0].shape[0] // 4
    anyspace, vmem = pl.BlockSpec(memory_space=pl.ANY), pl.BlockSpec(memory_space=pltpu.VMEM)
    f32, bf16 = jnp.float32, jnp.bfloat16
    dma = pltpu.SemaphoreType.DMA

    def per_weight(parts):
        return [pltpu.VMEM((TILES, parts * b, TILE), f32) for b in (blk3, blk3, blk1)]

    return pl.pallas_call(
        functools.partial(backward_kernel, rows_total),
        out_shape=[jax.ShapeDtypeStruct((blk3, feats), f32), jax.ShapeDtypeStruct((blk3, feats), f32),
                   jax.ShapeDtypeStruct((blk1, feats), f32),
                   jax.ShapeDtypeStruct((4, feats), f32), jax.ShapeDtypeStruct((4, feats), f32)],
        in_specs=[anyspace] * 11 + [vmem] * 2,
        out_specs=[anyspace] * 3 + [vmem] * 2,
        scratch_shapes=[pltpu.VMEM((rows, feats), bf16), pltpu.VMEM((rows, feats), bf16),
                        pltpu.VMEM((4 * blk3, 2 * rows), bf16), pltpu.VMEM((4 * blk1, 2 * rows), bf16),
                        pltpu.VMEM((rows, feats), f32),
                        pltpu.VMEM((2, TILE, feats), bf16), pltpu.VMEM((2, rows, TILE), f32)]
        + per_weight(4) + per_weight(2) + per_weight(1)
        + [pltpu.VMEM((2, 4, feats), f32), pltpu.VMEM((2, 8, 4, feats), f32),
           dma((5,)), dma((TILES,)), dma((TILES,)), dma((3, TILES)), dma((3, TILES)), dma((3, TILES)), dma((3, TILES)),
           dma((2, 8)), dma((2, 8)), dma((3, TILES)), dma((2,)), dma((2,)), pltpu.SemaphoreType.REGULAR],
        compiler_params=pltpu.CompilerParams(collective_id=cid, has_side_effects=True, vmem_limit_bytes=67043328),
        name="backward",
    )(dz, *x2, *x1, *h, w3, w2, n2, n1, vec2, vec1)


def norm_forward(values, total_rows, cid):
    feats = values.shape[-1]
    col_sums = jnp.stack([jnp.sum(values, axis=1), jnp.sum(values * values, axis=1)])
    col_sums = sum_devices(col_sums.reshape(4, feats), cid).reshape(2, 2, feats)
    col_mean = col_sums[0] / total_rows
    inv_std = lax.rsqrt(col_sums[1] / total_rows - col_mean * col_mean + NORM_EPS)
    return (values - col_mean[:, None, :]) * inv_std[:, None, :], inv_std


def norm_backward(grad_out, normed, inv_std, total_rows, cid):
    feats = grad_out.shape[-1]
    col_sums = jnp.stack([jnp.sum(grad_out, axis=1), jnp.sum(grad_out * normed, axis=1)])
    col_sums = sum_devices(col_sums.reshape(4, feats), cid).reshape(2, 2, feats)
    grad_in = inv_std[:, None, :] * (grad_out - (col_sums[0][:, None, :] + normed * col_sums[1][:, None, :]) / total_rows)
    return grad_in, col_sums


def solution(mesh):
    shards = mesh.shape["data"]

    def local_step(h_a, h_b, w_one, w_two, w_three, gain_one, shift_one, gain_two, shift_two, lam_off):
        me = lax.axis_index("data")
        rows_dev = h_a.shape[0]
        feats = w_two.shape[0]
        total_rows = rows_dev * shards
        feat_rows = jnp.concatenate([h_a, h_b], axis=0)
        hidden_one = jnp.dot(feat_rows, w_one, preferred_element_type=jnp.float32).reshape(2, rows_dev, -1)
        normed_one, inv_one = norm_forward(hidden_one, total_rows, 0)
        pre_one = gain_one * normed_one + shift_one
        act_one = jax.nn.relu(pre_one).astype(jnp.bfloat16)
        hidden_two = jnp.dot(act_one, w_two, preferred_element_type=jnp.float32)
        normed_two, inv_two = norm_forward(hidden_two, total_rows, 1)
        pre_two = gain_two * normed_two + shift_two
        act_two = jax.nn.relu(pre_two).astype(jnp.bfloat16)
        proj_out = jnp.dot(act_two, w_three, preferred_element_type=jnp.float32)
        normed_out, inv_out = norm_forward(proj_out, total_rows, 2)
        embed_pair = normed_out.astype(jnp.bfloat16)
        blk = feats // shards
        act_one_rows = act_one.reshape(2 * rows_dev, feats)
        act_two_rows = act_two.reshape(2 * rows_dev, feats)

        corr_block = scatter_product(pair_columns(embed_pair[0], me, blk), give_columns(embed_pair[0], me, blk),
                                     embed_pair[1], swap(embed_pair[1], 1)) / total_rows
        row_index = me * blk + jnp.arange(blk)
        diag_mask = row_index[:, None] == jnp.arange(feats)[None, :]
        diag_gap = 1.0 - corr_block
        loss_part = jnp.sum(jnp.where(diag_mask, diag_gap * diag_gap, lam_off * corr_block * corr_block))
        grad_corr = jnp.where(diag_mask, -2.0 * diag_gap, 2.0 * lam_off * corr_block)
        grad_scaled = gather_blocks((grad_corr / total_rows).astype(jnp.bfloat16), me)
        loss_total = sum_devices(jnp.full((8, 128), loss_part, jnp.float32), 6)[0, 0]

        grad_embed_a = lax.dot_general(embed_pair[1], grad_scaled, (((1,), (1,)), ((), ())),
                                       preferred_element_type=jnp.float32)
        grad_embed_b = jnp.dot(embed_pair[0], grad_scaled, preferred_element_type=jnp.float32)
        grad_embed = jnp.stack([grad_embed_a, grad_embed_b])
        grad_proj = norm_backward(grad_embed, normed_out, inv_out, total_rows, 3)[0].astype(jnp.bfloat16)

        def operand(rows):
            turned = rows.T
            width = turned.shape[0] // shards
            pick = lambda masks: jnp.concatenate(
                [lax.dynamic_slice_in_dim(turned, (me ^ m) * width, width, axis=0) for m in masks], axis=0)
            return pick((0, 2, 6, 4)), swap(pick((1, 3, 7, 5)), 1)

        def vectors(gain, shift, inv_std):
            return jnp.concatenate([gain[None], shift[None], inv_std, jnp.zeros((4, feats), jnp.float32)], axis=0)

        grad_w_three, grad_w_two, grad_w_one, sums_two, sums_one = backward(
            total_rows, grad_proj.reshape(2 * rows_dev, feats), operand(act_two_rows), operand(act_one_rows),
            operand(feat_rows), w_three, w_two, normed_two.reshape(2 * rows_dev, feats),
            normed_one.reshape(2 * rows_dev, feats), vectors(gain_two, shift_two, inv_two),
            vectors(gain_one, shift_one, inv_one), 4)
        return (loss_total, grad_w_one, grad_w_two, grad_w_three,
                sums_one[2] + sums_one[3], sums_one[0] + sums_one[1],
                sums_two[2] + sums_two[3], sums_two[0] + sums_two[1])

    row_spec = P("data", None)
    whole_mat = P(None, None)
    whole_vec = P(None)
    return jax.shard_map(
        local_step, mesh=mesh,
        in_specs=(row_spec, row_spec, whole_mat, whole_mat, whole_mat,
                  whole_vec, whole_vec, whole_vec, whole_vec, P()),
        out_specs=(P(), row_spec, row_spec, row_spec, whole_vec, whole_vec, whole_vec, whole_vec),
        check_vma=False)
```

```python
import functools

import jax
import jax.numpy as jnp
from jax import lax
from jax.experimental import pallas as pl
from jax.experimental.pallas import tpu as pltpu
from jax.sharding import PartitionSpec as P

NORM_EPS = 1e-5
MESH = pl.DeviceIdType.MESH
DEVICES = 8
OWN, PAIR, XN, XP, YN, YP, DG, DP = range(DEVICES)
FAR_FIRST = (DG, DP, XN, XP, YN, YP, PAIR)
ORDER = (OWN, XN, DG, YN)
TWO = range(2)
TILE = 256
TILES = 8
WEIGHTS = 3
GAIN, SHIFT, INV, MEAN, VEC_ROWS = 0, 1, 2, 4, 6
VMEM_BYTES = 67043328
TURN_LEFT = (((0,), (0,)), ((), ()))
TURN_RIGHT = (((1,), (1,)), ((), ()))
F32, BF16 = jnp.float32, jnp.bfloat16
DMA = pltpu.SemaphoreType.DMA


def dot(left, right, dims=None):
    if dims is None:
        return jnp.dot(left, right, preferred_element_type=F32)
    return lax.dot_general(left, right, dims, preferred_element_type=F32)


def span(index, size):
    return pl.ds(pl.multiple_of(index * size, size), size)


def cols(n):
    return span(n, TILE)


def row(ref, r, c):
    return ref[r:r + 1, c]


def remote(src, dst, send, recv, mask):
    return pltpu.make_async_remote_copy(src_ref=src, dst_ref=dst, send_sem=send, recv_sem=recv,
                                        device_id=(lax.axis_index("data") ^ mask,), device_id_type=MESH)


def greet():
    for mask in FAR_FIRST:
        pl.semaphore_signal(pltpu.get_barrier_semaphore(), inc=1, device_id=(lax.axis_index("data") ^ mask,),
                            device_id_type=MESH)


def all_entered():
    pl.semaphore_wait(pltpu.get_barrier_semaphore(), len(FAR_FIRST))


def column_sums(ref, lead, r, c, first, second):
    ref[lead + (slice(r, r + 1), c)] = jnp.sum(first, axis=0, keepdims=True)
    ref[lead + (slice(r + 1, r + 2), c)] = jnp.sum(second, axis=0, keepdims=True)


def exchange(mine, slots, send, recv):
    me = lax.axis_index("data")

    def copy(e, mask):
        return remote(mine.at[e], slots.at[e, me], send.at[e, mask], recv.at[e, mask], mask)

    def start(e):
        for mask in FAR_FIRST:
            copy(e, mask).start()
        slots[e, me] = mine[e]

    def take(e):
        for mask in FAR_FIRST:
            copy(e, mask).wait()
        return functools.reduce(jnp.add, [slots[e, k] for k in range(DEVICES)])
    return start, take


def run(copies):
    for copy in copies:
        copy.start()
    return copies


def finish_all(copies):
    for copy in copies:
        copy.wait()


def backward_kernel(rows_total, dz, x2, x2_pair, x1, x1_pair, h_a, h_b, w3, w2, u2, u1, vec2, vec1,
                    gw3, gw2, gw1, sums2, sums1,
                    d, pd, xt, hv, hturn, ht, dpre, wbuf, nbuf, acc3, acc2, acc1, near3, near2, near1, far3, far2, far1,
                    mine, slots, load_sem, pair_send, pair_recv, hop_send, hop_recv, far_send, far_recv,
                    sum_send, sum_recv, h_send, h_recv, out_sem, w_sem, n_sem, free_sem):
    me = lax.axis_index("data")
    rows = d.shape[0]
    half = rows // 2
    greet()
    all_entered()
    send_sums, take_sums = exchange(mine, slots, sum_send, sum_recv)

    def pair_copy(src, n):
        return remote(src.at[:, cols(n)], pd.at[:, cols(n)], pair_send.at[n], pair_recv.at[n], PAIR)

    def both_colours(body):
        def step(i, carry):
            for colour in TWO:
                body(colour * (TILES // 2) + i, colour)
            return carry
        lax.fori_loop(0, TILES // 2, step, 0)

    class Product:
        def __init__(self, w, lhs, acc, near, far, out):
            self.w, self.lhs, self.acc, self.near, self.far, self.out = w, lhs, acc, near, far, out
            self.blk = out.shape[0]

        def block(self, j, count=1):
            return pl.ds(j * self.blk, count * self.blk)

        def first_hop(self, n, colour):
            return remote(self.acc.at[n, self.block(1 + colour, 2)], self.near.at[n],
                          hop_send.at[self.w, n], hop_recv.at[self.w, n], YN if colour else XN)

        def second_hop(self, n, colour):
            return remote(self.acc.at[n, self.block(1 if colour else 3)], self.far.at[n],
                          far_send.at[self.w, n], far_recv.at[self.w, n], XN if colour else YN)

        def out_copy(self, n):
            return pltpu.make_async_copy(self.acc.at[n, self.block(0)], self.out.at[:, cols(n)], out_sem.at[self.w, n])

        def compute(self, src):
            def body(n, colour):
                pair_copy(src, n).wait()
                self.acc[n] = self.lhs(0, d[:, cols(n)]) + self.lhs(1, pd[:, cols(n)])
                self.first_hop(n, colour).start()
            both_colours(body)

        def relay(self):
            def body(n, colour):
                onward, own = self.block(1 if colour else 3), self.block(0)
                self.first_hop(n, colour).wait_recv()
                self.acc[n, onward] = self.acc[n, onward] + self.near[n, self.block(1 - colour)]
                self.second_hop(n, colour).start()
                self.acc[n, own] = self.acc[n, own] + self.near[n, self.block(colour)]
            both_colours(body)

        def finish(self):
            def body(n, colour):
                own = self.block(0)
                self.second_hop(n, colour).wait_recv()
                self.acc[n, own] = self.acc[n, own] + self.far[n]
                self.out_copy(n).start()
            both_colours(body)

        def drain(self):
            def body(n, colour):
                self.first_hop(n, colour).wait_send()
                self.second_hop(n, colour).wait_send()
                self.out_copy(n).wait()
            both_colours(body)

    def w_tile(src, i):
        return pltpu.make_async_copy(src.at[cols(i)], wbuf.at[i % 2], w_sem.at[i % 2])

    def n_tile(src, i):
        return pltpu.make_async_copy(src.at[:, cols(i)], nbuf.at[i % 2], n_sem.at[i % 2])

    def tiles(streams, body):
        run([s(0) for s in streams])

        def step(i, carry):
            @pl.when(i < TILES - 1)
            def _():
                run([s(i + 1) for s in streams])
            finish_all([s(i) for s in streams])
            body(i, cols(i))
            return carry
        lax.fori_loop(0, TILES, step, 0)

    def normed_tile(i, c, v, vec):
        return (nbuf[i % 2, span(v, half), :] - row(vec, MEAN + v, c)) * row(vec, INV + v, c)

    def back_product(w_src, n_src, vec, which):
        def body(i, c):
            for v in TWO:
                grad = dot(d[span(v, half), :], wbuf[i % 2], TURN_RIGHT)
                normed = normed_tile(i, c, v, vec)
                grad = jnp.where(row(vec, GAIN, c) * normed + row(vec, SHIFT, c) > 0, grad, 0.0)
                dpre[span(v, half), c] = grad
                column_sums(mine, (which,), 2 * v, c, grad, grad * normed)
        tiles([functools.partial(w_tile, w_src), functools.partial(n_tile, n_src)], body)

    def norm_grad(n_src, vec, sums):
        def body(i, c):
            for v in TWO:
                part = span(v, half)
                mean, slope = row(sums, 2 * v, c) / rows_total, row(sums, 2 * v + 1, c) / rows_total
                grad = row(vec, GAIN, c) * row(vec, INV + v, c) * (
                    dpre[part, c] - (mean + normed_tile(i, c, v, vec) * slope))
                d[part, c] = grad.astype(BF16)
            pair_copy(d, i).start()
        tiles([functools.partial(n_tile, n_src)], body)

    def load(src, dst, k):
        return pltpu.make_async_copy(src, dst, load_sem.at[k])

    both_colours(lambda n, colour: pair_copy(dz, n).start())
    blk3, blk1 = gw3.shape[0], gw1.shape[0]

    def operand(src, pair):
        return [load(pair, xt.at[span(1, rows)], len(ORDER))] + [
            load(src.at[:, span(me ^ mask, blk3)], xt.at[span(0, rows), pl.ds(j * blk3, blk3)], j)
            for j, mask in enumerate(ORDER)]

    def lhs_x(k, right):
        return dot(xt[span(k, rows), :], right, TURN_LEFT)

    def lhs_h(k, right):
        return dot(ht[:, span(k, rows)], right)

    prod3 = Product(0, lhs_x, acc3, near3, far3, gw3)
    prod2 = Product(1, lhs_x, acc2, near2, far2, gw2)
    prod1 = Product(2, lhs_h, acc1, near1, far1, gw1)
    finish_all(run([load(dz, d, len(ORDER) + 1)] + operand(x2, x2_pair)))
    prod3.compute(dz)
    second = run(operand(x1, x1_pair))
    views = list(enumerate((h_a, h_b)))
    own_h = run([load(src, hv.at[span(v, half)], len(ORDER) + 1 + v) for v, src in views])
    pair_h = run([remote(src, hv.at[span(2 + v, half)], h_send.at[v], h_recv.at[v], PAIR) for v, src in views])
    back_product(w3, u2, vec2, 0)
    send_sums(0)
    prod3.relay()
    sums2[...] = take_sums(0)
    norm_grad(u2, vec2, sums2)
    finish_all(second)
    prod2.compute(d)
    pl.semaphore_signal(free_sem, inc=1, device_id=(me ^ PAIR,), device_id_type=MESH)
    back_product(w2, u1, vec1, 1)
    send_sums(1)
    finish_all(own_h + pair_h)
    for k in range(2 * len(TWO)):
        hturn[:, span(k, half)] = hv[span(k, half), :].T
    for j, mask in enumerate(ORDER):
        ht[span(j, blk1), :] = hturn[span(me ^ mask, blk1), :]
    prod3.finish()
    prod2.relay()
    sums1[...] = take_sums(1)
    pl.semaphore_wait(free_sem, 1)
    norm_grad(u1, vec1, sums1)
    prod1.compute(d)
    prod1.relay()
    prod2.finish()
    prod1.finish()
    for product in (prod3, prod2, prod1):
        product.drain()


ANYWHERE, ON_CHIP = pl.BlockSpec(memory_space=pl.ANY), pl.BlockSpec(memory_space=pltpu.VMEM)


def params(cid):
    return pltpu.CompilerParams(collective_id=cid, has_side_effects=True, vmem_limit_bytes=VMEM_BYTES)


def backward(rows_total, dz, *rest, cid):
    h_a = rest[4]
    rows, feats = dz.shape
    blk3, blk1 = feats // DEVICES, h_a.shape[1] // DEVICES
    groups = len(ORDER)
    blocks = (blk3, blk3, blk1)

    def per_weight(parts):
        return [pltpu.VMEM((TILES, parts * b, TILE), F32) for b in blocks]

    sums = jax.ShapeDtypeStruct((2 * len(TWO), feats), F32)
    return pl.pallas_call(
        functools.partial(backward_kernel, rows_total),
        out_shape=[jax.ShapeDtypeStruct((b, feats), F32) for b in blocks] + [sums, sums],
        in_specs=[ANYWHERE] * (len(rest) - 1) + [ON_CHIP] * 2,
        out_specs=[ANYWHERE] * WEIGHTS + [ON_CHIP] * 2,
        scratch_shapes=[pltpu.VMEM((rows, feats), BF16), pltpu.VMEM((rows, feats), BF16),
                        pltpu.VMEM((2 * rows, groups * blk3), BF16), pltpu.VMEM((2 * rows, h_a.shape[1]), BF16),
                        pltpu.VMEM((h_a.shape[1], 2 * rows), BF16), pltpu.VMEM((groups * blk1, 2 * rows), BF16),
                        pltpu.VMEM((rows, feats), F32),
                        pltpu.VMEM((2, TILE, feats), BF16), pltpu.VMEM((2, rows, TILE), F32)]
        + per_weight(groups) + per_weight(2) + per_weight(1)
        + [pltpu.VMEM((2,) + sums.shape, F32), pltpu.VMEM((2, DEVICES) + sums.shape, F32), DMA((DEVICES,))]
        + [DMA((TILES,))] * 2 + [DMA((WEIGHTS, TILES))] * 4 + [DMA((2, DEVICES))] * 2 + [DMA((2,))] * 2
        + [DMA((WEIGHTS, TILES))] + [DMA((2,))] * 2 + [pltpu.SemaphoreType.REGULAR],
        compiler_params=params(cid),
        name="backward",
    )(dz, *rest)


def forward_kernel(rows_total, lam, h_a, h_b, w1, w2, w3, gain1, shift1, gain2, shift2,
                   loss, u1, u2, x1, x2, x1_pair, x2_pair, dz, vec1, vec2,
                   hv, ubuf, vbuf, w2buf, w3buf, xbuf, zh, za, zb, corr, mine, slots, vec3, loss_mine, loss_slots,
                   load_sem, store_sem, pair_send, pair_recv, sum_send, sum_recv, za_send, za_recv, zb_send, zb_recv,
                   g_send, g_recv, loss_send, loss_recv, dz_sem):
    me = lax.axis_index("data")
    half = hv.shape[0] // 2
    feats = w2buf.shape[0]
    rblk, cblk = za.shape[2], zb.shape[2]
    greet()

    def load(src, dst, k):
        return pltpu.make_async_copy(src, dst, load_sem.at[k])

    w1_view = w3buf.at[pl.ds(0, w1.shape[0])]
    loads = run([load(h_a, hv.at[span(0, half)], 0), load(h_b, hv.at[span(1, half)], 1), load(w1, w1_view, 2)])
    all_entered()
    send_sums, take_sums = exchange(mine, slots, sum_send, sum_recv)
    send_loss, take_loss = exchange(loss_mine, loss_slots, loss_send, loss_recv)

    def each_tile(body):
        def step(n, carry):
            body(n, cols(n))
            return carry
        lax.fori_loop(0, TILES, step, 0)

    def take_vectors(e, v, vec):
        total = take_sums(e) / rows_total
        mean = total[:1]
        vec[pl.ds(MEAN + v, 1), :] = mean
        vec[pl.ds(INV + v, 1), :] = lax.rsqrt(total[1:] - mean * mean + NORM_EPS)

    def layer(e, v, left, weight, out):
        part = span(v, half)

        def body(n, c):
            value = dot(left[part, :], weight[:, c])
            out[part, c] = value
            column_sums(mine, (e,), 0, c, value, value * value)
        each_tile(body)
        send_sums(e)

    def normed_tile(values, v, c, vec):
        return (values[span(v, half), c] - row(vec, MEAN + v, c)) * row(vec, INV + v, c)

    def activate(v, values, vec):
        def body(n, c):
            pre = row(vec, GAIN, c) * normed_tile(values, v, c, vec) + row(vec, SHIFT, c)
            xbuf[span(v, half), c] = jnp.maximum(pre, 0.0).astype(BF16)
        each_tile(body)

    def store(src, dst, k):
        return pltpu.make_async_copy(src, dst, store_sem.at[k])

    def keep_rows(dst, pair, index):
        blk = feats // DEVICES
        return run([store(xbuf, dst, 2)] + [
            remote(xbuf.at[:, span(me ^ mask ^ PAIR, blk)], pair.at[:, pl.ds(j * blk, blk)],
                   pair_send.at[index, j], pair_recv.at[index, j], PAIR) for j, mask in enumerate(ORDER)])

    for vec, gain, shift in ((vec1, gain1, shift1), (vec2, gain2, shift2)):
        vec[pl.ds(GAIN, 1), :] = gain[...]
        vec[pl.ds(SHIFT, 1), :] = shift[...]
    finish_all(loads)
    load_w2 = load(w2, w2buf, 0)
    load_w2.start()
    for v in TWO:
        layer(v, v, hv, w1_view, ubuf)
    load_w3 = load(w3, w3buf, 2)
    store_u1 = store(ubuf, u1, 0)
    run([load_w3, store_u1])
    kept = []
    for v in TWO:
        take_vectors(v, v, vec1)
        activate(v, ubuf, vec1)
        if v:
            kept = keep_rows(x1, x1_pair, 0)
        else:
            load_w2.wait()
        layer(2 + v, v, xbuf, w2buf, vbuf)
    store_u2 = store(vbuf, u2, 1)
    store_u2.start()
    finish_all([store_u1, load_w3] + kept)
    for v in TWO:
        take_vectors(2 + v, v, vec2)
        activate(v, vbuf, vec2)
        if v:
            kept = keep_rows(x2, x2_pair, 1)
        layer(4 + v, v, xbuf, w3buf, ubuf)

    def embed(v):
        take_vectors(4 + v, v, vec3)

        def body(n, c):
            zh[span(v, half), c] = normed_tile(ubuf, v, c, vec3).astype(BF16)
        each_tile(body)

    def row_index(mask):
        dev = me ^ mask
        return dev // 4 * 2 + dev % 2

    def row_block(mask):
        return span(row_index(mask), rblk)

    def col_block(mask):
        return span((me ^ mask) // 2 % 2, cblk)

    quarter = half // 2
    started = []

    def go(copy):
        copy.start()
        started.append(copy)

    def za_direct(mask):
        return remote(zh.at[span(0, half), row_block(mask)], za.at[me], za_send.at[mask], za_recv.at[mask], mask)

    def za_relay(origin):
        slot = za.at[me ^ origin]
        return remote(slot, slot, za_send.at[origin ^ XN], za_recv.at[origin ^ XN], XN)

    def zb_slot(origin, k):
        return zb.at[me ^ origin, span(k, quarter)]

    def zb_direct(mask, k):
        return remote(zh.at[span(2 + k, quarter), col_block(mask)], zb_slot(OWN, k),
                      zb_send.at[mask, k], zb_recv.at[mask, k], mask)

    def zb_relay(origin, mask, k, send):
        return remote(zb_slot(origin, k), zb_slot(origin, k), zb_send.at[send, k], zb_recv.at[origin ^ mask, k], mask)

    def za_arrived(origin):
        slot = za.at[me ^ origin]
        remote(slot, slot, za_send.at[OWN], za_recv.at[origin], PAIR).wait_recv()

    def zb_arrived(origin, ks=TWO):
        for k in ks:
            zb_relay(origin, OWN, k, OWN).wait_recv()

    def accumulate(origin):
        corr[...] = corr[...] + dot(za[me ^ origin], zb[me ^ origin], TURN_LEFT)

    embed(0)
    for mask in (YN, XN, YP, XP, PAIR):
        go(za_direct(mask))
    embed(1)
    for k in TWO:
        for mask in (XN, YN, PAIR):
            go(zb_direct(mask, k))
    corr[...] = dot(zh[span(0, half), row_block(OWN)], zh[span(1, half), col_block(OWN)], TURN_LEFT)
    za_arrived(PAIR)
    zb_arrived(PAIR)
    accumulate(PAIR)
    for origin in (YN, YP):
        za_arrived(origin)
        go(za_relay(origin))
    for k in TWO:
        zb_arrived(XN, (k,))
        go(zb_relay(XN, YN, k, XP))
        go(zb_relay(XN, PAIR, k, YP))
        zb_arrived(YN, (k,))
        go(zb_relay(YN, PAIR, k, DG))
    za_arrived(XN)
    accumulate(XN)
    accumulate(YN)
    za_arrived(XP)
    for origin in (XP, YP):
        zb_arrived(origin)
        accumulate(origin)
    for k in TWO:
        zb_arrived(DG, (k,))
        go(zb_relay(DG, PAIR, k, DP))
    za_arrived(DG)
    accumulate(DG)
    za_arrived(DP)
    zb_arrived(DP)
    accumulate(DP)

    lam_off = lam[0]
    row_start, col_start = row_index(OWN) * rblk, me // 2 % 2 * cblk

    def grad_body(n, total):
        value = corr[:, cols(n)] / rows_total
        row_ids = row_start + lax.broadcasted_iota(jnp.int32, value.shape, 0)
        col_ids = col_start + n * TILE + lax.broadcasted_iota(jnp.int32, value.shape, 1)
        diag = row_ids == col_ids
        gap = 1.0 - value
        terms = jnp.where(diag, gap * gap, lam_off * value * value)
        grad = jnp.where(diag, -2.0 * gap, 2.0 * lam_off * value) / rows_total
        w2buf[row_block(OWN), pl.ds(pl.multiple_of(col_start + n * TILE, TILE), TILE)] = grad.astype(BF16)
        return total + jnp.sum(terms, axis=0, keepdims=True)
    loss_row = lax.fori_loop(0, cblk // TILE, grad_body, jnp.zeros((1, TILE), F32))

    pieces = g_send.shape[1]
    piece = rblk // pieces

    def g_slot(origin, k):
        return w2buf.at[span(row_index(origin) * pieces + k, piece), col_block(origin)]

    def g_copy(origin, mask, k, send):
        return remote(g_slot(origin, k), g_slot(origin, k), g_send.at[send, k], g_recv.at[origin ^ mask, k], mask)

    def g_arrived(origin, ks):
        for k in ks:
            g_copy(origin, OWN, k, OWN).wait_recv()

    def contribute(origin, k, count):
        part = span(row_index(origin) * (pieces // count) + k // count, count * piece)
        block = w2buf[part, col_block(origin)]
        first = dot(zh[span(1, half), col_block(origin)], block, TURN_RIGHT)
        where_a, where_b = (span(0, half), part), (span(1, half), col_block(origin))
        vbuf[where_a] = vbuf[where_a] + first if origin & XN else first
        second = dot(zh[span(0, half), part], block)
        vbuf[where_b] = second if origin in (OWN, XN) and not k else vbuf[where_b] + second

    every = range(pieces)
    even, odd = every[::2], every[1::2]
    for k, j in zip((*even, *odd), (*odd, *even)):
        go(g_copy(OWN, XN, k, PAIR))
        go(g_copy(OWN, YN, j, XN))
    for k in every:
        go(g_copy(OWN, PAIR, k, XP))
    loss_mine[0] = jnp.broadcast_to(jnp.sum(loss_row, axis=1, keepdims=True), loss_mine.shape[1:])
    send_loss(0)
    store_u2.wait()
    contribute(OWN, 0, pieces)
    g_arrived(PAIR, every)
    contribute(PAIR, 0, pieces)
    for k, j in zip(even, odd):
        g_arrived(XN, (k,))
        go(g_copy(XN, YN, k, YN))
        go(g_copy(XN, PAIR, k, YP))
        g_arrived(YN, (j,))
        go(g_copy(YN, XN, j, YN))
        go(g_copy(YN, PAIR, j, DG))
    for k, j in zip(odd, even):
        g_arrived(XN, (k,))
        go(g_copy(XN, PAIR, k, YP))
        g_arrived(YN, (j,))
        go(g_copy(YN, PAIR, j, DG))
    contribute(YN, 0, pieces)
    contribute(XN, 0, pieces)
    for origin in (YP, XP):
        g_arrived(origin, every)
        contribute(origin, 0, pieces)
    for k in even:
        now = (k, k + 1)
        for j in now:
            g_arrived(DG, (j,))
            go(g_copy(DG, PAIR, j, DP))
        contribute(DG, k, len(now))
        g_arrived(DP, now)
        contribute(DP, k, len(now))

    def sums_body(n, c):
        for v in TWO:
            grad = vbuf[span(v, half), c]
            column_sums(mine, (DG + v,), 0, c, grad, grad * normed_tile(ubuf, v, c, vec3))
    each_tile(sums_body)
    for v in TWO:
        send_sums(DG + v)
    finish_all(kept)
    loss[...] = take_loss(0)
    for v in TWO:
        mine[DG + v] = take_sums(DG + v) / rows_total

    def dz_copy(n):
        return pltpu.make_async_copy(xbuf.at[:, cols(n)], dz.at[:, cols(n)], dz_sem.at[n])

    def dz_body(n, c):
        for v in TWO:
            sums = mine[DG + v, :, c]
            grad = row(vec3, INV + v, c) * (
                vbuf[span(v, half), c] - (sums[:1] + normed_tile(ubuf, v, c, vec3) * sums[1:]))
            xbuf[span(v, half), c] = grad.astype(BF16)
        dz_copy(n).start()
    each_tile(dz_body)
    for copy in started:
        copy.wait_send()
    each_tile(lambda n, c: dz_copy(n).wait())


def forward(rows_total, lam, h_a, h_b, w1, w2, w3, *vectors, cid):
    half, depth = h_a.shape
    feats = w2.shape[0]
    full, pair, vec = (2 * half, feats), (2 * half, feats // 2), (VEC_ROWS, feats)
    small = (DEVICES, 128)
    outs = [(small, F32), (full, F32), (full, F32), (full, BF16), (full, BF16), (pair, BF16), (pair, BF16), (full, BF16),
            (vec, F32), (vec, F32)]
    scratch = [((2 * half, depth), BF16), (full, F32), (full, F32), ((feats, feats), BF16), ((feats, feats), BF16),
               (full, BF16), (full, BF16), ((DEVICES, half, feats // 4), BF16), ((DEVICES, half, feats // 2), BF16),
               ((feats // 4, feats // 2), F32), ((DEVICES, 2, feats), F32), ((DEVICES, DEVICES, 2, feats), F32),
               (vec, F32), ((1,) + small, F32), ((1, DEVICES) + small, F32)]
    return pl.pallas_call(
        functools.partial(forward_kernel, rows_total),
        out_shape=[jax.ShapeDtypeStruct(*out) for out in outs],
        in_specs=[pl.BlockSpec(memory_space=pltpu.SMEM)] + [ANYWHERE] * 5 + [ON_CHIP] * len(vectors),
        out_specs=[ON_CHIP] + [ANYWHERE] * (len(outs) - WEIGHTS) + [ON_CHIP] * 2,
        scratch_shapes=[pltpu.VMEM(*item) for item in scratch]
        + [DMA((WEIGHTS,))] * 2 + [DMA((2, len(ORDER)))] * 2 + [DMA((DEVICES, DEVICES))] * 2 + [DMA((DEVICES,))] * 2
        + [DMA((DEVICES, 2))] * 2 + [DMA((DEVICES, 4))] * 2 + [DMA((1, DEVICES))] * 2 + [DMA((TILES,))],
        compiler_params=params(cid),
        name="forward",
    )(lam, h_a, h_b, w1, w2, w3, *vectors)


def emit_kernel(gw3, gw2, gw1, sums2, sums1, out3, out2, out1, gain1, shift1, gain2, shift2, buf, in_sem, out_sem):
    step = gw1.shape[0]
    pieces = [(src, dst, k) for src, dst in ((gw3, out3), (gw2, out2), (gw1, out1)) for k in range(src.shape[0] // step)]
    ins = run([pltpu.make_async_copy(src.at[span(k, step)], buf.at[i], in_sem.at[i])
               for i, (src, dst, k) in enumerate(pieces)])
    outs = [pltpu.make_async_copy(buf.at[i], dst.at[span(k, step)], out_sem.at[i])
            for i, (src, dst, k) in enumerate(pieces)]
    for sums, gain, shift in ((sums1, gain1, shift1), (sums2, gain2, shift2)):
        both = sums[:2, :] + sums[2:, :]
        shift[...] = both[:1]
        gain[...] = both[1:]
    for before, after in zip(ins, outs):
        before.wait()
        after.start()
    finish_all(outs)


def emit(gw3, gw2, gw1, sums2, sums1):
    weights = (gw3, gw2, gw1)
    step, feats = gw1.shape
    count = sum(g.shape[0] for g in weights) // step
    return pl.pallas_call(
        emit_kernel,
        out_shape=[jax.ShapeDtypeStruct(g.shape, F32) for g in weights] + [jax.ShapeDtypeStruct((1, feats), F32)] * 4,
        in_specs=[ANYWHERE] * WEIGHTS + [ON_CHIP] * 2,
        out_specs=[ANYWHERE] * WEIGHTS + [ON_CHIP] * 4,
        scratch_shapes=[pltpu.VMEM((count, step, feats), F32)] + [DMA((count,))] * 2,
        name="emit",
    )(*weights, sums2, sums1)


def solution(mesh):
    shards = mesh.shape["data"]

    def local_step(h_a, h_b, w_one, w_two, w_three, gain_one, shift_one, gain_two, shift_two, lam_off):
        total_rows = h_a.shape[0] * shards
        loss, u1, u2, x1, x2, x1_pair, x2_pair, dz, vec1, vec2 = forward(
            total_rows, lam_off.reshape(1), h_a, h_b, w_one, w_two, w_three,
            *[v[None] for v in (gain_one, shift_one, gain_two, shift_two)], cid=0)
        grads = backward(total_rows, dz, x2, x2_pair, x1, x1_pair, h_a, h_b, w_three, w_two, u2, u1, vec2, vec1, cid=1)
        grad_w_three, grad_w_two, grad_w_one, *rest = emit(*grads)
        return (loss[0, 0], grad_w_one, grad_w_two, grad_w_three, *[v[0] for v in rest])

    row_spec = P("data", None)
    whole_mat = P(None, None)
    whole_vec = P(None)
    return jax.shard_map(
        local_step, mesh=mesh,
        in_specs=(row_spec, row_spec, whole_mat, whole_mat, whole_mat,
                  whole_vec, whole_vec, whole_vec, whole_vec, P()),
        out_specs=(P(), row_spec, row_spec, row_spec, whole_vec, whole_vec, whole_vec, whole_vec),
        check_vma=False)
```

```python
import functools

import jax
import jax.numpy as jnp
from jax import lax
from jax.experimental import pallas as pl
from jax.experimental.pallas import tpu as pltpu
from jax.sharding import PartitionSpec as P

NORM_EPS = 1e-5
MESH = pl.DeviceIdType.MESH
DEVICES = 8
OWN, PAIR, XN, XP, YN, YP, DG, DP = range(DEVICES)
FAR_FIRST = (DG, DP, XN, XP, YN, YP, PAIR)
ORDER = (OWN, XN, DG, YN)
TWO = range(2)
TILE = 256
TILES = 8
WEIGHTS = 3
GAIN, SHIFT, INV, MEAN, VEC_ROWS = 0, 1, 2, 4, 6
VMEM_BYTES = 67043328
TURN_LEFT = (((0,), (0,)), ((), ()))
TURN_RIGHT = (((1,), (1,)), ((), ()))
F32, BF16 = jnp.float32, jnp.bfloat16
DMA = pltpu.SemaphoreType.DMA


def dot(left, right, dims=None):
    if dims is None:
        return jnp.dot(left, right, preferred_element_type=F32)
    return lax.dot_general(left, right, dims, preferred_element_type=F32)


def span(index, size):
    return pl.ds(pl.multiple_of(index * size, size), size)


def cols(n):
    return span(n, TILE)


def row(ref, r, c):
    return ref[r:r + 1, c]


def remote(src, dst, send, recv, mask):
    return pltpu.make_async_remote_copy(src_ref=src, dst_ref=dst, send_sem=send, recv_sem=recv,
                                        device_id=(lax.axis_index("data") ^ mask,), device_id_type=MESH)


def greet():
    for mask in FAR_FIRST:
        pl.semaphore_signal(pltpu.get_barrier_semaphore(), inc=1, device_id=(lax.axis_index("data") ^ mask,),
                            device_id_type=MESH)


def all_entered():
    pl.semaphore_wait(pltpu.get_barrier_semaphore(), len(FAR_FIRST))


def column_sums(ref, lead, r, c, first, second):
    ref[lead + (slice(r, r + 1), c)] = jnp.sum(first, axis=0, keepdims=True)
    ref[lead + (slice(r + 1, r + 2), c)] = jnp.sum(second, axis=0, keepdims=True)


def exchange(mine, slots, send, recv):
    me = lax.axis_index("data")

    def copy(e, mask):
        return remote(mine.at[e], slots.at[e, me], send.at[e, mask], recv.at[e, mask], mask)

    def start(e):
        for mask in FAR_FIRST:
            copy(e, mask).start()
        slots[e, me] = mine[e]

    def take(e):
        for mask in FAR_FIRST:
            copy(e, mask).wait()
        return functools.reduce(jnp.add, [slots[e, k] for k in range(DEVICES)])
    return start, take


def exchange_halves(mine, mate, chips, whole, send, recv):
    me = lax.axis_index("data")
    width = mate.shape[-1]
    core, chip = me % 2, me // 2
    others = (DG, XN, YN)

    def pair_copy(e):
        return remote(mine.at[e, :, span(1 - core, width)], mate.at[e], send.at[e, OWN], recv.at[e, OWN], PAIR)

    def chip_copy(e, mask):
        return remote(chips.at[e, chip], chips.at[e, chip], send.at[e, mask], recv.at[e, mask], mask)

    def share(e):
        half = whole.at[e, :, span(core, width)]
        return remote(half, half, send.at[e, PAIR], recv.at[e, PAIR], PAIR)

    def start(e):
        pair_copy(e).start()

    def middle(e):
        pair_copy(e).wait()
        chips[e, chip] = mine[e, :, span(core, width)] + mate[e]
        for mask in others:
            chip_copy(e, mask).start()

    def take(e):
        for mask in others:
            chip_copy(e, mask).wait()
        whole[e, :, span(core, width)] = functools.reduce(jnp.add, [chips[e, k] for k in range(DEVICES // 2)])
        share(e).start()
        share(e).wait()
        return whole[e]
    return start, middle, take


def run(copies):
    for copy in copies:
        copy.start()
    return copies


def finish_all(copies):
    for copy in copies:
        copy.wait()


def backward_kernel(rows_total, dz, dz_pair, x2, x2_pair, x1, x1_pair, h_a, h_b, w3, w2, u2, u1, vec2, vec1,
                    gw3, gw2, gw1, sums2, sums1,
                    d, pd, xt, hv, hturn, ht, dpre, wbuf, nbuf, acc3, acc2, acc1, near3, near2, near1, far3, far2, far1,
                    mine, mate, chips, whole, load_sem, tile_sem, pair_send, pair_recv, hop_send, hop_recv, far_send, far_recv,
                    sum_send, sum_recv, h_send, h_recv, out_sem, w_sem, n_sem, free_sem):
    me = lax.axis_index("data")
    rows = d.shape[0]
    half = rows // 2
    greet()
    send_sums, pass_sums, take_sums = exchange_halves(mine, mate, chips, whole, sum_send, sum_recv)

    def pair_copy(n):
        return remote(d.at[:, cols(n)], pd.at[:, cols(n)], pair_send.at[n], pair_recv.at[n], PAIR)

    def both_colours(body):
        def step(i, carry):
            for colour in TWO:
                body(colour * (TILES // 2) + i, colour)
            return carry
        lax.fori_loop(0, TILES // 2, step, 0)

    class Product:
        def __init__(self, w, lhs, acc, near, far, out):
            self.w, self.lhs, self.acc, self.near, self.far, self.out = w, lhs, acc, near, far, out
            self.blk = out.shape[0]

        def block(self, j, count=1):
            return pl.ds(j * self.blk, count * self.blk)

        def first_hop(self, n, colour):
            return remote(self.acc.at[n, self.block(1 + colour, 2)], self.near.at[n],
                          hop_send.at[self.w, n], hop_recv.at[self.w, n], YN if colour else XN)

        def second_hop(self, n, colour):
            return remote(self.acc.at[n, self.block(1 if colour else 3)], self.far.at[n],
                          far_send.at[self.w, n], far_recv.at[self.w, n], XN if colour else YN)

        def out_copy(self, n):
            return pltpu.make_async_copy(self.acc.at[n, self.block(0)], self.out.at[:, cols(n)], out_sem.at[self.w, n])

        def fill(self, n, part):
            self.acc[n, part] = self.lhs(0, part, d[:, cols(n)]) + self.lhs(1, part, pd[:, cols(n)])

        def compute(self, parts, arrive, send):
            def body(n, colour):
                if arrive:
                    arrive(n)
                for j, count in parts[colour]:
                    self.fill(n, self.block(j, count))
                if send:
                    self.first_hop(n, colour).start()
            both_colours(body)

        def relay(self):
            def body(n, colour):
                onward, own = self.block(1 if colour else 3), self.block(0)
                self.first_hop(n, colour).wait_recv()
                self.acc[n, onward] = self.acc[n, onward] + self.near[n, self.block(1 - colour)]
                self.second_hop(n, colour).start()
                self.acc[n, own] = self.acc[n, own] + self.near[n, self.block(colour)]
            both_colours(body)

        def finish(self):
            def body(n, colour):
                own = self.block(0)
                self.second_hop(n, colour).wait_recv()
                self.acc[n, own] = self.acc[n, own] + self.far[n]
                self.out_copy(n).start()
            both_colours(body)

        def drain(self):
            def body(n, colour):
                self.first_hop(n, colour).wait_send()
                self.second_hop(n, colour).wait_send()
                self.out_copy(n).wait()
            both_colours(body)

    def w_tile(src, i):
        return pltpu.make_async_copy(src.at[cols(i)], wbuf.at[i % 2], w_sem.at[i % 2])

    def n_tile(src, i):
        return pltpu.make_async_copy(src.at[:, cols(i)], nbuf.at[i % 2], n_sem.at[i % 2])

    def tiles(streams, body):
        run([s(0) for s in streams])

        def step(i, carry):
            @pl.when(i < TILES - 1)
            def _():
                run([s(i + 1) for s in streams])
            finish_all([s(i) for s in streams])
            body(i, cols(i))
            return carry
        lax.fori_loop(0, TILES, step, 0)

    def normed_tile(i, c, v, vec):
        return (nbuf[i % 2, span(v, half), :] - row(vec, MEAN + v, c)) * row(vec, INV + v, c)

    def back_product(w_src, n_src, vec, which):
        def body(i, c):
            for v in TWO:
                grad = dot(d[span(v, half), :], wbuf[i % 2], TURN_RIGHT)
                normed = normed_tile(i, c, v, vec)
                grad = jnp.where(row(vec, GAIN, c) * normed + row(vec, SHIFT, c) > 0, grad, 0.0)
                dpre[span(v, half), c] = grad
                column_sums(mine, (which,), 2 * v, c, grad, grad * normed)
        tiles([functools.partial(w_tile, w_src), functools.partial(n_tile, n_src)], body)

    def norm_grad(n_src, vec, sums):
        def body(i, c):
            for v in TWO:
                part = span(v, half)
                mean, slope = row(sums, 2 * v, c) / rows_total, row(sums, 2 * v + 1, c) / rows_total
                grad = row(vec, GAIN, c) * row(vec, INV + v, c) * (
                    dpre[part, c] - (mean + normed_tile(i, c, v, vec) * slope))
                d[part, c] = grad.astype(BF16)
            pair_copy(i).start()
        tiles([functools.partial(n_tile, n_src)], body)

    def load(src, dst, k):
        return pltpu.make_async_copy(src, dst, load_sem.at[k])

    def dz_tiles(n):
        return [pltpu.make_async_copy(src.at[:, cols(n)], dst.at[:, cols(n)], tile_sem.at[k, n])
                for k, (src, dst) in enumerate(((dz, d), (dz_pair, pd)))]

    blk3, blk1 = gw3.shape[0], gw1.shape[0]

    def operand(src, pair):
        return [load(pair, xt.at[span(1, rows)], len(ORDER))] + [
            load(src.at[:, span(me ^ mask, blk3)], xt.at[span(0, rows), pl.ds(j * blk3, blk3)], j)
            for j, mask in enumerate(ORDER)]

    def lhs_x(k, part, right):
        return dot(xt[span(k, rows), part], right, TURN_LEFT)

    def lhs_h(k, part, right):
        return dot(ht[part, span(k, rows)], right)

    prod3 = Product(0, lhs_x, acc3, near3, far3, gw3)
    prod2 = Product(1, lhs_x, acc2, near2, far2, gw2)
    prod1 = Product(2, lhs_h, acc1, near1, far1, gw1)
    first = run(operand(x2, x2_pair))
    both_colours(lambda n, colour: run(dz_tiles(n)) and None)
    all_entered()
    finish_all(first)
    everything = ([(0, len(ORDER))],) * 2
    prod3.compute(([(1, 2)], [(2, 2)]), lambda n: finish_all(dz_tiles(n)), True)
    back_product(w3, u2, vec2, 0)
    send_sums(0)
    prod3.compute(([(0, 1), (3, 1)], [(0, 2)]), None, False)
    pass_sums(0)
    second = run(operand(x1, x1_pair))
    views = list(enumerate((h_a, h_b)))
    own_h = run([load(src, hv.at[span(v, half)], len(ORDER) + 1 + v) for v, src in views])
    pair_h = run([remote(src, hv.at[span(2 + v, half)], h_send.at[v], h_recv.at[v], PAIR) for v, src in views])
    prod3.relay()
    sums2[...] = take_sums(0)
    norm_grad(u2, vec2, sums2)
    finish_all(second)
    prod2.compute(everything, lambda n: pair_copy(n).wait(), True)
    pl.semaphore_signal(free_sem, inc=1, device_id=(me ^ PAIR,), device_id_type=MESH)
    back_product(w2, u1, vec1, 1)
    send_sums(1)
    finish_all(own_h + pair_h)
    for k in range(2 * len(TWO)):
        hturn[:, span(k, half)] = hv[span(k, half), :].T
    for j, mask in enumerate(ORDER):
        ht[span(j, blk1), :] = hturn[span(me ^ mask, blk1), :]
    pass_sums(1)
    prod3.finish()
    prod2.relay()
    sums1[...] = take_sums(1)
    pl.semaphore_wait(free_sem, 1)
    norm_grad(u1, vec1, sums1)
    prod1.compute(everything, lambda n: pair_copy(n).wait(), True)
    prod1.relay()
    prod2.finish()
    prod1.finish()
    for product in (prod3, prod2, prod1):
        product.drain()


ANYWHERE, ON_CHIP = pl.BlockSpec(memory_space=pl.ANY), pl.BlockSpec(memory_space=pltpu.VMEM)
SCALARS = pl.BlockSpec(memory_space=pltpu.SMEM)


def params(cid):
    return pltpu.CompilerParams(collective_id=cid, has_side_effects=True, vmem_limit_bytes=VMEM_BYTES)


def backward(rows_total, dz, *rest, cid):
    h_a = rest[5]
    rows, feats = dz.shape
    blk3, blk1 = feats // DEVICES, h_a.shape[1] // DEVICES
    groups = len(ORDER)
    blocks = (blk3, blk3, blk1)

    def per_weight(parts):
        return [pltpu.VMEM((TILES, parts * b, TILE), F32) for b in blocks]

    sums = jax.ShapeDtypeStruct((2 * len(TWO), feats), F32)
    half_sums = (2 * len(TWO), feats // 2)
    return pl.pallas_call(
        functools.partial(backward_kernel, rows_total),
        out_shape=[jax.ShapeDtypeStruct((b, feats), F32) for b in blocks] + [sums, sums],
        in_specs=[ANYWHERE] * (len(rest) - 1) + [ON_CHIP] * 2,
        out_specs=[ANYWHERE] * WEIGHTS + [ON_CHIP] * 2,
        scratch_shapes=[pltpu.VMEM((rows, feats), BF16), pltpu.VMEM((rows, feats), BF16),
                        pltpu.VMEM((2 * rows, groups * blk3), BF16), pltpu.VMEM((2 * rows, h_a.shape[1]), BF16),
                        pltpu.VMEM((h_a.shape[1], 2 * rows), BF16), pltpu.VMEM((groups * blk1, 2 * rows), BF16),
                        pltpu.VMEM((rows, feats), F32),
                        pltpu.VMEM((2, TILE, feats), BF16), pltpu.VMEM((2, rows, TILE), F32)]
        + per_weight(groups) + per_weight(2) + per_weight(1)
        + [pltpu.VMEM(shape, F32) for shape in ((2,) + sums.shape, (2,) + half_sums, (2, DEVICES // 2) + half_sums,
                                                (2,) + sums.shape)]
        + [DMA((DEVICES,)), DMA((2, TILES))]
        + [DMA((TILES,))] * 2 + [DMA((WEIGHTS, TILES))] * 4 + [DMA((2, DEVICES))] * 2 + [DMA((2,))] * 2
        + [DMA((WEIGHTS, TILES))] + [DMA((2,))] * 2 + [pltpu.SemaphoreType.REGULAR],
        compiler_params=params(cid),
        name="backward",
    )(dz, *rest)


def forward_kernel(rows_total, lam, h_a, h_b, w1, w2, w3, gain1, shift1, gain2, shift2,
                   loss, u1, u2, x1, x2, x1_pair, x2_pair, dz, dz_pair, vec1, vec2,
                   hv, ubuf, vbuf, w2buf, w3buf, xbuf, zh, za, zb, corr, mine, slots, vec3, loss_mine, loss_slots,
                   load_sem, store_sem, pair_send, pair_recv, sum_send, sum_recv, za_send, za_recv, zb_send, zb_recv,
                   g_send, g_recv, loss_send, loss_recv, dz_sem, dz_send, dz_recv):
    me = lax.axis_index("data")
    half = hv.shape[0] // 2
    feats = w2buf.shape[0]
    rblk, cblk = za.shape[2], zb.shape[2]
    greet()

    def load(src, dst, k):
        return pltpu.make_async_copy(src, dst, load_sem.at[k])

    w1_view = w3buf.at[pl.ds(0, w1.shape[0])]
    loads = run([load(h_a, hv.at[span(0, half)], 0), load(h_b, hv.at[span(1, half)], 1), load(w1, w1_view, 2)])
    all_entered()
    send_sums, take_sums = exchange(mine, slots, sum_send, sum_recv)
    send_loss, take_loss = exchange(loss_mine, loss_slots, loss_send, loss_recv)

    def each_tile(body):
        def step(n, carry):
            body(n, cols(n))
            return carry
        lax.fori_loop(0, TILES, step, 0)

    def take_vectors(e, v, vec):
        total = take_sums(e) / rows_total
        mean = total[:1]
        vec[pl.ds(MEAN + v, 1), :] = mean
        vec[pl.ds(INV + v, 1), :] = lax.rsqrt(total[1:] - mean * mean + NORM_EPS)

    def layer(e, v, left, weight, out):
        part = span(v, half)

        def body(n, c):
            value = dot(left[part, :], weight[:, c])
            out[part, c] = value
            column_sums(mine, (e,), 0, c, value, value * value)
        each_tile(body)
        send_sums(e)

    def normed_tile(values, v, c, vec):
        return (values[span(v, half), c] - row(vec, MEAN + v, c)) * row(vec, INV + v, c)

    def activate(v, values, vec):
        def body(n, c):
            pre = row(vec, GAIN, c) * normed_tile(values, v, c, vec) + row(vec, SHIFT, c)
            xbuf[span(v, half), c] = jnp.maximum(pre, 0.0).astype(BF16)
        each_tile(body)

    def store(src, dst, k):
        return pltpu.make_async_copy(src, dst, store_sem.at[k])

    def keep_rows(dst, pair, index):
        blk = feats // DEVICES
        return run([store(xbuf, dst, 2)] + [
            remote(xbuf.at[:, span(me ^ mask ^ PAIR, blk)], pair.at[:, pl.ds(j * blk, blk)],
                   pair_send.at[index, j], pair_recv.at[index, j], PAIR) for j, mask in enumerate(ORDER)])

    for vec, gain, shift in ((vec1, gain1, shift1), (vec2, gain2, shift2)):
        vec[pl.ds(GAIN, 1), :] = gain[...]
        vec[pl.ds(SHIFT, 1), :] = shift[...]
    finish_all(loads)
    load_w2 = load(w2, w2buf, 0)
    load_w2.start()
    for v in TWO:
        layer(v, v, hv, w1_view, ubuf)
    load_w3 = load(w3, w3buf, 2)
    store_u1 = store(ubuf, u1, 0)
    run([load_w3, store_u1])
    kept = []
    for v in TWO:
        take_vectors(v, v, vec1)
        activate(v, ubuf, vec1)
        if v:
            kept = keep_rows(x1, x1_pair, 0)
        else:
            load_w2.wait()
        layer(2 + v, v, xbuf, w2buf, vbuf)
    store_u2 = store(vbuf, u2, 1)
    store_u2.start()
    finish_all([store_u1, load_w3] + kept)
    for v in TWO:
        take_vectors(2 + v, v, vec2)
        activate(v, vbuf, vec2)
        if v:
            kept = keep_rows(x2, x2_pair, 1)
        layer(4 + v, v, xbuf, w3buf, ubuf)

    def embed(v):
        take_vectors(4 + v, v, vec3)

        def body(n, c):
            zh[span(v, half), c] = normed_tile(ubuf, v, c, vec3).astype(BF16)
        each_tile(body)

    def row_index(mask):
        dev = me ^ mask
        return dev // 4 * 2 + dev % 2

    def row_block(mask):
        return span(row_index(mask), rblk)

    def col_block(mask):
        return span((me ^ mask) // 2 % 2, cblk)

    quarter = half // 2
    started = []

    def go(copy):
        copy.start()
        started.append(copy)

    def za_direct(mask):
        return remote(zh.at[span(0, half), row_block(mask)], za.at[me], za_send.at[mask], za_recv.at[mask], mask)

    def za_relay(origin):
        slot = za.at[me ^ origin]
        return remote(slot, slot, za_send.at[origin ^ XN], za_recv.at[origin ^ XN], XN)

    def zb_slot(origin, k):
        return zb.at[me ^ origin, span(k, quarter)]

    def zb_direct(mask, k):
        return remote(zh.at[span(2 + k, quarter), col_block(mask)], zb_slot(OWN, k),
                      zb_send.at[mask, k], zb_recv.at[mask, k], mask)

    def zb_relay(origin, mask, k, send):
        return remote(zb_slot(origin, k), zb_slot(origin, k), zb_send.at[send, k], zb_recv.at[origin ^ mask, k], mask)

    def za_arrived(origin):
        slot = za.at[me ^ origin]
        remote(slot, slot, za_send.at[OWN], za_recv.at[origin], PAIR).wait_recv()

    def zb_arrived(origin, ks=TWO):
        for k in ks:
            zb_relay(origin, OWN, k, OWN).wait_recv()

    def accumulate(origin):
        corr[...] = corr[...] + dot(za[me ^ origin], zb[me ^ origin], TURN_LEFT)

    embed(0)
    for mask in (YN, XN, YP, XP, PAIR):
        go(za_direct(mask))
    embed(1)
    for k in TWO:
        for mask in (XN, YN, PAIR):
            go(zb_direct(mask, k))
    corr[...] = dot(zh[span(0, half), row_block(OWN)], zh[span(1, half), col_block(OWN)], TURN_LEFT)
    za_arrived(PAIR)
    zb_arrived(PAIR)
    accumulate(PAIR)
    for origin in (YN, YP):
        za_arrived(origin)
        go(za_relay(origin))
    for k in TWO:
        zb_arrived(XN, (k,))
        go(zb_relay(XN, YN, k, XP))
        go(zb_relay(XN, PAIR, k, YP))
        zb_arrived(YN, (k,))
        go(zb_relay(YN, PAIR, k, DG))
    za_arrived(XN)
    accumulate(XN)
    accumulate(YN)
    za_arrived(XP)
    for origin in (XP, YP):
        zb_arrived(origin)
        accumulate(origin)
    for k in TWO:
        zb_arrived(DG, (k,))
        go(zb_relay(DG, PAIR, k, DP))
    za_arrived(DG)
    accumulate(DG)
    za_arrived(DP)
    zb_arrived(DP)
    accumulate(DP)

    lam_off = lam[0]
    row_start, col_start = row_index(OWN) * rblk, me // 2 % 2 * cblk

    def grad_body(n, total):
        value = corr[:, cols(n)] / rows_total
        row_ids = row_start + lax.broadcasted_iota(jnp.int32, value.shape, 0)
        col_ids = col_start + n * TILE + lax.broadcasted_iota(jnp.int32, value.shape, 1)
        diag = row_ids == col_ids
        gap = 1.0 - value
        terms = jnp.where(diag, gap * gap, lam_off * value * value)
        grad = jnp.where(diag, -2.0 * gap, 2.0 * lam_off * value) / rows_total
        w2buf[row_block(OWN), pl.ds(pl.multiple_of(col_start + n * TILE, TILE), TILE)] = grad.astype(BF16)
        return total + jnp.sum(terms, axis=0, keepdims=True)
    loss_row = lax.fori_loop(0, cblk // TILE, grad_body, jnp.zeros((1, TILE), F32))

    pieces = g_send.shape[1]
    piece = rblk // pieces

    def g_slot(origin, k):
        return w2buf.at[span(row_index(origin) * pieces + k, piece), col_block(origin)]

    def g_copy(origin, mask, k, send):
        return remote(g_slot(origin, k), g_slot(origin, k), g_send.at[send, k], g_recv.at[origin ^ mask, k], mask)

    def g_arrived(origin, ks):
        for k in ks:
            g_copy(origin, OWN, k, OWN).wait_recv()

    def contribute(origin, k, count):
        part = span(row_index(origin) * (pieces // count) + k // count, count * piece)
        block = w2buf[part, col_block(origin)]
        first = dot(zh[span(1, half), col_block(origin)], block, TURN_RIGHT)
        where_a, where_b = (span(0, half), part), (span(1, half), col_block(origin))
        vbuf[where_a] = vbuf[where_a] + first if origin & XN else first
        second = dot(zh[span(0, half), part], block)
        vbuf[where_b] = second if origin in (OWN, XN) and not k else vbuf[where_b] + second

    every = range(pieces)
    even, odd = every[::2], every[1::2]
    for k, j in zip((*even, *odd), (*odd, *even)):
        go(g_copy(OWN, XN, k, PAIR))
        go(g_copy(OWN, YN, j, XN))
    for k in every:
        go(g_copy(OWN, PAIR, k, XP))
    loss_mine[0] = jnp.broadcast_to(jnp.sum(loss_row, axis=1, keepdims=True), loss_mine.shape[1:])
    send_loss(0)
    store_u2.wait()
    contribute(OWN, 0, pieces)
    g_arrived(PAIR, every)
    contribute(PAIR, 0, pieces)
    for k, j in zip(even, odd):
        g_arrived(XN, (k,))
        go(g_copy(XN, YN, k, YN))
        go(g_copy(XN, PAIR, k, YP))
        g_arrived(YN, (j,))
        go(g_copy(YN, XN, j, YN))
        go(g_copy(YN, PAIR, j, DG))
    for k, j in zip(odd, even):
        g_arrived(XN, (k,))
        go(g_copy(XN, PAIR, k, YP))
        g_arrived(YN, (j,))
        go(g_copy(YN, PAIR, j, DG))
    contribute(YN, 0, pieces)
    contribute(XN, 0, pieces)
    for origin in (YP, XP):
        g_arrived(origin, every)
        contribute(origin, 0, pieces)
    for k in even:
        now = (k, k + 1)
        for j in now:
            g_arrived(DG, (j,))
            go(g_copy(DG, PAIR, j, DP))
        contribute(DG, k, len(now))
        g_arrived(DP, now)
        contribute(DP, k, len(now))

    def sums_body(n, c):
        for v in TWO:
            grad = vbuf[span(v, half), c]
            column_sums(mine, (DG + v,), 0, c, grad, grad * normed_tile(ubuf, v, c, vec3))
    each_tile(sums_body)
    for v in TWO:
        send_sums(DG + v)
    finish_all(kept)
    loss[...] = take_loss(0)
    for v in TWO:
        mine[DG + v] = take_sums(DG + v) / rows_total

    def dz_copies(n):
        tile = xbuf.at[:, cols(n)]
        return [remote(tile, dz_pair.at[:, cols(n)], dz_send.at[n], dz_recv.at[n], PAIR),
                pltpu.make_async_copy(tile, dz.at[:, cols(n)], dz_sem.at[n])]

    def dz_body(n, c):
        for v in TWO:
            sums = mine[DG + v, :, c]
            grad = row(vec3, INV + v, c) * (
                vbuf[span(v, half), c] - (sums[:1] + normed_tile(ubuf, v, c, vec3) * sums[1:]))
            xbuf[span(v, half), c] = grad.astype(BF16)
        run(dz_copies(n))
    each_tile(dz_body)
    for copy in started:
        copy.wait_send()
    each_tile(lambda n, c: finish_all(dz_copies(n)))


def forward(rows_total, lam, h_a, h_b, w1, w2, w3, *vectors, cid):
    half, depth = h_a.shape
    feats = w2.shape[0]
    full, pair, vec = (2 * half, feats), (2 * half, feats // 2), (VEC_ROWS, feats)
    small = (DEVICES, 128)
    outs = [(small, F32), (full, F32), (full, F32), (full, BF16), (full, BF16), (pair, BF16), (pair, BF16), (full, BF16), (full, BF16),
            (vec, F32), (vec, F32)]
    scratch = [((2 * half, depth), BF16), (full, F32), (full, F32), ((feats, feats), BF16), ((feats, feats), BF16),
               (full, BF16), (full, BF16), ((DEVICES, half, feats // 4), BF16), ((DEVICES, half, feats // 2), BF16),
               ((feats // 4, feats // 2), F32), ((DEVICES, 2, feats), F32), ((DEVICES, DEVICES, 2, feats), F32),
               (vec, F32), ((1,) + small, F32), ((1, DEVICES) + small, F32)]
    return pl.pallas_call(
        functools.partial(forward_kernel, rows_total),
        out_shape=[jax.ShapeDtypeStruct(*out) for out in outs],
        in_specs=[SCALARS] + [ANYWHERE] * 5 + [ON_CHIP] * len(vectors),
        out_specs=[ON_CHIP] + [ANYWHERE] * (len(outs) - WEIGHTS) + [ON_CHIP] * 2,
        scratch_shapes=[pltpu.VMEM(*item) for item in scratch]
        + [DMA((WEIGHTS,))] * 2 + [DMA((2, len(ORDER)))] * 2 + [DMA((DEVICES, DEVICES))] * 2 + [DMA((DEVICES,))] * 2
        + [DMA((DEVICES, 2))] * 2 + [DMA((DEVICES, 4))] * 2 + [DMA((1, DEVICES))] * 2 + [DMA((TILES,))] * WEIGHTS,
        compiler_params=params(cid),
        name="forward",
    )(lam, h_a, h_b, w1, w2, w3, *vectors)


def emit_kernel(gw3, gw2, gw1, sums2, sums1, loss, loss_out, out3, out2, out1, gain1, shift1, gain2, shift2, buf, in_sem, out_sem):
    step = gw1.shape[0]
    pieces = [(src, dst, k) for src, dst in ((gw3, out3), (gw2, out2), (gw1, out1)) for k in range(src.shape[0] // step)]
    ins = run([pltpu.make_async_copy(src.at[span(k, step)], buf.at[i], in_sem.at[i])
               for i, (src, dst, k) in enumerate(pieces)])
    outs = [pltpu.make_async_copy(buf.at[i], dst.at[span(k, step)], out_sem.at[i])
            for i, (src, dst, k) in enumerate(pieces)]
    for sums, gain, shift in ((sums1, gain1, shift1), (sums2, gain2, shift2)):
        both = sums[:2, :] + sums[2:, :]
        shift[...] = both[:1]
        gain[...] = both[1:]
    loss_out[0, 0] = loss[0, 0]
    for before, after in zip(ins, outs):
        before.wait()
        after.start()
    finish_all(outs)


def emit(gw3, gw2, gw1, sums2, sums1, loss):
    weights = (gw3, gw2, gw1)
    step, feats = gw1.shape
    count = sum(g.shape[0] for g in weights) // step
    return pl.pallas_call(
        emit_kernel,
        out_shape=[jax.ShapeDtypeStruct((1, 1), F32)] + [jax.ShapeDtypeStruct(g.shape, F32) for g in weights]
        + [jax.ShapeDtypeStruct((1, feats), F32)] * 4,
        in_specs=[ANYWHERE] * WEIGHTS + [ON_CHIP] * 2 + [SCALARS],
        out_specs=[SCALARS] + [ANYWHERE] * WEIGHTS + [ON_CHIP] * 4,
        scratch_shapes=[pltpu.VMEM((count, step, feats), F32)] + [DMA((count,))] * 2,
        name="emit",
    )(*weights, sums2, sums1, loss)


def solution(mesh):
    shards = mesh.shape["data"]

    def local_step(h_a, h_b, w_one, w_two, w_three, gain_one, shift_one, gain_two, shift_two, lam_off):
        total_rows = h_a.shape[0] * shards
        loss, u1, u2, x1, x2, x1_pair, x2_pair, dz, dz_pair, vec1, vec2 = forward(
            total_rows, lam_off.reshape(1), h_a, h_b, w_one, w_two, w_three,
            *[v[None] for v in (gain_one, shift_one, gain_two, shift_two)], cid=0)
        grads = backward(total_rows, dz, dz_pair, x2, x2_pair, x1, x1_pair, h_a, h_b, w_three, w_two, u2, u1, vec2, vec1,
                         cid=1)
        loss, grad_w_three, grad_w_two, grad_w_one, *rest = emit(*grads, loss)
        return (loss.reshape(()), grad_w_one, grad_w_two, grad_w_three, *[v[0] for v in rest])

    row_spec = P("data", None)
    whole_mat = P(None, None)
    whole_vec = P(None)
    return jax.shard_map(
        local_step, mesh=mesh,
        in_specs=(row_spec, row_spec, whole_mat, whole_mat, whole_mat,
                  whole_vec, whole_vec, whole_vec, whole_vec, P()),
        out_specs=(P(), row_spec, row_spec, row_spec, whole_vec, whole_vec, whole_vec, whole_vec),
        check_vma=False)
```

```python
import functools

import jax
import jax.numpy as jnp
from jax import lax
from jax.experimental import pallas as pl
from jax.experimental.pallas import tpu as pltpu
from jax.sharding import PartitionSpec as P

NORM_EPS = 1e-5
MESH = pl.DeviceIdType.MESH
DEVICES = 8
OWN, PAIR, XN, XP, YN, YP, DG, DP = range(DEVICES)
FAR_FIRST = (DG, DP, XN, XP, YN, YP, PAIR)
ORDER = (OWN, XN, DG, YN)
TWO = range(2)
TILE = 256
TILES = 8
WEIGHTS = 3
GAIN, SHIFT, INV, MEAN, VEC_ROWS = 0, 1, 2, 4, 6
VMEM_BYTES = 67043328
TURN_LEFT = (((0,), (0,)), ((), ()))
TURN_RIGHT = (((1,), (1,)), ((), ()))
F32, BF16 = jnp.float32, jnp.bfloat16
DMA = pltpu.SemaphoreType.DMA


def dot(left, right, dims=None):
    if dims is None:
        return jnp.dot(left, right, preferred_element_type=F32)
    return lax.dot_general(left, right, dims, preferred_element_type=F32)


def span(index, size):
    return pl.ds(pl.multiple_of(index * size, size), size)


def cols(n):
    return span(n, TILE)


def row(ref, r, c):
    return ref[r:r + 1, c]


def remote(src, dst, send, recv, mask):
    return pltpu.make_async_remote_copy(src_ref=src, dst_ref=dst, send_sem=send, recv_sem=recv,
                                        device_id=(lax.axis_index("data") ^ mask,), device_id_type=MESH)


def greet():
    for mask in FAR_FIRST:
        pl.semaphore_signal(pltpu.get_barrier_semaphore(), inc=1, device_id=(lax.axis_index("data") ^ mask,),
                            device_id_type=MESH)


def all_entered():
    pl.semaphore_wait(pltpu.get_barrier_semaphore(), len(FAR_FIRST))


def column_sums(ref, lead, r, c, first, second):
    ref[lead + (slice(r, r + 1), c)] = jnp.sum(first, axis=0, keepdims=True)
    ref[lead + (slice(r + 1, r + 2), c)] = jnp.sum(second, axis=0, keepdims=True)


def exchange(mine, slots, send, recv):
    me = lax.axis_index("data")

    def copy(e, mask):
        return remote(mine.at[e], slots.at[e, me], send.at[e, mask], recv.at[e, mask], mask)

    def start(e):
        for mask in FAR_FIRST:
            copy(e, mask).start()
        slots[e, me] = mine[e]

    def take(e):
        for mask in FAR_FIRST:
            copy(e, mask).wait()
        return functools.reduce(jnp.add, [slots[e, k] for k in range(DEVICES)])
    return start, take


def exchange_halves(mine, mate, chips, whole, send, recv):
    me = lax.axis_index("data")
    width = mate.shape[-1]
    core, chip = me % 2, me // 2
    others = (DG, XN, YN)

    def pair_copy(e):
        return remote(mine.at[e, :, span(1 - core, width)], mate.at[e], send.at[e, OWN], recv.at[e, OWN], PAIR)

    def chip_copy(e, mask):
        return remote(chips.at[e, chip], chips.at[e, chip], send.at[e, mask], recv.at[e, mask], mask)

    def share(e):
        half = whole.at[e, :, span(core, width)]
        return remote(half, half, send.at[e, PAIR], recv.at[e, PAIR], PAIR)

    def start(e):
        pair_copy(e).start()

    def middle(e):
        pair_copy(e).wait()
        chips[e, chip] = mine[e, :, span(core, width)] + mate[e]
        for mask in others:
            chip_copy(e, mask).start()

    def take(e):
        for mask in others:
            chip_copy(e, mask).wait()
        whole[e, :, span(core, width)] = functools.reduce(jnp.add, [chips[e, k] for k in range(DEVICES // 2)])
        share(e).start()
        share(e).wait()
        return whole[e]
    return start, middle, take


def run(copies):
    for copy in copies:
        copy.start()
    return copies


def finish_all(copies):
    for copy in copies:
        copy.wait()


def backward_kernel(rows_total, dz, dz_pair, x2, x2_pair, x1, x1_pair, h_a, h_b, w3, w2, u2, u1, vec2, vec1,
                    gw3, gw2, gw1, sums2, sums1,
                    d, pd, xt, hv, hturn, ht, dpre, wbuf, nbuf, acc3, acc2, acc1, near3, near2, near1, far3, far2, far1,
                    mine, mate, chips, whole, load_sem, tile_sem, pair_send, pair_recv, hop_send, hop_recv, far_send, far_recv,
                    sum_send, sum_recv, h_send, h_recv, out_sem, w_sem, n_sem, free_sem):
    me = lax.axis_index("data")
    rows = d.shape[0]
    half = rows // 2
    greet()
    send_sums, pass_sums, take_sums = exchange_halves(mine, mate, chips, whole, sum_send, sum_recv)

    def pair_copy(n, src=d):
        return remote(src.at[:, cols(n)], pd.at[:, cols(n)], pair_send.at[n], pair_recv.at[n], PAIR)

    def both_colours(body):
        def step(i, carry):
            for colour in TWO:
                body(colour * (TILES // 2) + i, colour)
            return carry
        lax.fori_loop(0, TILES // 2, step, 0)

    class Product:
        def __init__(self, w, lhs, acc, near, far, out):
            self.w, self.lhs, self.acc, self.near, self.far, self.out = w, lhs, acc, near, far, out
            self.blk = out.shape[0]

        def block(self, j, count=1):
            return pl.ds(j * self.blk, count * self.blk)

        def first_hop(self, n, colour):
            return remote(self.acc.at[n, self.block(1 + colour, 2)], self.near.at[n],
                          hop_send.at[self.w, n], hop_recv.at[self.w, n], YN if colour else XN)

        def second_hop(self, n, colour):
            return remote(self.acc.at[n, self.block(1 if colour else 3)], self.far.at[n],
                          far_send.at[self.w, n], far_recv.at[self.w, n], XN if colour else YN)

        def out_copy(self, n):
            return pltpu.make_async_copy(self.acc.at[n, self.block(0)], self.out.at[:, cols(n)], out_sem.at[self.w, n])

        def fill(self, n, part):
            self.acc[n, part] = self.lhs(0, part, d[:, cols(n)]) + self.lhs(1, part, pd[:, cols(n)])

        def compute(self, parts, arrive, send):
            def body(n, colour):
                if arrive:
                    arrive(n)
                for j, count in parts[colour]:
                    self.fill(n, self.block(j, count))
                if send:
                    self.first_hop(n, colour).start()
            both_colours(body)

        def relay(self):
            def body(n, colour):
                onward, own = self.block(1 if colour else 3), self.block(0)
                self.first_hop(n, colour).wait_recv()
                self.acc[n, onward] = self.acc[n, onward] + self.near[n, self.block(1 - colour)]
                self.second_hop(n, colour).start()
                self.acc[n, own] = self.acc[n, own] + self.near[n, self.block(colour)]
            both_colours(body)

        def finish(self):
            def body(n, colour):
                own = self.block(0)
                self.second_hop(n, colour).wait_recv()
                self.acc[n, own] = self.acc[n, own] + self.far[n]
                self.out_copy(n).start()
            both_colours(body)

        def drain(self):
            def body(n, colour):
                self.first_hop(n, colour).wait_send()
                self.second_hop(n, colour).wait_send()
                self.out_copy(n).wait()
            both_colours(body)

    def w_tile(src, i):
        return pltpu.make_async_copy(src.at[cols(i)], wbuf.at[i % 2], w_sem.at[i % 2])

    def n_tile(src, i):
        return pltpu.make_async_copy(src.at[:, cols(i)], nbuf.at[i % 2], n_sem.at[i % 2])

    def tiles(streams, body):
        run([s(0) for s in streams])

        def step(i, carry):
            @pl.when(i < TILES - 1)
            def _():
                run([s(i + 1) for s in streams])
            finish_all([s(i) for s in streams])
            body(i, cols(i))
            return carry
        lax.fori_loop(0, TILES, step, 0)

    def normed_tile(i, c, v, vec):
        return (nbuf[i % 2, span(v, half), :] - row(vec, MEAN + v, c)) * row(vec, INV + v, c)

    def back_product(w_src, n_src, vec, which):
        def body(i, c):
            for v in TWO:
                grad = dot(d[span(v, half), :], wbuf[i % 2], TURN_RIGHT)
                normed = normed_tile(i, c, v, vec)
                grad = jnp.where(row(vec, GAIN, c) * normed + row(vec, SHIFT, c) > 0, grad, 0.0)
                dpre[span(v, half), c] = grad
                column_sums(mine, (which,), 2 * v, c, grad, grad * normed)
        tiles([functools.partial(w_tile, w_src), functools.partial(n_tile, n_src)], body)

    def norm_grad(n_src, vec, sums):
        def body(i, c):
            for v in TWO:
                part = span(v, half)
                mean, slope = row(sums, 2 * v, c) / rows_total, row(sums, 2 * v + 1, c) / rows_total
                grad = row(vec, GAIN, c) * row(vec, INV + v, c) * (
                    dpre[part, c] - (mean + normed_tile(i, c, v, vec) * slope))
                d[part, c] = grad.astype(BF16)
            pair_copy(i).start()
        tiles([functools.partial(n_tile, n_src)], body)

    def load(src, dst, k):
        return pltpu.make_async_copy(src, dst, load_sem.at[k])

    def dz_tile(n):
        return pltpu.make_async_copy(dz.at[:, cols(n)], d.at[:, cols(n)], tile_sem.at[n])

    heads = (0, TILES // 2)
    passed = [pair_copy(n, dz) for i in range(1, TILES // 2) for n in (i, TILES // 2 + i)]

    def dz_arrived(n):
        dz_tile(n).wait()
        pair_copy(n).wait_recv()

    blk3, blk1 = gw3.shape[0], gw1.shape[0]

    def operand(src, pair):
        return [load(pair, xt.at[span(1, rows)], len(ORDER))] + [
            load(src.at[:, span(me ^ mask, blk3)], xt.at[span(0, rows), pl.ds(j * blk3, blk3)], j)
            for j, mask in enumerate(ORDER)]

    def lhs_x(k, part, right):
        return dot(xt[span(k, rows), part], right, TURN_LEFT)

    def lhs_h(k, part, right):
        return dot(ht[part, span(k, rows)], right)

    prod3 = Product(0, lhs_x, acc3, near3, far3, gw3)
    prod2 = Product(1, lhs_x, acc2, near2, far2, gw2)
    prod1 = Product(2, lhs_h, acc1, near1, far1, gw1)
    first = run(operand(x2, x2_pair))
    run([pltpu.make_async_copy(dz_pair.at[:, cols(k)], pd.at[:, cols(n)], pair_recv.at[n]) for k, n in enumerate(heads)])
    both_colours(lambda n, colour: dz_tile(n).start())
    all_entered()
    run(passed)
    finish_all(first)
    everything = ([(0, len(ORDER))],) * 2
    prod3.compute(([(1, 2)], [(2, 2)]), dz_arrived, True)
    back_product(w3, u2, vec2, 0)
    send_sums(0)
    prod3.compute(([(0, 1), (3, 1)], [(0, 2)]), None, False)
    for copy in passed:
        copy.wait_send()
    pass_sums(0)
    second = run(operand(x1, x1_pair))
    views = list(enumerate((h_a, h_b)))
    own_h = run([load(src, hv.at[span(v, half)], len(ORDER) + 1 + v) for v, src in views])
    pair_h = run([remote(src, hv.at[span(2 + v, half)], h_send.at[v], h_recv.at[v], PAIR) for v, src in views])
    prod3.relay()
    sums2[...] = take_sums(0)
    norm_grad(u2, vec2, sums2)
    finish_all(second)
    prod2.compute(everything, lambda n: pair_copy(n).wait(), True)
    pl.semaphore_signal(free_sem, inc=1, device_id=(me ^ PAIR,), device_id_type=MESH)
    back_product(w2, u1, vec1, 1)
    send_sums(1)
    finish_all(own_h + pair_h)
    for k in range(2 * len(TWO)):
        hturn[:, span(k, half)] = hv[span(k, half), :].T
    for j, mask in enumerate(ORDER):
        ht[span(j, blk1), :] = hturn[span(me ^ mask, blk1), :]
    pass_sums(1)
    prod3.finish()
    prod2.relay()
    sums1[...] = take_sums(1)
    pl.semaphore_wait(free_sem, 1)
    norm_grad(u1, vec1, sums1)
    prod1.compute(everything, lambda n: pair_copy(n).wait(), True)
    prod1.relay()
    prod2.finish()
    prod1.finish()
    for product in (prod3, prod2, prod1):
        product.drain()


ANYWHERE, ON_CHIP = pl.BlockSpec(memory_space=pl.ANY), pl.BlockSpec(memory_space=pltpu.VMEM)
SCALARS = pl.BlockSpec(memory_space=pltpu.SMEM)


def params(cid):
    return pltpu.CompilerParams(collective_id=cid, has_side_effects=True, vmem_limit_bytes=VMEM_BYTES)


def backward(rows_total, dz, *rest, cid):
    h_a = rest[5]
    rows, feats = dz.shape
    blk3, blk1 = feats // DEVICES, h_a.shape[1] // DEVICES
    groups = len(ORDER)
    blocks = (blk3, blk3, blk1)

    def per_weight(parts):
        return [pltpu.VMEM((TILES, parts * b, TILE), F32) for b in blocks]

    sums = jax.ShapeDtypeStruct((2 * len(TWO), feats), F32)
    half_sums = (2 * len(TWO), feats // 2)
    return pl.pallas_call(
        functools.partial(backward_kernel, rows_total),
        out_shape=[jax.ShapeDtypeStruct((b, feats), F32) for b in blocks] + [sums, sums],
        in_specs=[ANYWHERE] * (len(rest) - 1) + [ON_CHIP] * 2,
        out_specs=[ANYWHERE] * WEIGHTS + [ON_CHIP] * 2,
        scratch_shapes=[pltpu.VMEM((rows, feats), BF16), pltpu.VMEM((rows, feats), BF16),
                        pltpu.VMEM((2 * rows, groups * blk3), BF16), pltpu.VMEM((2 * rows, h_a.shape[1]), BF16),
                        pltpu.VMEM((h_a.shape[1], 2 * rows), BF16), pltpu.VMEM((groups * blk1, 2 * rows), BF16),
                        pltpu.VMEM((rows, feats), F32),
                        pltpu.VMEM((2, TILE, feats), BF16), pltpu.VMEM((2, rows, TILE), F32)]
        + per_weight(groups) + per_weight(2) + per_weight(1)
        + [pltpu.VMEM(shape, F32) for shape in ((2,) + sums.shape, (2,) + half_sums, (2, DEVICES // 2) + half_sums,
                                                (2,) + sums.shape)]
        + [DMA((DEVICES,)), DMA((TILES,))]
        + [DMA((TILES,))] * 2 + [DMA((WEIGHTS, TILES))] * 4 + [DMA((2, DEVICES))] * 2 + [DMA((2,))] * 2
        + [DMA((WEIGHTS, TILES))] + [DMA((2,))] * 2 + [pltpu.SemaphoreType.REGULAR],
        compiler_params=params(cid),
        name="backward",
    )(dz, *rest)


def forward_kernel(rows_total, lam, h_a, h_b, w1, w2, w3, gain1, shift1, gain2, shift2,
                   loss, u1, u2, x1, x2, x1_pair, x2_pair, dz, dz_pair, vec1, vec2,
                   hv, ubuf, vbuf, w2buf, w3buf, xbuf, zh, za, zb, corr, mine, slots, vec3, loss_mine, loss_slots,
                   load_sem, store_sem, pair_send, pair_recv, sum_send, sum_recv, za_send, za_recv, zb_send, zb_recv,
                   g_send, g_recv, loss_send, loss_recv, dz_sem, dz_send, dz_recv):
    me = lax.axis_index("data")
    half = hv.shape[0] // 2
    feats = w2buf.shape[0]
    rblk, cblk = za.shape[2], zb.shape[2]
    greet()

    def load(src, dst, k):
        return pltpu.make_async_copy(src, dst, load_sem.at[k])

    w1_view = w3buf.at[pl.ds(0, w1.shape[0])]
    loads = run([load(h_a, hv.at[span(0, half)], 0), load(h_b, hv.at[span(1, half)], 1), load(w1, w1_view, 2)])
    all_entered()
    send_sums, take_sums = exchange(mine, slots, sum_send, sum_recv)
    send_loss, take_loss = exchange(loss_mine, loss_slots, loss_send, loss_recv)

    def each_tile(body):
        def step(n, carry):
            body(n, cols(n))
            return carry
        lax.fori_loop(0, TILES, step, 0)

    def take_vectors(e, v, vec):
        total = take_sums(e) / rows_total
        mean = total[:1]
        vec[pl.ds(MEAN + v, 1), :] = mean
        vec[pl.ds(INV + v, 1), :] = lax.rsqrt(total[1:] - mean * mean + NORM_EPS)

    def layer(e, v, left, weight, out):
        part = span(v, half)

        def body(n, c):
            value = dot(left[part, :], weight[:, c])
            out[part, c] = value
            column_sums(mine, (e,), 0, c, value, value * value)
        each_tile(body)
        send_sums(e)

    def normed_tile(values, v, c, vec):
        return (values[span(v, half), c] - row(vec, MEAN + v, c)) * row(vec, INV + v, c)

    def activate(v, values, vec):
        def body(n, c):
            pre = row(vec, GAIN, c) * normed_tile(values, v, c, vec) + row(vec, SHIFT, c)
            xbuf[span(v, half), c] = jnp.maximum(pre, 0.0).astype(BF16)
        each_tile(body)

    def store(src, dst, k):
        return pltpu.make_async_copy(src, dst, store_sem.at[k])

    def keep_rows(dst, pair, index):
        blk = feats // DEVICES
        return run([store(xbuf, dst, 2)] + [
            remote(xbuf.at[:, span(me ^ mask ^ PAIR, blk)], pair.at[:, pl.ds(j * blk, blk)],
                   pair_send.at[index, j], pair_recv.at[index, j], PAIR) for j, mask in enumerate(ORDER)])

    for vec, gain, shift in ((vec1, gain1, shift1), (vec2, gain2, shift2)):
        vec[pl.ds(GAIN, 1), :] = gain[...]
        vec[pl.ds(SHIFT, 1), :] = shift[...]
    finish_all(loads)
    load_w2 = load(w2, w2buf, 0)
    load_w2.start()
    for v in TWO:
        layer(v, v, hv, w1_view, ubuf)
    load_w3 = load(w3, w3buf, 2)
    store_u1 = store(ubuf, u1, 0)
    run([load_w3, store_u1])
    kept = []
    for v in TWO:
        take_vectors(v, v, vec1)
        activate(v, ubuf, vec1)
        if v:
            kept = keep_rows(x1, x1_pair, 0)
        else:
            load_w2.wait()
        layer(2 + v, v, xbuf, w2buf, vbuf)
    store_u2 = store(vbuf, u2, 1)
    store_u2.start()
    finish_all([store_u1, load_w3] + kept)
    for v in TWO:
        take_vectors(2 + v, v, vec2)
        activate(v, vbuf, vec2)
        if v:
            kept = keep_rows(x2, x2_pair, 1)
        layer(4 + v, v, xbuf, w3buf, ubuf)

    def embed(v):
        take_vectors(4 + v, v, vec3)

        def body(n, c):
            zh[span(v, half), c] = normed_tile(ubuf, v, c, vec3).astype(BF16)
        each_tile(body)

    def row_index(mask):
        dev = me ^ mask
        return dev // 4 * 2 + dev % 2

    def row_block(mask):
        return span(row_index(mask), rblk)

    def col_block(mask):
        return span((me ^ mask) // 2 % 2, cblk)

    quarter = half // 2
    started = []

    def go(copy):
        copy.start()
        started.append(copy)

    def za_direct(mask):
        return remote(zh.at[span(0, half), row_block(mask)], za.at[me], za_send.at[mask], za_recv.at[mask], mask)

    def za_relay(origin):
        slot = za.at[me ^ origin]
        return remote(slot, slot, za_send.at[origin ^ XN], za_recv.at[origin ^ XN], XN)

    def zb_slot(origin, k):
        return zb.at[me ^ origin, span(k, quarter)]

    def zb_direct(mask, k):
        return remote(zh.at[span(2 + k, quarter), col_block(mask)], zb_slot(OWN, k),
                      zb_send.at[mask, k], zb_recv.at[mask, k], mask)

    def zb_relay(origin, mask, k, send):
        return remote(zb_slot(origin, k), zb_slot(origin, k), zb_send.at[send, k], zb_recv.at[origin ^ mask, k], mask)

    def za_arrived(origin):
        slot = za.at[me ^ origin]
        remote(slot, slot, za_send.at[OWN], za_recv.at[origin], PAIR).wait_recv()

    def zb_arrived(origin, ks=TWO):
        for k in ks:
            zb_relay(origin, OWN, k, OWN).wait_recv()

    def accumulate(origin):
        corr[...] = corr[...] + dot(za[me ^ origin], zb[me ^ origin], TURN_LEFT)

    embed(0)
    for mask in (YN, XN, YP, XP, PAIR):
        go(za_direct(mask))
    embed(1)
    for k in TWO:
        for mask in (XN, YN, PAIR):
            go(zb_direct(mask, k))
    corr[...] = dot(zh[span(0, half), row_block(OWN)], zh[span(1, half), col_block(OWN)], TURN_LEFT)
    za_arrived(PAIR)
    zb_arrived(PAIR)
    accumulate(PAIR)
    for origin in (YN, YP):
        za_arrived(origin)
        go(za_relay(origin))
    for k in TWO:
        zb_arrived(XN, (k,))
        go(zb_relay(XN, YN, k, XP))
        go(zb_relay(XN, PAIR, k, YP))
        zb_arrived(YN, (k,))
        go(zb_relay(YN, PAIR, k, DG))
    za_arrived(XN)
    accumulate(XN)
    accumulate(YN)
    za_arrived(XP)
    for origin in (XP, YP):
        zb_arrived(origin)
        accumulate(origin)
    for k in TWO:
        zb_arrived(DG, (k,))
        go(zb_relay(DG, PAIR, k, DP))
    za_arrived(DG)
    accumulate(DG)
    za_arrived(DP)
    zb_arrived(DP)
    accumulate(DP)

    lam_off = lam[0]
    row_start, col_start = row_index(OWN) * rblk, me // 2 % 2 * cblk

    pieces = g_send.shape[1]
    piece = rblk // pieces

    def g_slot(origin, k):
        return w2buf.at[span(row_index(origin) * pieces + k, piece), col_block(origin)]

    def g_copy(origin, mask, k, send):
        return remote(g_slot(origin, k), g_slot(origin, k), g_send.at[send, k], g_recv.at[origin ^ mask, k], mask)

    def g_arrived(origin, ks):
        for k in ks:
            g_copy(origin, OWN, k, OWN).wait_recv()

    def grad_piece(k):
        value = corr[span(k, piece), :] / rows_total
        row_ids = row_start + k * piece + lax.broadcasted_iota(jnp.int32, value.shape, 0)
        col_ids = col_start + lax.broadcasted_iota(jnp.int32, value.shape, 1)
        diag = row_ids == col_ids
        gap = 1.0 - value
        terms = jnp.where(diag, gap * gap, lam_off * value * value)
        grad = jnp.where(diag, -2.0 * gap, 2.0 * lam_off * value) / rows_total
        w2buf[span(row_index(OWN) * pieces + k, piece), col_block(OWN)] = grad.astype(BF16)
        return jnp.sum(terms, axis=0, keepdims=True)

    every = range(pieces)
    even, odd = every[::2], every[1::2]
    loss_row = jnp.zeros((1, cblk), F32)
    for k in every:
        loss_row = loss_row + grad_piece(k)
        go(g_copy(OWN, *((YN, k, XN) if k in odd else (XN, k, PAIR))))
    for k, j in zip(odd, even):
        go(g_copy(OWN, XN, k, PAIR))
        go(g_copy(OWN, YN, j, XN))

    def contribute(origin, k, count):
        part = span(row_index(origin) * (pieces // count) + k // count, count * piece)
        block = w2buf[part, col_block(origin)]
        first = dot(zh[span(1, half), col_block(origin)], block, TURN_RIGHT)
        where_a, where_b = (span(0, half), part), (span(1, half), col_block(origin))
        vbuf[where_a] = vbuf[where_a] + first if origin & XN else first
        second = dot(zh[span(0, half), part], block)
        vbuf[where_b] = second if origin in (OWN, XN) and not k else vbuf[where_b] + second

    for k in every:
        go(g_copy(OWN, PAIR, k, XP))
    loss_mine[0] = jnp.broadcast_to(jnp.sum(loss_row, axis=1, keepdims=True), loss_mine.shape[1:])
    send_loss(0)
    store_u2.wait()
    contribute(OWN, 0, pieces)
    g_arrived(PAIR, every)
    contribute(PAIR, 0, pieces)
    for k, j in zip(even, odd):
        g_arrived(XN, (k,))
        go(g_copy(XN, YN, k, YN))
        go(g_copy(XN, PAIR, k, YP))
        g_arrived(YN, (j,))
        go(g_copy(YN, XN, j, YN))
        go(g_copy(YN, PAIR, j, DG))
    for k, j in zip(odd, even):
        g_arrived(XN, (k,))
        go(g_copy(XN, PAIR, k, YP))
        g_arrived(YN, (j,))
        go(g_copy(YN, PAIR, j, DG))
    contribute(YN, 0, pieces)
    contribute(XN, 0, pieces)
    for origin in (YP, XP):
        g_arrived(origin, every)
        contribute(origin, 0, pieces)
    def dz_columns(v, late):
        first = me // 2 % 2 if v else me // 4
        return span(1 - first if late else first, cblk)

    def dz_sum_copy(v, late, mask):
        e, c = DG + v, dz_columns(v, late)
        k = DEVICES + v if late else e
        return remote(mine.at[e, :, c], slots.at[e, me, :, c], sum_send.at[k, mask], sum_recv.at[k, mask], mask)

    def dz_sums(late):
        for v in TWO:
            def body(t, carry, v=v):
                start = dz_columns(v, late).start + t * TILE
                c = pl.ds(pl.multiple_of(start, TILE), TILE)
                grad = vbuf[span(v, half), c]
                column_sums(mine, (DG + v,), 0, c, grad, grad * normed_tile(ubuf, v, c, vec3))
                return carry
            lax.fori_loop(0, cblk // TILE, body, 0)
            run([dz_sum_copy(v, late, mask) for mask in FAR_FIRST])

    dz_sums(False)
    for k in even:
        now = (k, k + 1)
        for j in now:
            g_arrived(DG, (j,))
            go(g_copy(DG, PAIR, j, DP))
        contribute(DG, k, len(now))
        g_arrived(DP, now)
        contribute(DP, k, len(now))

    dz_sums(True)
    finish_all(kept)
    loss[...] = take_loss(0)
    for v in TWO:
        slots[DG + v, me] = mine[DG + v]
    for v in TWO:
        finish_all([dz_sum_copy(v, late, mask) for late in (False, True) for mask in FAR_FIRST])
        mine[DG + v] = functools.reduce(jnp.add, [slots[DG + v, k] for k in range(DEVICES)]) / rows_total

    def dz_copy(n):
        return pltpu.make_async_copy(xbuf.at[:, cols(n)], dz.at[:, cols(n)], dz_sem.at[n])

    def dz_tile(n):
        c = cols(n)
        for v in TWO:
            sums = mine[DG + v, :, c]
            grad = row(vec3, INV + v, c) * (
                vbuf[span(v, half), c] - (sums[:1] + normed_tile(ubuf, v, c, vec3) * sums[1:]))
            xbuf[span(v, half), c] = grad.astype(BF16)
        dz_copy(n).start()

    heads = (0, TILES // 2)
    for k, n in enumerate(heads):
        dz_tile(n)
        go(remote(xbuf.at[:, cols(n)], dz_pair.at[:, cols(k)], dz_send.at[k], dz_recv.at[k], PAIR))

    def dz_body(i, carry):
        for n in heads:
            dz_tile(n + i)
        return carry
    lax.fori_loop(1, TILES // 2, dz_body, 0)
    for copy in started:
        copy.wait_send()
    for copy in started[-len(heads):]:
        copy.wait_recv()
    each_tile(lambda n, c: dz_copy(n).wait())


def forward(rows_total, lam, h_a, h_b, w1, w2, w3, *vectors, cid):
    half, depth = h_a.shape
    feats = w2.shape[0]
    full, pair, vec = (2 * half, feats), (2 * half, feats // 2), (VEC_ROWS, feats)
    small = (DEVICES, 128)
    outs = [(small, F32), (full, F32), (full, F32), (full, BF16), (full, BF16), (pair, BF16), (pair, BF16), (full, BF16), ((2 * half, 2 * TILE), BF16),
            (vec, F32), (vec, F32)]
    scratch = [((2 * half, depth), BF16), (full, F32), (full, F32), ((feats, feats), BF16), ((feats, feats), BF16),
               (full, BF16), (full, BF16), ((DEVICES, half, feats // 4), BF16), ((DEVICES, half, feats // 2), BF16),
               ((feats // 4, feats // 2), F32), ((DEVICES, 2, feats), F32), ((DEVICES, DEVICES, 2, feats), F32),
               (vec, F32), ((1,) + small, F32), ((1, DEVICES) + small, F32)]
    return pl.pallas_call(
        functools.partial(forward_kernel, rows_total),
        out_shape=[jax.ShapeDtypeStruct(*out) for out in outs],
        in_specs=[SCALARS] + [ANYWHERE] * 5 + [ON_CHIP] * len(vectors),
        out_specs=[ON_CHIP] + [ANYWHERE] * (len(outs) - WEIGHTS) + [ON_CHIP] * 2,
        scratch_shapes=[pltpu.VMEM(*item) for item in scratch]
        + [DMA((WEIGHTS,))] * 2 + [DMA((2, len(ORDER)))] * 2 + [DMA((DEVICES + 2, DEVICES))] * 2 + [DMA((DEVICES,))] * 2
        + [DMA((DEVICES, 2))] * 2 + [DMA((DEVICES, 4))] * 2 + [DMA((1, DEVICES))] * 2 + [DMA((TILES,))] + [DMA((2,))] * 2,
        compiler_params=params(cid),
        name="forward",
    )(lam, h_a, h_b, w1, w2, w3, *vectors)


def emit_kernel(gw3, gw2, gw1, sums2, sums1, loss, loss_out, out3, out2, out1, gain1, shift1, gain2, shift2, buf, in_sem, out_sem):
    step = gw1.shape[0]
    pieces = [(src, dst, k) for src, dst in ((gw3, out3), (gw2, out2), (gw1, out1)) for k in range(src.shape[0] // step)]
    ins = run([pltpu.make_async_copy(src.at[span(k, step)], buf.at[i], in_sem.at[i])
               for i, (src, dst, k) in enumerate(pieces)])
    outs = [pltpu.make_async_copy(buf.at[i], dst.at[span(k, step)], out_sem.at[i])
            for i, (src, dst, k) in enumerate(pieces)]
    for sums, gain, shift in ((sums1, gain1, shift1), (sums2, gain2, shift2)):
        both = sums[:2, :] + sums[2:, :]
        shift[...] = both[:1]
        gain[...] = both[1:]
    loss_out[0, 0] = loss[0, 0]
    for before, after in zip(ins, outs):
        before.wait()
        after.start()
    finish_all(outs)


def emit(gw3, gw2, gw1, sums2, sums1, loss):
    weights = (gw3, gw2, gw1)
    step, feats = gw1.shape
    count = sum(g.shape[0] for g in weights) // step
    return pl.pallas_call(
        emit_kernel,
        out_shape=[jax.ShapeDtypeStruct((1, 1), F32)] + [jax.ShapeDtypeStruct(g.shape, F32) for g in weights]
        + [jax.ShapeDtypeStruct((1, feats), F32)] * 4,
        in_specs=[ANYWHERE] * WEIGHTS + [ON_CHIP] * 2 + [SCALARS],
        out_specs=[SCALARS] + [ANYWHERE] * WEIGHTS + [ON_CHIP] * 4,
        scratch_shapes=[pltpu.VMEM((count, step, feats), F32)] + [DMA((count,))] * 2,
        name="emit",
    )(*weights, sums2, sums1, loss)


def solution(mesh):
    shards = mesh.shape["data"]

    def local_step(h_a, h_b, w_one, w_two, w_three, gain_one, shift_one, gain_two, shift_two, lam_off):
        total_rows = h_a.shape[0] * shards
        loss, u1, u2, x1, x2, x1_pair, x2_pair, dz, dz_pair, vec1, vec2 = forward(
            total_rows, lam_off.reshape(1), h_a, h_b, w_one, w_two, w_three,
            *[v[None] for v in (gain_one, shift_one, gain_two, shift_two)], cid=0)
        grads = backward(total_rows, dz, dz_pair, x2, x2_pair, x1, x1_pair, h_a, h_b, w_three, w_two, u2, u1, vec2, vec1,
                         cid=1)
        loss, grad_w_three, grad_w_two, grad_w_one, *rest = emit(*grads, loss)
        return (loss.reshape(()), grad_w_one, grad_w_two, grad_w_three, *[v[0] for v in rest])

    row_spec = P("data", None)
    whole_mat = P(None, None)
    whole_vec = P(None)
    return jax.shard_map(
        local_step, mesh=mesh,
        in_specs=(row_spec, row_spec, whole_mat, whole_mat, whole_mat,
                  whole_vec, whole_vec, whole_vec, whole_vec, P()),
        out_specs=(P(), row_spec, row_spec, row_spec, whole_vec, whole_vec, whole_vec, whole_vec),
        check_vma=False)
```

```python
import functools

import jax
import jax.numpy as jnp
from jax import lax
from jax.experimental import pallas as pl
from jax.experimental.pallas import tpu as pltpu
from jax.sharding import PartitionSpec as P

NORM_EPS = 1e-5
MESH = pl.DeviceIdType.MESH
DEVICES = 8
OWN, PAIR, XN, XP, YN, YP, DG, DP = range(DEVICES)
FAR_FIRST = (DG, DP, XN, XP, YN, YP, PAIR)
ORDER = (OWN, XN, DG, YN)
TWO = range(2)
TILE = 256
TILES = 8
WEIGHTS = 3
GAIN, SHIFT, INV, MEAN, VEC_ROWS = 0, 1, 2, 4, 6
VMEM_BYTES = 67043328
TURN_LEFT = (((0,), (0,)), ((), ()))
TURN_RIGHT = (((1,), (1,)), ((), ()))
F32, BF16 = jnp.float32, jnp.bfloat16
DMA = pltpu.SemaphoreType.DMA


def dot(left, right, dims=None):
    if dims is None:
        return jnp.dot(left, right, preferred_element_type=F32)
    return lax.dot_general(left, right, dims, preferred_element_type=F32)


def span(index, size):
    return pl.ds(pl.multiple_of(index * size, size), size)


def cols(n):
    return span(n, TILE)


def row(ref, r, c):
    return ref[r:r + 1, c]


def remote(src, dst, send, recv, mask):
    return pltpu.make_async_remote_copy(src_ref=src, dst_ref=dst, send_sem=send, recv_sem=recv,
                                        device_id=(lax.axis_index("data") ^ mask,), device_id_type=MESH)


def greet():
    for mask in FAR_FIRST:
        pl.semaphore_signal(pltpu.get_barrier_semaphore(), inc=1, device_id=(lax.axis_index("data") ^ mask,),
                            device_id_type=MESH)


def all_entered():
    pl.semaphore_wait(pltpu.get_barrier_semaphore(), len(FAR_FIRST))


def column_sums(ref, lead, r, c, first, second):
    ref[lead + (slice(r, r + 1), c)] = jnp.sum(first, axis=0, keepdims=True)
    ref[lead + (slice(r + 1, r + 2), c)] = jnp.sum(second, axis=0, keepdims=True)


def exchange(mine, slots, send, recv):
    me = lax.axis_index("data")

    def copy(e, mask):
        return remote(mine.at[e], slots.at[e, me], send.at[e, mask], recv.at[e, mask], mask)

    def start(e):
        for mask in FAR_FIRST:
            copy(e, mask).start()
        slots[e, me] = mine[e]

    def take(e):
        for mask in FAR_FIRST:
            copy(e, mask).wait()
        return functools.reduce(jnp.add, [slots[e, k] for k in range(DEVICES)])
    return start, take


def exchange_halves(mine, mate, chips, whole, send, recv):
    me = lax.axis_index("data")
    width = mate.shape[-1]
    core, chip = me % 2, me // 2
    others = (DG, XN, YN)

    def pair_copy(e):
        return remote(mine.at[e, :, span(1 - core, width)], mate.at[e], send.at[e, OWN], recv.at[e, OWN], PAIR)

    def chip_copy(e, mask):
        return remote(chips.at[e, chip], chips.at[e, chip], send.at[e, mask], recv.at[e, mask], mask)

    def share(e):
        half = whole.at[e, :, span(core, width)]
        return remote(half, half, send.at[e, PAIR], recv.at[e, PAIR], PAIR)

    def start(e):
        pair_copy(e).start()

    def middle(e):
        pair_copy(e).wait()
        chips[e, chip] = mine[e, :, span(core, width)] + mate[e]
        for mask in others:
            chip_copy(e, mask).start()

    def take(e):
        for mask in others:
            chip_copy(e, mask).wait()
        whole[e, :, span(core, width)] = functools.reduce(jnp.add, [chips[e, k] for k in range(DEVICES // 2)])
        share(e).start()
        share(e).wait()
    return start, middle, take


def run(copies):
    for copy in copies:
        copy.start()
    return copies


def finish_all(copies):
    for copy in copies:
        copy.wait()


def backward_kernel(rows_total, dz, dz_pair, x2, x2_pair, x1, x1_pair, h_a, h_b, w3, w2, u2, u1, vec2_hbm, vec1_hbm,
                    gw3, gw2, gw1, sums2, sums1,
                    vec2, vec1, d, pd, xt, hv, hturn, ht, dpre, wbuf, nbuf, acc3, acc2, acc1, near3, near2, near1, far3, far2, far1,
                    mine, mate, chips, whole, vec_sem, load_sem, tile_sem, pair_send, pair_recv, hop_send, hop_recv, far_send, far_recv,
                    sum_send, sum_recv, h_send, h_recv, out_sem, w_sem, n_sem, free_sem):
    me = lax.axis_index("data")
    rows = d.shape[0]
    half = rows // 2
    greet()

    def small(src, dst, k):
        return pltpu.make_async_copy(src, dst, vec_sem.at[k])

    vectors_in = [small(vec2_hbm, vec2, 0), small(vec1_hbm, vec1, 1)]
    send_sums, pass_sums, take_sums = exchange_halves(mine, mate, chips, whole, sum_send, sum_recv)

    def pair_copy(n, src=d):
        return remote(src.at[:, cols(n)], pd.at[:, cols(n)], pair_send.at[n], pair_recv.at[n], PAIR)

    def both_colours(body):
        def step(i, carry):
            for colour in TWO:
                body(colour * (TILES // 2) + i, colour)
            return carry
        lax.fori_loop(0, TILES // 2, step, 0)

    class Product:
        def __init__(self, w, lhs, acc, near, far, out):
            self.w, self.lhs, self.acc, self.near, self.far, self.out = w, lhs, acc, near, far, out
            self.blk = out.shape[0]

        def block(self, j, count=1):
            return pl.ds(j * self.blk, count * self.blk)

        def first_hop(self, n, colour):
            return remote(self.acc.at[n, self.block(1 + colour, 2)], self.near.at[n],
                          hop_send.at[self.w, n], hop_recv.at[self.w, n], YN if colour else XN)

        def second_hop(self, n, colour):
            return remote(self.acc.at[n, self.block(1 if colour else 3)], self.far.at[n],
                          far_send.at[self.w, n], far_recv.at[self.w, n], XN if colour else YN)

        def out_copy(self, n):
            return pltpu.make_async_copy(self.acc.at[n, self.block(0)], self.out.at[:, cols(n)], out_sem.at[self.w, n])

        def fill(self, n, part):
            self.acc[n, part] = self.lhs(0, part, d[:, cols(n)]) + self.lhs(1, part, pd[:, cols(n)])

        def compute(self, parts, arrive, send):
            def body(n, colour):
                if arrive:
                    arrive(n)
                for j, count in parts[colour]:
                    self.fill(n, self.block(j, count))
                if send:
                    self.first_hop(n, colour).start()
            both_colours(body)

        def relay(self):
            def body(n, colour):
                onward, own = self.block(1 if colour else 3), self.block(0)
                self.first_hop(n, colour).wait_recv()
                self.acc[n, onward] = self.acc[n, onward] + self.near[n, self.block(1 - colour)]
                self.second_hop(n, colour).start()
                self.acc[n, own] = self.acc[n, own] + self.near[n, self.block(colour)]
            both_colours(body)

        def finish(self):
            def body(n, colour):
                own = self.block(0)
                self.second_hop(n, colour).wait_recv()
                self.acc[n, own] = self.acc[n, own] + self.far[n]
                self.out_copy(n).start()
            both_colours(body)

        def drain(self):
            def body(n, colour):
                self.first_hop(n, colour).wait_send()
                self.second_hop(n, colour).wait_send()
                self.out_copy(n).wait()
            both_colours(body)

    def w_tile(src, i):
        return pltpu.make_async_copy(src.at[cols(i)], wbuf.at[i % 2], w_sem.at[i % 2])

    def n_tile(src, i):
        return pltpu.make_async_copy(src.at[:, cols(i)], nbuf.at[i % 2], n_sem.at[i % 2])

    def tiles(streams, body):
        run([s(0) for s in streams])

        def step(i, carry):
            @pl.when(i < TILES - 1)
            def _():
                run([s(i + 1) for s in streams])
            finish_all([s(i) for s in streams])
            body(i, cols(i))
            return carry
        lax.fori_loop(0, TILES, step, 0)

    def normed_tile(i, c, v, vec):
        return (nbuf[i % 2, span(v, half), :] - row(vec, MEAN + v, c)) * row(vec, INV + v, c)

    def back_product(w_src, n_src, vec, which):
        def body(i, c):
            for v in TWO:
                grad = dot(d[span(v, half), :], wbuf[i % 2], TURN_RIGHT)
                normed = normed_tile(i, c, v, vec)
                grad = jnp.where(row(vec, GAIN, c) * normed + row(vec, SHIFT, c) > 0, grad, 0.0)
                dpre[span(v, half), c] = grad
                column_sums(mine, (which,), 2 * v, c, grad, grad * normed)
        tiles([functools.partial(w_tile, w_src), functools.partial(n_tile, n_src)], body)

    def norm_grad(n_src, vec, sums):
        def body(i, c):
            for v in TWO:
                part = span(v, half)
                mean, slope = row(sums, 2 * v, c) / rows_total, row(sums, 2 * v + 1, c) / rows_total
                grad = row(vec, GAIN, c) * row(vec, INV + v, c) * (
                    dpre[part, c] - (mean + normed_tile(i, c, v, vec) * slope))
                d[part, c] = grad.astype(BF16)
            pair_copy(i).start()
        tiles([functools.partial(n_tile, n_src)], body)

    def load(src, dst, k):
        return pltpu.make_async_copy(src, dst, load_sem.at[k])

    def dz_tile(n):
        return pltpu.make_async_copy(dz.at[:, cols(n)], d.at[:, cols(n)], tile_sem.at[n])

    heads = (0, TILES // 2)
    passed = [pair_copy(n, dz) for i in range(1, TILES // 2) for n in (i, TILES // 2 + i)]

    def dz_arrived(n):
        dz_tile(n).wait()
        pair_copy(n).wait_recv()

    blk3, blk1 = gw3.shape[0], gw1.shape[0]

    def operand(src, pair):
        return [load(pair, xt.at[span(1, rows)], len(ORDER))] + [
            load(src.at[:, span(me ^ mask, blk3)], xt.at[span(0, rows), pl.ds(j * blk3, blk3)], j)
            for j, mask in enumerate(ORDER)]

    def lhs_x(k, part, right):
        return dot(xt[span(k, rows), part], right, TURN_LEFT)

    def lhs_h(k, part, right):
        return dot(ht[part, span(k, rows)], right)

    prod3 = Product(0, lhs_x, acc3, near3, far3, gw3)
    prod2 = Product(1, lhs_x, acc2, near2, far2, gw2)
    prod1 = Product(2, lhs_h, acc1, near1, far1, gw1)
    first = run(operand(x2, x2_pair))
    run([pltpu.make_async_copy(dz_pair.at[:, cols(k)], pd.at[:, cols(n)], pair_recv.at[n]) for k, n in enumerate(heads)])
    both_colours(lambda n, colour: dz_tile(n).start())
    run(vectors_in)
    all_entered()
    run(passed)
    finish_all(first + vectors_in)
    everything = ([(0, len(ORDER))],) * 2
    prod3.compute(([(1, 2)], [(2, 2)]), dz_arrived, True)
    back_product(w3, u2, vec2, 0)
    send_sums(0)
    prod3.compute(([(0, 1), (3, 1)], [(0, 2)]), None, False)
    for copy in passed:
        copy.wait_send()
    pass_sums(0)
    second = run(operand(x1, x1_pair))
    views = list(enumerate((h_a, h_b)))
    own_h = run([load(src, hv.at[span(v, half)], len(ORDER) + 1 + v) for v, src in views])
    pair_h = run([remote(src, hv.at[span(2 + v, half)], h_send.at[v], h_recv.at[v], PAIR) for v, src in views])
    prod3.relay()
    take_sums(0)
    sums_out = run([small(whole.at[0], sums2, 2)])
    norm_grad(u2, vec2, whole.at[0])
    finish_all(second)
    prod2.compute(everything, lambda n: pair_copy(n).wait(), True)
    pl.semaphore_signal(free_sem, inc=1, device_id=(me ^ PAIR,), device_id_type=MESH)
    back_product(w2, u1, vec1, 1)
    send_sums(1)
    finish_all(own_h + pair_h)
    for k in range(2 * len(TWO)):
        hturn[:, span(k, half)] = hv[span(k, half), :].T
    for j, mask in enumerate(ORDER):
        ht[span(j, blk1), :] = hturn[span(me ^ mask, blk1), :]
    pass_sums(1)
    prod3.finish()
    prod2.relay()
    take_sums(1)
    sums_out += run([small(whole.at[1], sums1, 3)])
    pl.semaphore_wait(free_sem, 1)
    norm_grad(u1, vec1, whole.at[1])
    prod1.compute(everything, lambda n: pair_copy(n).wait(), True)
    prod1.relay()
    prod2.finish()
    prod1.finish()
    for product in (prod3, prod2, prod1):
        product.drain()
    finish_all(sums_out)


ANYWHERE = pl.BlockSpec(memory_space=pl.ANY)
SCALARS = pl.BlockSpec(memory_space=pltpu.SMEM)


def params(cid):
    return pltpu.CompilerParams(collective_id=cid, has_side_effects=True, vmem_limit_bytes=VMEM_BYTES)


def backward(rows_total, dz, *rest, cid):
    h_a = rest[5]
    rows, feats = dz.shape
    blk3, blk1 = feats // DEVICES, h_a.shape[1] // DEVICES
    groups = len(ORDER)
    blocks = (blk3, blk3, blk1)

    def per_weight(parts):
        return [pltpu.VMEM((TILES, parts * b, TILE), F32) for b in blocks]

    sums = jax.ShapeDtypeStruct((2 * len(TWO), feats), F32)
    half_sums = (2 * len(TWO), feats // 2)
    return pl.pallas_call(
        functools.partial(backward_kernel, rows_total),
        out_shape=[jax.ShapeDtypeStruct((b, feats), F32) for b in blocks] + [sums, sums],
        in_specs=[ANYWHERE] * (len(rest) + 1),
        out_specs=[ANYWHERE] * (WEIGHTS + 2),
        scratch_shapes=[pltpu.VMEM((VEC_ROWS, feats), F32)] * 2 + [pltpu.VMEM((rows, feats), BF16), pltpu.VMEM((rows, feats), BF16),
                        pltpu.VMEM((2 * rows, groups * blk3), BF16), pltpu.VMEM((2 * rows, h_a.shape[1]), BF16),
                        pltpu.VMEM((h_a.shape[1], 2 * rows), BF16), pltpu.VMEM((groups * blk1, 2 * rows), BF16),
                        pltpu.VMEM((rows, feats), F32),
                        pltpu.VMEM((2, TILE, feats), BF16), pltpu.VMEM((2, rows, TILE), F32)]
        + per_weight(groups) + per_weight(2) + per_weight(1)
        + [pltpu.VMEM(shape, F32) for shape in ((2,) + sums.shape, (2,) + half_sums, (2, DEVICES // 2) + half_sums,
                                                (2,) + sums.shape)]
        + [DMA((len(ORDER),)), DMA((DEVICES,)), DMA((TILES,))]
        + [DMA((TILES,))] * 2 + [DMA((WEIGHTS, TILES))] * 4 + [DMA((2, DEVICES))] * 2 + [DMA((2,))] * 2
        + [DMA((WEIGHTS, TILES))] + [DMA((2,))] * 2 + [pltpu.SemaphoreType.REGULAR],
        compiler_params=params(cid),
        name="backward",
    )(dz, *rest)


def forward_kernel(rows_total, lam, h_a, h_b, w1, w2, w3, gain1, shift1, gain2, shift2,
                   loss, u1, u2, x1, x2, x1_pair, x2_pair, dz, dz_pair, vec1_out, vec2_out,
                   affine, vec1, vec2, vec_sem, hv, ubuf, vbuf, w2buf, w3buf, xbuf, zh, za, zb, corr, mine, slots, vec3, loss_mine, loss_slots,
                   load_sem, store_sem, pair_send, pair_recv, sum_send, sum_recv, za_send, za_recv, zb_send, zb_recv,
                   g_send, g_recv, loss_send, loss_recv, dz_sem, dz_send, dz_recv):
    me = lax.axis_index("data")
    half = hv.shape[0] // 2
    feats = w2buf.shape[0]
    rblk, cblk = za.shape[2], zb.shape[2]
    greet()

    def load(src, dst, k):
        return pltpu.make_async_copy(src, dst, load_sem.at[k])

    w1_view = w3buf.at[pl.ds(0, w1.shape[0])]
    loads = run([load(h_a, hv.at[span(0, half)], 0), load(h_b, hv.at[span(1, half)], 1), load(w1, w1_view, 2)])
    affine_in = run([pltpu.make_async_copy(src, affine.at[k], vec_sem.at[k])
                     for k, src in enumerate((gain1, shift1, gain2, shift2))])
    all_entered()
    send_sums, take_sums = exchange(mine, slots, sum_send, sum_recv)
    send_loss, take_loss = exchange(loss_mine, loss_slots, loss_send, loss_recv)

    def each_tile(body):
        def step(n, carry):
            body(n, cols(n))
            return carry
        lax.fori_loop(0, TILES, step, 0)

    def take_vectors(e, v, vec):
        total = take_sums(e) / rows_total
        mean = total[:1]
        vec[pl.ds(MEAN + v, 1), :] = mean
        vec[pl.ds(INV + v, 1), :] = lax.rsqrt(total[1:] - mean * mean + NORM_EPS)

    def layer(e, v, left, weight, out):
        part = span(v, half)

        def body(n, c):
            value = dot(left[part, :], weight[:, c])
            out[part, c] = value
            column_sums(mine, (e,), 0, c, value, value * value)
        each_tile(body)
        send_sums(e)

    def normed_tile(values, v, c, vec):
        return (values[span(v, half), c] - row(vec, MEAN + v, c)) * row(vec, INV + v, c)

    def activate(v, values, vec):
        def body(n, c):
            pre = row(vec, GAIN, c) * normed_tile(values, v, c, vec) + row(vec, SHIFT, c)
            xbuf[span(v, half), c] = jnp.maximum(pre, 0.0).astype(BF16)
        each_tile(body)

    def store(src, dst, k):
        return pltpu.make_async_copy(src, dst, store_sem.at[k])

    def keep_rows(dst, pair, index):
        blk = feats // DEVICES
        return run([store(xbuf, dst, 2)] + [
            remote(xbuf.at[:, span(me ^ mask ^ PAIR, blk)], pair.at[:, pl.ds(j * blk, blk)],
                   pair_send.at[index, j], pair_recv.at[index, j], PAIR) for j, mask in enumerate(ORDER)])

    finish_all(loads + affine_in)
    for k, vec in enumerate((vec1, vec2)):
        vec[pl.ds(GAIN, 1), :] = affine[2 * k]
        vec[pl.ds(SHIFT, 1), :] = affine[2 * k + 1]
    load_w2 = load(w2, w2buf, 0)
    load_w2.start()
    for v in TWO:
        layer(v, v, hv, w1_view, ubuf)
    load_w3 = load(w3, w3buf, 2)
    store_u1 = store(ubuf, u1, 0)
    run([load_w3, store_u1])
    kept = []
    for v in TWO:
        take_vectors(v, v, vec1)
        activate(v, ubuf, vec1)
        if v:
            kept = keep_rows(x1, x1_pair, 0)
        else:
            load_w2.wait()
        layer(2 + v, v, xbuf, w2buf, vbuf)
    store_u2 = store(vbuf, u2, 1)
    store_u2.start()
    finish_all([store_u1, load_w3] + kept)
    for v in TWO:
        take_vectors(2 + v, v, vec2)
        activate(v, vbuf, vec2)
        if v:
            kept = keep_rows(x2, x2_pair, 1)
        layer(4 + v, v, xbuf, w3buf, ubuf)

    small_out = run([pltpu.make_async_copy(vec, out, vec_sem.at[k])
                     for k, (vec, out) in enumerate(((vec1, vec1_out), (vec2, vec2_out)))])

    def embed(v):
        take_vectors(4 + v, v, vec3)

        def body(n, c):
            zh[span(v, half), c] = normed_tile(ubuf, v, c, vec3).astype(BF16)
        each_tile(body)

    def row_index(mask):
        dev = me ^ mask
        return dev // 4 * 2 + dev % 2

    def row_block(mask):
        return span(row_index(mask), rblk)

    def col_block(mask):
        return span((me ^ mask) // 2 % 2, cblk)

    quarter = half // 2
    started = []

    def go(copy):
        copy.start()
        started.append(copy)

    def za_direct(mask):
        return remote(zh.at[span(0, half), row_block(mask)], za.at[me], za_send.at[mask], za_recv.at[mask], mask)

    def za_relay(origin):
        slot = za.at[me ^ origin]
        return remote(slot, slot, za_send.at[origin ^ XN], za_recv.at[origin ^ XN], XN)

    def zb_slot(origin, k):
        return zb.at[me ^ origin, span(k, quarter)]

    def zb_direct(mask, k):
        return remote(zh.at[span(2 + k, quarter), col_block(mask)], zb_slot(OWN, k),
                      zb_send.at[mask, k], zb_recv.at[mask, k], mask)

    def zb_relay(origin, mask, k, send):
        return remote(zb_slot(origin, k), zb_slot(origin, k), zb_send.at[send, k], zb_recv.at[origin ^ mask, k], mask)

    def za_arrived(origin):
        slot = za.at[me ^ origin]
        remote(slot, slot, za_send.at[OWN], za_recv.at[origin], PAIR).wait_recv()

    def zb_arrived(origin, ks=TWO):
        for k in ks:
            zb_relay(origin, OWN, k, OWN).wait_recv()

    def accumulate(origin):
        corr[...] = corr[...] + dot(za[me ^ origin], zb[me ^ origin], TURN_LEFT)

    embed(0)
    for mask in (YN, XN, YP, XP, PAIR):
        go(za_direct(mask))
    embed(1)
    for k in TWO:
        for mask in (XN, YN, PAIR):
            go(zb_direct(mask, k))
    corr[...] = dot(zh[span(0, half), row_block(OWN)], zh[span(1, half), col_block(OWN)], TURN_LEFT)
    za_arrived(PAIR)
    zb_arrived(PAIR)
    accumulate(PAIR)
    for origin in (YN, YP):
        za_arrived(origin)
        go(za_relay(origin))
    for k in TWO:
        zb_arrived(XN, (k,))
        go(zb_relay(XN, YN, k, XP))
        go(zb_relay(XN, PAIR, k, YP))
        zb_arrived(YN, (k,))
        go(zb_relay(YN, PAIR, k, DG))
    za_arrived(XN)
    accumulate(XN)
    accumulate(YN)
    za_arrived(XP)
    for origin in (XP, YP):
        zb_arrived(origin)
        accumulate(origin)
    for k in TWO:
        zb_arrived(DG, (k,))
        go(zb_relay(DG, PAIR, k, DP))
    za_arrived(DG)
    accumulate(DG)
    za_arrived(DP)
    zb_arrived(DP)
    accumulate(DP)

    lam_off = lam[0]
    row_start, col_start = row_index(OWN) * rblk, me // 2 % 2 * cblk

    pieces = g_send.shape[1]
    piece = rblk // pieces

    def g_slot(origin, k):
        return w2buf.at[span(row_index(origin) * pieces + k, piece), col_block(origin)]

    def g_copy(origin, mask, k, send):
        return remote(g_slot(origin, k), g_slot(origin, k), g_send.at[send, k], g_recv.at[origin ^ mask, k], mask)

    def g_arrived(origin, ks):
        for k in ks:
            g_copy(origin, OWN, k, OWN).wait_recv()

    def grad_piece(k):
        value = corr[span(k, piece), :] / rows_total
        row_ids = row_start + k * piece + lax.broadcasted_iota(jnp.int32, value.shape, 0)
        col_ids = col_start + lax.broadcasted_iota(jnp.int32, value.shape, 1)
        diag = row_ids == col_ids
        gap = 1.0 - value
        terms = jnp.where(diag, gap * gap, lam_off * value * value)
        grad = jnp.where(diag, -2.0 * gap, 2.0 * lam_off * value) / rows_total
        w2buf[span(row_index(OWN) * pieces + k, piece), col_block(OWN)] = grad.astype(BF16)
        return jnp.sum(terms, axis=0, keepdims=True)

    every = range(pieces)
    even, odd = every[::2], every[1::2]
    loss_row = jnp.zeros((1, cblk), F32)
    for k in every:
        loss_row = loss_row + grad_piece(k)
        go(g_copy(OWN, *((YN, k, XN) if k in odd else (XN, k, PAIR))))
    for k, j in zip(odd, even):
        go(g_copy(OWN, XN, k, PAIR))
        go(g_copy(OWN, YN, j, XN))

    def contribute(origin, k, count):
        part = span(row_index(origin) * (pieces // count) + k // count, count * piece)
        block = w2buf[part, col_block(origin)]
        first = dot(zh[span(1, half), col_block(origin)], block, TURN_RIGHT)
        where_a, where_b = (span(0, half), part), (span(1, half), col_block(origin))
        vbuf[where_a] = vbuf[where_a] + first if origin & XN else first
        second = dot(zh[span(0, half), part], block)
        vbuf[where_b] = second if origin in (OWN, XN) and not k else vbuf[where_b] + second

    for k in every:
        go(g_copy(OWN, PAIR, k, XP))
    loss_mine[0] = jnp.broadcast_to(jnp.sum(loss_row, axis=1, keepdims=True), loss_mine.shape[1:])
    send_loss(0)
    store_u2.wait()
    contribute(OWN, 0, pieces)
    g_arrived(PAIR, every)
    contribute(PAIR, 0, pieces)
    for k, j in zip(even, odd):
        g_arrived(XN, (k,))
        go(g_copy(XN, YN, k, YN))
        go(g_copy(XN, PAIR, k, YP))
        g_arrived(YN, (j,))
        go(g_copy(YN, XN, j, YN))
        go(g_copy(YN, PAIR, j, DG))
    for k, j in zip(odd, even):
        g_arrived(XN, (k,))
        go(g_copy(XN, PAIR, k, YP))
        g_arrived(YN, (j,))
        go(g_copy(YN, PAIR, j, DG))
    contribute(YN, 0, pieces)
    contribute(XN, 0, pieces)
    for origin in (YP, XP):
        g_arrived(origin, every)
        contribute(origin, 0, pieces)
    def dz_columns(v, late):
        first = me // 2 % 2 if v else me // 4
        return span(1 - first if late else first, cblk)

    def dz_sum_copy(v, late, mask):
        e, c = DG + v, dz_columns(v, late)
        k = DEVICES + v if late else e
        return remote(mine.at[e, :, c], slots.at[e, me, :, c], sum_send.at[k, mask], sum_recv.at[k, mask], mask)

    def dz_sums(late):
        for v in TWO:
            def body(t, carry, v=v):
                start = dz_columns(v, late).start + t * TILE
                c = pl.ds(pl.multiple_of(start, TILE), TILE)
                grad = vbuf[span(v, half), c]
                column_sums(mine, (DG + v,), 0, c, grad, grad * normed_tile(ubuf, v, c, vec3))
                return carry
            lax.fori_loop(0, cblk // TILE, body, 0)
            run([dz_sum_copy(v, late, mask) for mask in FAR_FIRST])

    dz_sums(False)
    for k in even:
        now = (k, k + 1)
        for j in now:
            g_arrived(DG, (j,))
            go(g_copy(DG, PAIR, j, DP))
        contribute(DG, k, len(now))
        g_arrived(DP, now)
        contribute(DP, k, len(now))

    dz_sums(True)
    finish_all(kept)
    loss_mine[0] = take_loss(0)
    small_out += run([pltpu.make_async_copy(loss_mine.at[0], loss, vec_sem.at[2])])
    for v in TWO:
        slots[DG + v, me] = mine[DG + v]
    for v in TWO:
        finish_all([dz_sum_copy(v, late, mask) for late in (False, True) for mask in FAR_FIRST])
        mine[DG + v] = functools.reduce(jnp.add, [slots[DG + v, k] for k in range(DEVICES)]) / rows_total

    def dz_copy(n):
        return pltpu.make_async_copy(xbuf.at[:, cols(n)], dz.at[:, cols(n)], dz_sem.at[n])

    def dz_tile(n):
        c = cols(n)
        for v in TWO:
            sums = mine[DG + v, :, c]
            grad = row(vec3, INV + v, c) * (
                vbuf[span(v, half), c] - (sums[:1] + normed_tile(ubuf, v, c, vec3) * sums[1:]))
            xbuf[span(v, half), c] = grad.astype(BF16)
        dz_copy(n).start()

    heads = (0, TILES // 2)
    for k, n in enumerate(heads):
        dz_tile(n)
        go(remote(xbuf.at[:, cols(n)], dz_pair.at[:, cols(k)], dz_send.at[k], dz_recv.at[k], PAIR))

    def dz_body(i, carry):
        for n in heads:
            dz_tile(n + i)
        return carry
    lax.fori_loop(1, TILES // 2, dz_body, 0)
    for copy in started:
        copy.wait_send()
    for copy in started[-len(heads):]:
        copy.wait_recv()
    finish_all(small_out)
    each_tile(lambda n, c: dz_copy(n).wait())


def forward(rows_total, lam, h_a, h_b, w1, w2, w3, *vectors, cid):
    half, depth = h_a.shape
    feats = w2.shape[0]
    full, pair, vec = (2 * half, feats), (2 * half, feats // 2), (VEC_ROWS, feats)
    small = (DEVICES, 128)
    outs = [(small, F32), (full, F32), (full, F32), (full, BF16), (full, BF16), (pair, BF16), (pair, BF16), (full, BF16), ((2 * half, 2 * TILE), BF16),
            (vec, F32), (vec, F32)]
    scratch = [((2 * half, depth), BF16), (full, F32), (full, F32), ((feats, feats), BF16), ((feats, feats), BF16),
               (full, BF16), (full, BF16), ((DEVICES, half, feats // 4), BF16), ((DEVICES, half, feats // 2), BF16),
               ((feats // 4, feats // 2), F32), ((DEVICES, 2, feats), F32), ((DEVICES, DEVICES, 2, feats), F32),
               (vec, F32), ((1,) + small, F32), ((1, DEVICES) + small, F32)]
    return pl.pallas_call(
        functools.partial(forward_kernel, rows_total),
        out_shape=[jax.ShapeDtypeStruct(*out) for out in outs],
        in_specs=[SCALARS] + [ANYWHERE] * (5 + len(vectors)),
        out_specs=[ANYWHERE] * len(outs),
        scratch_shapes=[pltpu.VMEM((len(vectors), 1, feats), F32)] + [pltpu.VMEM(vec, F32)] * 2
        + [DMA((len(vectors),))] + [pltpu.VMEM(*item) for item in scratch]
        + [DMA((WEIGHTS,))] * 2 + [DMA((2, len(ORDER)))] * 2 + [DMA((DEVICES + 2, DEVICES))] * 2 + [DMA((DEVICES,))] * 2
        + [DMA((DEVICES, 2))] * 2 + [DMA((DEVICES, 4))] * 2 + [DMA((1, DEVICES))] * 2 + [DMA((TILES,))] + [DMA((2,))] * 2,
        compiler_params=params(cid),
        name="forward",
    )(lam, h_a, h_b, w1, w2, w3, *vectors)


def emit_kernel(gw3, gw2, gw1, sums2, sums1, loss, loss_out, out3, out2, out1, gain1, shift1, gain2, shift2,
                buf, sums, vecs, in_sem, out_sem, sum_sem, vec_sem):
    step = gw1.shape[0]
    pieces = [(src, dst, k) for src, dst in ((gw3, out3), (gw2, out2), (gw1, out1)) for k in range(src.shape[0] // step)]
    ins = run([pltpu.make_async_copy(src.at[span(k, step)], buf.at[i], in_sem.at[i])
               for i, (src, dst, k) in enumerate(pieces)])
    sums_in = run([pltpu.make_async_copy(src, sums.at[i], sum_sem.at[i]) for i, src in enumerate((sums1, sums2))])
    outs = [pltpu.make_async_copy(buf.at[i], dst.at[span(k, step)], out_sem.at[i])
            for i, (src, dst, k) in enumerate(pieces)]
    loss_out[0, 0] = loss[0, 0]
    half = len(ins) // 2
    for before, after in zip(ins[:half], outs):
        before.wait()
        after.start()
    finish_all(sums_in)
    for i in TWO:
        both = sums[i, :2, :] + sums[i, 2:, :]
        vecs[2 * i] = both[1:]
        vecs[2 * i + 1] = both[:1]
    vecs_out = run([pltpu.make_async_copy(vecs.at[i], dst, vec_sem.at[i])
                    for i, dst in enumerate((gain1, shift1, gain2, shift2))])
    for before, after in zip(ins[half:], outs[half:]):
        before.wait()
        after.start()
    finish_all(outs + vecs_out)


def emit(gw3, gw2, gw1, sums2, sums1, loss):
    weights = (gw3, gw2, gw1)
    step, feats = gw1.shape
    count = sum(g.shape[0] for g in weights) // step
    vectors = [jax.ShapeDtypeStruct((1, feats), F32)] * 4
    return pl.pallas_call(
        emit_kernel,
        out_shape=[jax.ShapeDtypeStruct((1, 1), F32)] + [jax.ShapeDtypeStruct(g.shape, F32) for g in weights] + vectors,
        in_specs=[ANYWHERE] * (WEIGHTS + 2) + [SCALARS],
        out_specs=[SCALARS] + [ANYWHERE] * (WEIGHTS + len(vectors)),
        scratch_shapes=[pltpu.VMEM((count, step, feats), F32), pltpu.VMEM((2,) + sums1.shape, F32),
                        pltpu.VMEM((len(vectors), 1, feats), F32)]
        + [DMA((count,))] * 2 + [DMA((2,)), DMA((len(vectors),))],
        name="emit",
    )(*weights, sums2, sums1, loss)


def solution(mesh):
    shards = mesh.shape["data"]

    def local_step(h_a, h_b, w_one, w_two, w_three, gain_one, shift_one, gain_two, shift_two, lam_off):
        total_rows = h_a.shape[0] * shards
        loss, u1, u2, x1, x2, x1_pair, x2_pair, dz, dz_pair, vec1, vec2 = forward(
            total_rows, lam_off.reshape(1), h_a, h_b, w_one, w_two, w_three,
            *[v[None] for v in (gain_one, shift_one, gain_two, shift_two)], cid=0)
        grads = backward(total_rows, dz, dz_pair, x2, x2_pair, x1, x1_pair, h_a, h_b, w_three, w_two, u2, u1, vec2, vec1,
                         cid=1)
        loss, grad_w_three, grad_w_two, grad_w_one, *rest = emit(*grads, loss)
        return (loss.reshape(()), grad_w_one, grad_w_two, grad_w_three, *[v[0] for v in rest])

    row_spec = P("data", None)
    whole_mat = P(None, None)
    whole_vec = P(None)
    return jax.shard_map(
        local_step, mesh=mesh,
        in_specs=(row_spec, row_spec, whole_mat, whole_mat, whole_mat,
                  whole_vec, whole_vec, whole_vec, whole_vec, P()),
        out_specs=(P(), row_spec, row_spec, row_spec, whole_vec, whole_vec, whole_vec, whole_vec),
        check_vma=False)
```

```python
import functools

import jax
import jax.numpy as jnp
from jax import lax
from jax.experimental import pallas as pl
from jax.experimental.pallas import tpu as pltpu
from jax.sharding import PartitionSpec as P

NORM_EPS = 1e-5
MESH = pl.DeviceIdType.MESH
DEVICES = 8
OWN, PAIR, XN, XP, YN, YP, DG, DP = range(DEVICES)
FAR_FIRST = (DG, DP, XN, XP, YN, YP, PAIR)
ORDER = (OWN, XN, DG, YN)
TWO = range(2)
TILE = 256
TILES = 8
WIDE = 512
WEIGHTS = 3
GAIN, SHIFT, INV, MEAN, VEC_ROWS = 0, 1, 2, 4, 6
VMEM_BYTES = 67043328
TURN_LEFT = (((0,), (0,)), ((), ()))
TURN_RIGHT = (((1,), (1,)), ((), ()))
F32, BF16 = jnp.float32, jnp.bfloat16
DMA = pltpu.SemaphoreType.DMA


def dot(left, right, dims=None):
    if dims is None:
        return jnp.dot(left, right, preferred_element_type=F32)
    return lax.dot_general(left, right, dims, preferred_element_type=F32)


def span(index, size):
    return pl.ds(pl.multiple_of(index * size, size), size)


def cols(n):
    return span(n, TILE)


def row(ref, r, c):
    return ref[r:r + 1, c]


def remote(src, dst, send, recv, mask):
    return pltpu.make_async_remote_copy(src_ref=src, dst_ref=dst, send_sem=send, recv_sem=recv,
                                        device_id=(lax.axis_index("data") ^ mask,), device_id_type=MESH)


def greet():
    for mask in FAR_FIRST:
        pl.semaphore_signal(pltpu.get_barrier_semaphore(), inc=1, device_id=(lax.axis_index("data") ^ mask,),
                            device_id_type=MESH)


def all_entered():
    pl.semaphore_wait(pltpu.get_barrier_semaphore(), len(FAR_FIRST))


def column_sums(ref, lead, r, c, first, second):
    ref[lead + (slice(r, r + 1), c)] = jnp.sum(first, axis=0, keepdims=True)
    ref[lead + (slice(r + 1, r + 2), c)] = jnp.sum(second, axis=0, keepdims=True)


def exchange(mine, slots, send, recv):
    me = lax.axis_index("data")

    def copy(e, mask):
        return remote(mine.at[e], slots.at[e, me], send.at[e, mask], recv.at[e, mask], mask)

    def start(e):
        for mask in FAR_FIRST:
            copy(e, mask).start()
        slots[e, me] = mine[e]

    def take(e):
        for mask in FAR_FIRST:
            copy(e, mask).wait()
        return functools.reduce(jnp.add, [slots[e, k] for k in range(DEVICES)])
    return start, take


def exchange_halves(mine, mate, chips, whole, send, recv):
    me = lax.axis_index("data")
    width = mate.shape[-1]
    core, chip = me % 2, me // 2
    others = (DG, XN, YN)

    def pair_copy(e):
        return remote(mine.at[e, :, span(1 - core, width)], mate.at[e], send.at[e, OWN], recv.at[e, OWN], PAIR)

    def chip_copy(e, mask):
        return remote(chips.at[e, chip], chips.at[e, chip], send.at[e, mask], recv.at[e, mask], mask)

    def share(e):
        half = whole.at[e, :, span(core, width)]
        return remote(half, half, send.at[e, PAIR], recv.at[e, PAIR], PAIR)

    def start(e):
        pair_copy(e).start()

    def middle(e):
        pair_copy(e).wait()
        chips[e, chip] = mine[e, :, span(core, width)] + mate[e]
        for mask in others:
            chip_copy(e, mask).start()

    def take(e):
        for mask in others:
            chip_copy(e, mask).wait()
        whole[e, :, span(core, width)] = functools.reduce(jnp.add, [chips[e, k] for k in range(DEVICES // 2)])
        share(e).start()
        share(e).wait()
    return start, middle, take


def run(copies):
    for copy in copies:
        copy.start()
    return copies


def finish_all(copies):
    for copy in copies:
        copy.wait()


def backward_kernel(rows_total, dz, dz_pair, x2, x2_pair, x1, x1_pair, h_a, h_b, w3, w2, u2, u1, vec2_hbm, vec1_hbm,
                    gw3, gw2, gw1, sums2, sums1,
                    vec2, vec1, d, pd, xt, hv, hturn, ht, dpre, wbuf, nbuf, acc3, acc2, acc1, near3, near2, near1, far3, far2, far1,
                    mine, mate, chips, whole, vec_sem, load_sem, tile_sem, pair_send, pair_recv, hop_send, hop_recv, far_send, far_recv,
                    sum_send, sum_recv, h_send, h_recv, out_sem, w_sem, n_sem, free_sem):
    me = lax.axis_index("data")
    rows = d.shape[0]
    half = rows // 2
    greet()

    def small(src, dst, k):
        return pltpu.make_async_copy(src, dst, vec_sem.at[k])

    vectors_in = [small(vec2_hbm, vec2, 0), small(vec1_hbm, vec1, 1)]
    send_sums, pass_sums, take_sums = exchange_halves(mine, mate, chips, whole, sum_send, sum_recv)

    def pair_copy(n, src=d):
        return remote(src.at[:, cols(n)], pd.at[:, cols(n)], pair_send.at[n], pair_recv.at[n], PAIR)

    def both_colours(body):
        def step(i, carry):
            for colour in TWO:
                body(colour * (TILES // 2) + i, colour)
            return carry
        lax.fori_loop(0, TILES // 2, step, 0)

    class Product:
        def __init__(self, w, lhs, acc, near, far, out):
            self.w, self.lhs, self.acc, self.near, self.far, self.out = w, lhs, acc, near, far, out
            self.blk = out.shape[0]

        def block(self, j, count=1):
            return pl.ds(j * self.blk, count * self.blk)

        def first_hop(self, n, colour):
            return remote(self.acc.at[n, self.block(1 + colour, 2)], self.near.at[n],
                          hop_send.at[self.w, n], hop_recv.at[self.w, n], YN if colour else XN)

        def second_hop(self, n, colour):
            return remote(self.acc.at[n, self.block(1 if colour else 3)], self.far.at[n],
                          far_send.at[self.w, n], far_recv.at[self.w, n], XN if colour else YN)

        def out_copy(self, n):
            return pltpu.make_async_copy(self.acc.at[n, self.block(0)], self.out.at[:, cols(n)], out_sem.at[self.w, n])

        def fill(self, n, part):
            self.acc[n, part] = self.lhs(0, part, d[:, cols(n)]) + self.lhs(1, part, pd[:, cols(n)])

        def compute(self, parts, arrive, send):
            def body(n, colour):
                if arrive:
                    arrive(n)
                for j, count in parts[colour]:
                    self.fill(n, self.block(j, count))
                if send:
                    self.first_hop(n, colour).start()
            both_colours(body)

        def relay(self):
            def body(n, colour):
                onward, own = self.block(1 if colour else 3), self.block(0)
                self.first_hop(n, colour).wait_recv()
                self.acc[n, onward] = self.acc[n, onward] + self.near[n, self.block(1 - colour)]
                self.second_hop(n, colour).start()
                self.acc[n, own] = self.acc[n, own] + self.near[n, self.block(colour)]
            both_colours(body)

        def finish(self):
            def body(n, colour):
                own = self.block(0)
                self.second_hop(n, colour).wait_recv()
                self.acc[n, own] = self.acc[n, own] + self.far[n]
                self.out_copy(n).start()
            both_colours(body)

        def drain(self):
            def body(n, colour):
                self.first_hop(n, colour).wait_send()
                self.second_hop(n, colour).wait_send()
                self.out_copy(n).wait()
            both_colours(body)

    def w_tile(src, i):
        return pltpu.make_async_copy(src.at[cols(i)], wbuf.at[i % 2], w_sem.at[i % 2])

    def n_tile(src, i):
        return pltpu.make_async_copy(src.at[:, cols(i)], nbuf.at[i % 2], n_sem.at[i % 2])

    def tiles(streams, body):
        run([s(0) for s in streams])

        def step(i, carry):
            @pl.when(i < TILES - 1)
            def _():
                run([s(i + 1) for s in streams])
            finish_all([s(i) for s in streams])
            body(i, cols(i))
            return carry
        lax.fori_loop(0, TILES, step, 0)

    def normed_tile(i, c, v, vec):
        return (nbuf[i % 2, span(v, half), :] - row(vec, MEAN + v, c)) * row(vec, INV + v, c)

    def back_product(w_src, n_src, vec, which):
        def body(i, c):
            for v in TWO:
                grad = dot(d[span(v, half), :], wbuf[i % 2], TURN_RIGHT)
                normed = normed_tile(i, c, v, vec)
                grad = jnp.where(row(vec, GAIN, c) * normed + row(vec, SHIFT, c) > 0, grad, 0.0)
                dpre[span(v, half), c] = grad
                column_sums(mine, (which,), 2 * v, c, grad, grad * normed)
        tiles([functools.partial(w_tile, w_src), functools.partial(n_tile, n_src)], body)

    def norm_grad(n_src, vec, sums):
        def body(i, c):
            for v in TWO:
                part = span(v, half)
                mean, slope = row(sums, 2 * v, c) / rows_total, row(sums, 2 * v + 1, c) / rows_total
                grad = row(vec, GAIN, c) * row(vec, INV + v, c) * (
                    dpre[part, c] - (mean + normed_tile(i, c, v, vec) * slope))
                d[part, c] = grad.astype(BF16)
            pair_copy(i).start()
        tiles([functools.partial(n_tile, n_src)], body)

    def load(src, dst, k):
        return pltpu.make_async_copy(src, dst, load_sem.at[k])

    def dz_tile(n):
        return pltpu.make_async_copy(dz.at[:, cols(n)], d.at[:, cols(n)], tile_sem.at[n])

    heads = (0, TILES // 2)
    passed = [pair_copy(n, dz) for i in range(1, TILES // 2) for n in (i, TILES // 2 + i)]

    def dz_arrived(n):
        dz_tile(n).wait()
        pair_copy(n).wait_recv()

    blk3, blk1 = gw3.shape[0], gw1.shape[0]

    def operand(src, pair):
        return [load(pair, xt.at[span(1, rows)], len(ORDER))] + [
            load(src.at[:, span(me ^ mask, blk3)], xt.at[span(0, rows), pl.ds(j * blk3, blk3)], j)
            for j, mask in enumerate(ORDER)]

    def lhs_x(k, part, right):
        return dot(xt[span(k, rows), part], right, TURN_LEFT)

    def lhs_h(k, part, right):
        return dot(ht[part, span(k, rows)], right)

    prod3 = Product(0, lhs_x, acc3, near3, far3, gw3)
    prod2 = Product(1, lhs_x, acc2, near2, far2, gw2)
    prod1 = Product(2, lhs_h, acc1, near1, far1, gw1)
    first = run(operand(x2, x2_pair))
    run([pltpu.make_async_copy(dz_pair.at[:, cols(k)], pd.at[:, cols(n)], pair_recv.at[n]) for k, n in enumerate(heads)])
    both_colours(lambda n, colour: dz_tile(n).start())
    run(vectors_in)
    all_entered()
    run(passed)
    finish_all(first + vectors_in)
    everything = ([(0, len(ORDER))],) * 2
    prod3.compute(([(1, 2)], [(2, 2)]), dz_arrived, True)
    back_product(w3, u2, vec2, 0)
    send_sums(0)
    prod3.compute(([(0, 1), (3, 1)], [(0, 2)]), None, False)
    for copy in passed:
        copy.wait_send()
    pass_sums(0)
    second = run(operand(x1, x1_pair))
    views = list(enumerate((h_a, h_b)))
    own_h = run([load(src, hv.at[span(v, half)], len(ORDER) + 1 + v) for v, src in views])
    pair_h = run([remote(src, hv.at[span(2 + v, half)], h_send.at[v], h_recv.at[v], PAIR) for v, src in views])
    prod3.relay()
    take_sums(0)
    sums_out = run([small(whole.at[0], sums2, 2)])
    norm_grad(u2, vec2, whole.at[0])
    finish_all(second)
    prod2.compute(everything, lambda n: pair_copy(n).wait(), True)
    pl.semaphore_signal(free_sem, inc=1, device_id=(me ^ PAIR,), device_id_type=MESH)
    back_product(w2, u1, vec1, 1)
    send_sums(1)
    finish_all(own_h + pair_h)
    for k in range(2 * len(TWO)):
        hturn[:, span(k, half)] = hv[span(k, half), :].T
    for j, mask in enumerate(ORDER):
        ht[span(j, blk1), :] = hturn[span(me ^ mask, blk1), :]
    pass_sums(1)
    prod3.finish()
    prod2.relay()
    take_sums(1)
    sums_out += run([small(whole.at[1], sums1, 3)])
    pl.semaphore_wait(free_sem, 1)
    norm_grad(u1, vec1, whole.at[1])
    prod1.compute(everything, lambda n: pair_copy(n).wait(), True)
    prod1.relay()
    prod2.finish()
    prod1.finish()
    for product in (prod3, prod2, prod1):
        product.drain()
    finish_all(sums_out)


ANYWHERE = pl.BlockSpec(memory_space=pl.ANY)
SCALARS = pl.BlockSpec(memory_space=pltpu.SMEM)


def params(cid):
    return pltpu.CompilerParams(collective_id=cid, has_side_effects=True, vmem_limit_bytes=VMEM_BYTES)


def backward(rows_total, dz, *rest, cid):
    h_a = rest[5]
    rows, feats = dz.shape
    blk3, blk1 = feats // DEVICES, h_a.shape[1] // DEVICES
    groups = len(ORDER)
    blocks = (blk3, blk3, blk1)

    def per_weight(parts):
        return [pltpu.VMEM((TILES, parts * b, TILE), F32) for b in blocks]

    sums = jax.ShapeDtypeStruct((2 * len(TWO), feats), F32)
    half_sums = (2 * len(TWO), feats // 2)
    return pl.pallas_call(
        functools.partial(backward_kernel, rows_total),
        out_shape=[jax.ShapeDtypeStruct((b, feats), F32) for b in blocks] + [sums, sums],
        in_specs=[ANYWHERE] * (len(rest) + 1),
        out_specs=[ANYWHERE] * (WEIGHTS + 2),
        scratch_shapes=[pltpu.VMEM((VEC_ROWS, feats), F32)] * 2 + [pltpu.VMEM((rows, feats), BF16), pltpu.VMEM((rows, feats), BF16),
                        pltpu.VMEM((2 * rows, groups * blk3), BF16), pltpu.VMEM((2 * rows, h_a.shape[1]), BF16),
                        pltpu.VMEM((h_a.shape[1], 2 * rows), BF16), pltpu.VMEM((groups * blk1, 2 * rows), BF16),
                        pltpu.VMEM((rows, feats), F32),
                        pltpu.VMEM((2, TILE, feats), BF16), pltpu.VMEM((2, rows, TILE), F32)]
        + per_weight(groups) + per_weight(2) + per_weight(1)
        + [pltpu.VMEM(shape, F32) for shape in ((2,) + sums.shape, (2,) + half_sums, (2, DEVICES // 2) + half_sums,
                                                (2,) + sums.shape)]
        + [DMA((len(ORDER),)), DMA((DEVICES,)), DMA((TILES,))]
        + [DMA((TILES,))] * 2 + [DMA((WEIGHTS, TILES))] * 4 + [DMA((2, DEVICES))] * 2 + [DMA((2,))] * 2
        + [DMA((WEIGHTS, TILES))] + [DMA((2,))] * 2 + [pltpu.SemaphoreType.REGULAR],
        compiler_params=params(cid),
        name="backward",
    )(dz, *rest)


def forward_kernel(rows_total, lam, h_a, h_b, w1, w2, w3, gain1, shift1, gain2, shift2,
                   loss, u1, u2, x1, x2, x1_pair, x2_pair, dz, dz_pair, vec1_out, vec2_out,
                   affine, vec1, vec2, vec_sem, hv, ubuf, vbuf, w2buf, w3buf, xbuf, zh, za, zb, corr, mine, slots, vec3, loss_mine, loss_slots,
                   load_sem, store_sem, pair_send, pair_recv, sum_send, sum_recv, za_send, za_recv, zb_send, zb_recv,
                   g_send, g_recv, loss_send, loss_recv, dz_sem, dz_send, dz_recv):
    me = lax.axis_index("data")
    half = hv.shape[0] // 2
    feats = w2buf.shape[0]
    rblk, cblk = za.shape[2], zb.shape[2]
    greet()

    def load(src, dst, k):
        return pltpu.make_async_copy(src, dst, load_sem.at[k])

    w1_view = w3buf.at[pl.ds(0, w1.shape[0])]
    loads = run([load(h_a, hv.at[span(0, half)], 0), load(h_b, hv.at[span(1, half)], 1), load(w1, w1_view, 2)])
    affine_in = run([pltpu.make_async_copy(src, affine.at[k], vec_sem.at[k])
                     for k, src in enumerate((gain1, shift1, gain2, shift2))])
    all_entered()
    send_sums, take_sums = exchange(mine, slots, sum_send, sum_recv)
    send_loss, take_loss = exchange(loss_mine, loss_slots, loss_send, loss_recv)

    def each_tile(body):
        def step(n, carry):
            body(n, cols(n))
            return carry
        lax.fori_loop(0, TILES, step, 0)

    def take_vectors(e, v, vec):
        total = take_sums(e) / rows_total
        mean = total[:1]
        vec[pl.ds(MEAN + v, 1), :] = mean
        vec[pl.ds(INV + v, 1), :] = lax.rsqrt(total[1:] - mean * mean + NORM_EPS)

    def layer(e, v, left, weight, out, beside=None):
        part = span(v, half)

        def body(n, carry):
            c = span(n, WIDE)
            value = dot(left[part, :], weight[:, c])
            out[part, c] = value
            column_sums(mine, (e,), 0, c, value, value * value)
            if beside:
                beside(c)
            return carry
        lax.fori_loop(0, feats // WIDE, body, 0)
        send_sums(e)

    def normed_tile(values, v, c, vec):
        return (values[span(v, half), c] - row(vec, MEAN + v, c)) * row(vec, INV + v, c)

    def activate_tile(v, values, vec, c):
        pre = row(vec, GAIN, c) * normed_tile(values, v, c, vec) + row(vec, SHIFT, c)
        xbuf[span(v, half), c] = jnp.maximum(pre, 0.0).astype(BF16)

    def activate(v, values, vec):
        each_tile(lambda n, c: activate_tile(v, values, vec, c))

    def store(src, dst, k):
        return pltpu.make_async_copy(src, dst, store_sem.at[k])

    def keep_rows(dst, pair, index):
        blk = feats // DEVICES
        return run([store(xbuf, dst, 2)] + [
            remote(xbuf.at[:, span(me ^ mask ^ PAIR, blk)], pair.at[:, pl.ds(j * blk, blk)],
                   pair_send.at[index, j], pair_recv.at[index, j], PAIR) for j, mask in enumerate(ORDER)])

    finish_all(loads + affine_in)
    for k, vec in enumerate((vec1, vec2)):
        vec[pl.ds(GAIN, 1), :] = affine[2 * k]
        vec[pl.ds(SHIFT, 1), :] = affine[2 * k + 1]
    load_w2 = load(w2, w2buf, 0)
    load_w2.start()
    for v in TWO:
        layer(v, v, hv, w1_view, ubuf)
    load_w3 = load(w3, w3buf, 2)
    store_u1 = store(ubuf, u1, 0)
    run([load_w3, store_u1])
    for v in TWO:
        take_vectors(v, v, vec1)
    activate(0, ubuf, vec1)
    load_w2.wait()
    layer(2, 0, xbuf, w2buf, vbuf, functools.partial(activate_tile, 1, ubuf, vec1))
    kept = keep_rows(x1, x1_pair, 0)
    layer(3, 1, xbuf, w2buf, vbuf)
    store_u2 = store(vbuf, u2, 1)
    store_u2.start()
    finish_all([store_u1, load_w3] + kept)
    for v in TWO:
        take_vectors(2 + v, v, vec2)
        activate(v, vbuf, vec2)
        if v:
            kept = keep_rows(x2, x2_pair, 1)
        layer(4 + v, v, xbuf, w3buf, ubuf)

    small_out = run([pltpu.make_async_copy(vec, out, vec_sem.at[k])
                     for k, (vec, out) in enumerate(((vec1, vec1_out), (vec2, vec2_out)))])

    def embed(v):
        take_vectors(4 + v, v, vec3)

        def body(n, c):
            zh[span(v, half), c] = normed_tile(ubuf, v, c, vec3).astype(BF16)
        each_tile(body)

    def row_index(mask):
        dev = me ^ mask
        return dev // 4 * 2 + dev % 2

    def row_block(mask):
        return span(row_index(mask), rblk)

    def col_block(mask):
        return span((me ^ mask) // 2 % 2, cblk)

    quarter = half // 2
    started = []

    def go(copy):
        copy.start()
        started.append(copy)

    def za_direct(mask):
        return remote(zh.at[span(0, half), row_block(mask)], za.at[me], za_send.at[mask], za_recv.at[mask], mask)

    def za_relay(origin):
        slot = za.at[me ^ origin]
        return remote(slot, slot, za_send.at[origin ^ XN], za_recv.at[origin ^ XN], XN)

    def zb_slot(origin, k):
        return zb.at[me ^ origin, span(k, quarter)]

    def zb_direct(mask, k):
        return remote(zh.at[span(2 + k, quarter), col_block(mask)], zb_slot(OWN, k),
                      zb_send.at[mask, k], zb_recv.at[mask, k], mask)

    def zb_relay(origin, mask, k, send):
        return remote(zb_slot(origin, k), zb_slot(origin, k), zb_send.at[send, k], zb_recv.at[origin ^ mask, k], mask)

    def za_arrived(origin):
        slot = za.at[me ^ origin]
        remote(slot, slot, za_send.at[OWN], za_recv.at[origin], PAIR).wait_recv()

    def zb_arrived(origin, ks=TWO):
        for k in ks:
            zb_relay(origin, OWN, k, OWN).wait_recv()

    def accumulate(origin):
        corr[...] = corr[...] + dot(za[me ^ origin], zb[me ^ origin], TURN_LEFT)

    embed(0)
    for mask in (YN, XN, YP, XP, PAIR):
        go(za_direct(mask))
    embed(1)
    for k in TWO:
        for mask in (XN, YN, PAIR):
            go(zb_direct(mask, k))
    corr[...] = dot(zh[span(0, half), row_block(OWN)], zh[span(1, half), col_block(OWN)], TURN_LEFT)
    za_arrived(PAIR)
    zb_arrived(PAIR)
    accumulate(PAIR)
    for origin in (YN, YP):
        za_arrived(origin)
        go(za_relay(origin))
    for k in TWO:
        zb_arrived(XN, (k,))
        go(zb_relay(XN, YN, k, XP))
        go(zb_relay(XN, PAIR, k, YP))
        zb_arrived(YN, (k,))
        go(zb_relay(YN, PAIR, k, DG))
    za_arrived(XN)
    accumulate(XN)
    accumulate(YN)
    za_arrived(XP)
    for origin in (XP, YP):
        zb_arrived(origin)
        accumulate(origin)
    for k in TWO:
        zb_arrived(DG, (k,))
        go(zb_relay(DG, PAIR, k, DP))
    za_arrived(DG)
    accumulate(DG)
    za_arrived(DP)
    zb_arrived(DP)
    accumulate(DP)

    lam_off = lam[0]
    row_start, col_start = row_index(OWN) * rblk, me // 2 % 2 * cblk

    pieces = g_send.shape[1]
    piece = rblk // pieces

    def g_slot(origin, k):
        return w2buf.at[span(row_index(origin) * pieces + k, piece), col_block(origin)]

    def g_copy(origin, mask, k, send):
        return remote(g_slot(origin, k), g_slot(origin, k), g_send.at[send, k], g_recv.at[origin ^ mask, k], mask)

    def g_arrived(origin, ks):
        for k in ks:
            g_copy(origin, OWN, k, OWN).wait_recv()

    def grad_piece(k):
        value = corr[span(k, piece), :] / rows_total
        row_ids = row_start + k * piece + lax.broadcasted_iota(jnp.int32, value.shape, 0)
        col_ids = col_start + lax.broadcasted_iota(jnp.int32, value.shape, 1)
        diag = row_ids == col_ids
        gap = 1.0 - value
        terms = jnp.where(diag, gap * gap, lam_off * value * value)
        grad = jnp.where(diag, -2.0 * gap, 2.0 * lam_off * value) / rows_total
        w2buf[span(row_index(OWN) * pieces + k, piece), col_block(OWN)] = grad.astype(BF16)
        return jnp.sum(terms, axis=0, keepdims=True)

    every = range(pieces)
    even, odd = every[::2], every[1::2]
    loss_row = jnp.zeros((1, cblk), F32)
    for k in every:
        loss_row = loss_row + grad_piece(k)
        go(g_copy(OWN, *((YN, k, XN) if k in odd else (XN, k, PAIR))))
    for k, j in zip(odd, even):
        go(g_copy(OWN, XN, k, PAIR))
        go(g_copy(OWN, YN, j, XN))

    def contribute(origin, k, count):
        part = span(row_index(origin) * (pieces // count) + k // count, count * piece)
        block = w2buf[part, col_block(origin)]
        first = dot(zh[span(1, half), col_block(origin)], block, TURN_RIGHT)
        where_a, where_b = (span(0, half), part), (span(1, half), col_block(origin))
        vbuf[where_a] = vbuf[where_a] + first if origin & XN else first
        second = dot(zh[span(0, half), part], block)
        vbuf[where_b] = second if origin in (OWN, XN) and not k else vbuf[where_b] + second

    for k in every:
        go(g_copy(OWN, PAIR, k, XP))
    loss_mine[0] = jnp.broadcast_to(jnp.sum(loss_row, axis=1, keepdims=True), loss_mine.shape[1:])
    send_loss(0)
    store_u2.wait()
    contribute(OWN, 0, pieces)
    g_arrived(PAIR, every)
    contribute(PAIR, 0, pieces)
    for k, j in zip(even, odd):
        g_arrived(XN, (k,))
        go(g_copy(XN, YN, k, YN))
        go(g_copy(XN, PAIR, k, YP))
        g_arrived(YN, (j,))
        go(g_copy(YN, XN, j, YN))
        go(g_copy(YN, PAIR, j, DG))
    for k, j in zip(odd, even):
        g_arrived(XN, (k,))
        go(g_copy(XN, PAIR, k, YP))
        g_arrived(YN, (j,))
        go(g_copy(YN, PAIR, j, DG))
    contribute(YN, 0, pieces)
    contribute(XN, 0, pieces)
    for origin in (YP, XP):
        g_arrived(origin, every)
        contribute(origin, 0, pieces)
    def dz_columns(v, late):
        first = me // 2 % 2 if v else me // 4
        return span(1 - first if late else first, cblk)

    def dz_sum_copy(v, late, mask):
        e, c = DG + v, dz_columns(v, late)
        k = DEVICES + v if late else e
        return remote(mine.at[e, :, c], slots.at[e, me, :, c], sum_send.at[k, mask], sum_recv.at[k, mask], mask)

    def dz_sums(late):
        for v in TWO:
            def body(t, carry, v=v):
                start = dz_columns(v, late).start + t * TILE
                c = pl.ds(pl.multiple_of(start, TILE), TILE)
                grad = vbuf[span(v, half), c]
                column_sums(mine, (DG + v,), 0, c, grad, grad * normed_tile(ubuf, v, c, vec3))
                return carry
            lax.fori_loop(0, cblk // TILE, body, 0)
            run([dz_sum_copy(v, late, mask) for mask in FAR_FIRST])

    dz_sums(False)
    for k in even:
        now = (k, k + 1)
        for j in now:
            g_arrived(DG, (j,))
            go(g_copy(DG, PAIR, j, DP))
        contribute(DG, k, len(now))
        g_arrived(DP, now)
        contribute(DP, k, len(now))

    dz_sums(True)
    finish_all(kept)
    loss_mine[0] = take_loss(0)
    small_out += run([pltpu.make_async_copy(loss_mine.at[0], loss, vec_sem.at[2])])
    for v in TWO:
        slots[DG + v, me] = mine[DG + v]
    for v in TWO:
        finish_all([dz_sum_copy(v, late, mask) for late in (False, True) for mask in FAR_FIRST])
        mine[DG + v] = functools.reduce(jnp.add, [slots[DG + v, k] for k in range(DEVICES)]) / rows_total

    def dz_copy(n):
        return pltpu.make_async_copy(xbuf.at[:, cols(n)], dz.at[:, cols(n)], dz_sem.at[n])

    def dz_tile(n):
        c = cols(n)
        for v in TWO:
            sums = mine[DG + v, :, c]
            grad = row(vec3, INV + v, c) * (
                vbuf[span(v, half), c] - (sums[:1] + normed_tile(ubuf, v, c, vec3) * sums[1:]))
            xbuf[span(v, half), c] = grad.astype(BF16)
        dz_copy(n).start()

    heads = (0, TILES // 2)
    for k, n in enumerate(heads):
        dz_tile(n)
        go(remote(xbuf.at[:, cols(n)], dz_pair.at[:, cols(k)], dz_send.at[k], dz_recv.at[k], PAIR))

    def dz_body(i, carry):
        for n in heads:
            dz_tile(n + i)
        return carry
    lax.fori_loop(1, TILES // 2, dz_body, 0)
    for copy in started:
        copy.wait_send()
    for copy in started[-len(heads):]:
        copy.wait_recv()
    finish_all(small_out)
    each_tile(lambda n, c: dz_copy(n).wait())


def forward(rows_total, lam, h_a, h_b, w1, w2, w3, *vectors, cid):
    half, depth = h_a.shape
    feats = w2.shape[0]
    full, pair, vec = (2 * half, feats), (2 * half, feats // 2), (VEC_ROWS, feats)
    small = (DEVICES, 128)
    outs = [(small, F32), (full, F32), (full, F32), (full, BF16), (full, BF16), (pair, BF16), (pair, BF16), (full, BF16), ((2 * half, 2 * TILE), BF16),
            (vec, F32), (vec, F32)]
    scratch = [((2 * half, depth), BF16), (full, F32), (full, F32), ((feats, feats), BF16), ((feats, feats), BF16),
               (full, BF16), (full, BF16), ((DEVICES, half, feats // 4), BF16), ((DEVICES, half, feats // 2), BF16),
               ((feats // 4, feats // 2), F32), ((DEVICES, 2, feats), F32), ((DEVICES, DEVICES, 2, feats), F32),
               (vec, F32), ((1,) + small, F32), ((1, DEVICES) + small, F32)]
    return pl.pallas_call(
        functools.partial(forward_kernel, rows_total),
        out_shape=[jax.ShapeDtypeStruct(*out) for out in outs],
        in_specs=[SCALARS] + [ANYWHERE] * (5 + len(vectors)),
        out_specs=[ANYWHERE] * len(outs),
        scratch_shapes=[pltpu.VMEM((len(vectors), 1, feats), F32)] + [pltpu.VMEM(vec, F32)] * 2
        + [DMA((len(vectors),))] + [pltpu.VMEM(*item) for item in scratch]
        + [DMA((WEIGHTS,))] * 2 + [DMA((2, len(ORDER)))] * 2 + [DMA((DEVICES + 2, DEVICES))] * 2 + [DMA((DEVICES,))] * 2
        + [DMA((DEVICES, 2))] * 2 + [DMA((DEVICES, 4))] * 2 + [DMA((1, DEVICES))] * 2 + [DMA((TILES,))] + [DMA((2,))] * 2,
        compiler_params=params(cid),
        name="forward",
    )(lam, h_a, h_b, w1, w2, w3, *vectors)


def emit_kernel(gw3, gw2, gw1, sums2, sums1, loss, loss_out, out3, out2, out1, gain1, shift1, gain2, shift2,
                buf, sums, vecs, loss_in, in_sem, out_sem, sum_sem, vec_sem, loss_sem):
    step = gw1.shape[0]
    pieces = [(src, dst, k) for src, dst in ((gw3, out3), (gw2, out2), (gw1, out1)) for k in range(src.shape[0] // step)]
    ins = run([pltpu.make_async_copy(src.at[span(k, step)], buf.at[i], in_sem.at[i])
               for i, (src, dst, k) in enumerate(pieces)])
    sums_in = run([pltpu.make_async_copy(src, sums.at[i], sum_sem.at[i]) for i, src in enumerate((sums1, sums2))])
    outs = [pltpu.make_async_copy(buf.at[i], dst.at[span(k, step)], out_sem.at[i])
            for i, (src, dst, k) in enumerate(pieces)]
    loss_copy = pltpu.make_async_copy(loss, loss_in, loss_sem)
    loss_copy.start()
    half = len(ins) // 2
    for before, after in zip(ins[:half], outs):
        before.wait()
        after.start()
    finish_all(sums_in)
    for i in TWO:
        both = sums[i, :2, :] + sums[i, 2:, :]
        vecs[2 * i] = both[1:]
        vecs[2 * i + 1] = both[:1]
    vecs_out = run([pltpu.make_async_copy(vecs.at[i], dst, vec_sem.at[i])
                    for i, dst in enumerate((gain1, shift1, gain2, shift2))])
    for before, after in zip(ins[half:], outs[half:]):
        before.wait()
        after.start()
    loss_copy.wait()
    loss_out[0, 0] = loss_in[0, 0]
    finish_all(outs + vecs_out)


def emit(gw3, gw2, gw1, sums2, sums1, loss):
    weights = (gw3, gw2, gw1)
    step, feats = gw1.shape
    count = sum(g.shape[0] for g in weights) // step
    vectors = [jax.ShapeDtypeStruct((1, feats), F32)] * 4
    return pl.pallas_call(
        emit_kernel,
        out_shape=[jax.ShapeDtypeStruct((1, 1), F32)] + [jax.ShapeDtypeStruct(g.shape, F32) for g in weights] + vectors,
        in_specs=[ANYWHERE] * (WEIGHTS + WEIGHTS),
        out_specs=[SCALARS] + [ANYWHERE] * (WEIGHTS + len(vectors)),
        scratch_shapes=[pltpu.VMEM((count, step, feats), F32), pltpu.VMEM((2,) + sums1.shape, F32),
                        pltpu.VMEM((len(vectors), 1, feats), F32), pltpu.SMEM(loss.shape, F32)]
        + [DMA((count,))] * 2 + [DMA((2,)), DMA((len(vectors),)), DMA],
        name="emit",
    )(*weights, sums2, sums1, loss)


def solution(mesh):
    shards = mesh.shape["data"]

    def local_step(h_a, h_b, w_one, w_two, w_three, gain_one, shift_one, gain_two, shift_two, lam_off):
        total_rows = h_a.shape[0] * shards
        loss, u1, u2, x1, x2, x1_pair, x2_pair, dz, dz_pair, vec1, vec2 = forward(
            total_rows, lam_off.reshape(1), h_a, h_b, w_one, w_two, w_three,
            *[v[None] for v in (gain_one, shift_one, gain_two, shift_two)], cid=0)
        grads = backward(total_rows, dz, dz_pair, x2, x2_pair, x1, x1_pair, h_a, h_b, w_three, w_two, u2, u1, vec2, vec1,
                         cid=1)
        loss, grad_w_three, grad_w_two, grad_w_one, *rest = emit(*grads, loss)
        return (loss.reshape(()), grad_w_one, grad_w_two, grad_w_three, *[v[0] for v in rest])

    row_spec = P("data", None)
    whole_mat = P(None, None)
    whole_vec = P(None)
    return jax.shard_map(
        local_step, mesh=mesh,
        in_specs=(row_spec, row_spec, whole_mat, whole_mat, whole_mat,
                  whole_vec, whole_vec, whole_vec, whole_vec, P()),
        out_specs=(P(), row_spec, row_spec, row_spec, whole_vec, whole_vec, whole_vec, whole_vec),
        check_vma=False)
```

```python
import functools

import jax
import jax.numpy as jnp
from jax import lax
from jax.experimental import pallas as pl
from jax.experimental.pallas import tpu as pltpu
from jax.sharding import PartitionSpec as P

NORM_EPS = 1e-5
MESH = pl.DeviceIdType.MESH
DEVICES = 8
OWN, PAIR, XN, XP, YN, YP, DG, DP = range(DEVICES)
FAR_FIRST = (DG, DP, XN, XP, YN, YP, PAIR)
ORDER = (OWN, XN, DG, YN)
TWO = range(2)
TILE = 256
TILES = 8
WIDE = 512
WEIGHTS = 3
GAIN, SHIFT, INV, MEAN, VEC_ROWS = 0, 1, 2, 4, 6
VMEM_BYTES = 67043328
TURN_LEFT = (((0,), (0,)), ((), ()))
TURN_RIGHT = (((1,), (1,)), ((), ()))
F32, BF16 = jnp.float32, jnp.bfloat16
DMA = pltpu.SemaphoreType.DMA


def dot(left, right, dims=None):
    if dims is None:
        return jnp.dot(left, right, preferred_element_type=F32)
    return lax.dot_general(left, right, dims, preferred_element_type=F32)


def span(index, size):
    return pl.ds(pl.multiple_of(index * size, size), size)


def cols(n):
    return span(n, TILE)


def row(ref, r, c):
    return ref[r:r + 1, c]


def remote(src, dst, send, recv, mask):
    return pltpu.make_async_remote_copy(src_ref=src, dst_ref=dst, send_sem=send, recv_sem=recv,
                                        device_id=(lax.axis_index("data") ^ mask,), device_id_type=MESH)


def greet():
    for mask in FAR_FIRST:
        pl.semaphore_signal(pltpu.get_barrier_semaphore(), inc=1, device_id=(lax.axis_index("data") ^ mask,),
                            device_id_type=MESH)


def all_entered():
    pl.semaphore_wait(pltpu.get_barrier_semaphore(), len(FAR_FIRST))


def column_sums(ref, lead, r, c, first, second):
    ref[lead + (slice(r, r + 1), c)] = jnp.sum(first, axis=0, keepdims=True)
    ref[lead + (slice(r + 1, r + 2), c)] = jnp.sum(second, axis=0, keepdims=True)


def exchange(mine, slots, send, recv):
    me = lax.axis_index("data")

    def copy(e, mask):
        return remote(mine.at[e], slots.at[e, me], send.at[e, mask], recv.at[e, mask], mask)

    def start(e):
        for mask in FAR_FIRST:
            copy(e, mask).start()
        slots[e, me] = mine[e]

    def take(e):
        for mask in FAR_FIRST:
            copy(e, mask).wait()
        return functools.reduce(jnp.add, [slots[e, k] for k in range(DEVICES)])
    return start, take


def exchange_halves(mine, mate, chips, whole, send, recv):
    me = lax.axis_index("data")
    width = mate.shape[-1]
    core, chip = me % 2, me // 2
    others = (DG, XN, YN)

    def pair_copy(e):
        return remote(mine.at[e, :, span(1 - core, width)], mate.at[e], send.at[e, OWN], recv.at[e, OWN], PAIR)

    def chip_copy(e, mask):
        return remote(chips.at[e, chip], chips.at[e, chip], send.at[e, mask], recv.at[e, mask], mask)

    def share(e):
        half = whole.at[e, :, span(core, width)]
        return remote(half, half, send.at[e, PAIR], recv.at[e, PAIR], PAIR)

    def start(e):
        pair_copy(e).start()

    def middle(e):
        pair_copy(e).wait()
        chips[e, chip] = mine[e, :, span(core, width)] + mate[e]
        for mask in others:
            chip_copy(e, mask).start()

    def take(e):
        for mask in others:
            chip_copy(e, mask).wait()
        whole[e, :, span(core, width)] = functools.reduce(jnp.add, [chips[e, k] for k in range(DEVICES // 2)])
        share(e).start()
        share(e).wait()
    return start, middle, take


def run(copies):
    for copy in copies:
        copy.start()
    return copies


def finish_all(copies):
    for copy in copies:
        copy.wait()


def backward_kernel(rows_total, dz, dz_pair, x2, x2_pair, x1, x1_pair, h_a, h_b, w3, w2, u2, u1, vec2_hbm, vec1_hbm,
                    gw3, gw2, gw1, sums2, sums1,
                    vec2, vec1, d, pd, xt, hv, hturn, ht, dpre, wbuf, nbuf, acc3, acc2, acc1, near3, near2, near1, far3, far2, far1,
                    mine, mate, chips, whole, vec_sem, load_sem, tile_sem, pair_send, pair_recv, hop_send, hop_recv, far_send, far_recv,
                    sum_send, sum_recv, h_send, h_recv, out_sem, w_sem, n_sem, free_sem):
    me = lax.axis_index("data")
    rows = d.shape[0]
    half = rows // 2
    greet()

    def small(src, dst, k):
        return pltpu.make_async_copy(src, dst, vec_sem.at[k])

    vectors_in = [small(vec2_hbm, vec2, 0), small(vec1_hbm, vec1, 1)]
    send_sums, pass_sums, take_sums = exchange_halves(mine, mate, chips, whole, sum_send, sum_recv)

    def pair_copy(n, src=d):
        return remote(src.at[:, cols(n)], pd.at[:, cols(n)], pair_send.at[n], pair_recv.at[n], PAIR)

    def both_colours(body):
        def step(i, carry):
            for colour in TWO:
                body(colour * (TILES // 2) + i, colour)
            return carry
        lax.fori_loop(0, TILES // 2, step, 0)

    class Product:
        def __init__(self, w, lhs, acc, near, far, out):
            self.w, self.lhs, self.acc, self.near, self.far, self.out = w, lhs, acc, near, far, out
            self.blk = out.shape[0]

        def block(self, j, count=1):
            return pl.ds(j * self.blk, count * self.blk)

        def first_hop(self, n, colour):
            return remote(self.acc.at[n, self.block(1 + colour, 2)], self.near.at[n],
                          hop_send.at[self.w, n], hop_recv.at[self.w, n], YN if colour else XN)

        def second_hop(self, n, colour):
            return remote(self.acc.at[n, self.block(1 if colour else 3)], self.far.at[n],
                          far_send.at[self.w, n], far_recv.at[self.w, n], XN if colour else YN)

        def out_copy(self, n):
            return pltpu.make_async_copy(self.acc.at[n, self.block(0)], self.out.at[:, cols(n)], out_sem.at[self.w, n])

        def fill(self, n, part):
            self.acc[n, part] = self.lhs(0, part, d[:, cols(n)]) + self.lhs(1, part, pd[:, cols(n)])

        def compute(self, parts, arrive, send):
            def body(n, colour):
                if arrive:
                    arrive(n)
                for j, count in parts[colour]:
                    self.fill(n, self.block(j, count))
                if send:
                    self.first_hop(n, colour).start()
            both_colours(body)

        def relay(self):
            def body(n, colour):
                onward, own = self.block(1 if colour else 3), self.block(0)
                self.first_hop(n, colour).wait_recv()
                self.acc[n, onward] = self.acc[n, onward] + self.near[n, self.block(1 - colour)]
                self.second_hop(n, colour).start()
                self.acc[n, own] = self.acc[n, own] + self.near[n, self.block(colour)]
            both_colours(body)

        def finish(self):
            def body(n, colour):
                own = self.block(0)
                self.second_hop(n, colour).wait_recv()
                self.acc[n, own] = self.acc[n, own] + self.far[n]
                self.out_copy(n).start()
            both_colours(body)

        def drain(self):
            def body(n, colour):
                self.first_hop(n, colour).wait_send()
                self.second_hop(n, colour).wait_send()
                self.out_copy(n).wait()
            both_colours(body)

    def w_tile(src, i):
        return pltpu.make_async_copy(src.at[cols(i)], wbuf.at[i % 2], w_sem.at[i % 2])

    def n_tile(src, i):
        return pltpu.make_async_copy(src.at[:, cols(i)], nbuf.at[i % 2], n_sem.at[i % 2])

    def tiles(streams, body):
        run([s(0) for s in streams])

        def step(i, carry):
            @pl.when(i < TILES - 1)
            def _():
                run([s(i + 1) for s in streams])
            finish_all([s(i) for s in streams])
            body(i, cols(i))
            return carry
        lax.fori_loop(0, TILES, step, 0)

    def normed_tile(i, c, v, vec):
        return (nbuf[i % 2, span(v, half), :] - row(vec, MEAN + v, c)) * row(vec, INV + v, c)

    def back_product(w_src, n_src, vec, which):
        def body(i, c):
            for v in TWO:
                grad = dot(d[span(v, half), :], wbuf[i % 2], TURN_RIGHT)
                normed = normed_tile(i, c, v, vec)
                grad = jnp.where(row(vec, GAIN, c) * normed + row(vec, SHIFT, c) > 0, grad, 0.0)
                dpre[span(v, half), c] = grad
                column_sums(mine, (which,), 2 * v, c, grad, grad * normed)
        tiles([functools.partial(w_tile, w_src), functools.partial(n_tile, n_src)], body)

    def norm_grad(n_src, vec, sums):
        def body(i, c):
            for v in TWO:
                part = span(v, half)
                mean, slope = row(sums, 2 * v, c) / rows_total, row(sums, 2 * v + 1, c) / rows_total
                grad = row(vec, GAIN, c) * row(vec, INV + v, c) * (
                    dpre[part, c] - (mean + normed_tile(i, c, v, vec) * slope))
                d[part, c] = grad.astype(BF16)
            pair_copy(i).start()
        tiles([functools.partial(n_tile, n_src)], body)

    def load(src, dst, k):
        return pltpu.make_async_copy(src, dst, load_sem.at[k])

    def dz_tile(n):
        return pltpu.make_async_copy(dz.at[:, cols(n)], d.at[:, cols(n)], tile_sem.at[n])

    heads = (0, TILES // 2)
    passed = [pair_copy(n, dz) for i in range(1, TILES // 2) for n in (i, TILES // 2 + i)]

    def dz_arrived(n):
        dz_tile(n).wait()
        pair_copy(n).wait_recv()

    blk3, blk1 = gw3.shape[0], gw1.shape[0]

    def operand(src, pair):
        return [load(pair, xt.at[span(1, rows)], len(ORDER))] + [
            load(src.at[:, span(me ^ mask, blk3)], xt.at[span(0, rows), pl.ds(j * blk3, blk3)], j)
            for j, mask in enumerate(ORDER)]

    def lhs_x(k, part, right):
        return dot(xt[span(k, rows), part], right, TURN_LEFT)

    def lhs_h(k, part, right):
        return dot(ht[part, span(k, rows)], right)

    prod3 = Product(0, lhs_x, acc3, near3, far3, gw3)
    prod2 = Product(1, lhs_x, acc2, near2, far2, gw2)
    prod1 = Product(2, lhs_h, acc1, near1, far1, gw1)
    first = run(operand(x2, x2_pair))
    run([pltpu.make_async_copy(dz_pair.at[:, cols(k)], pd.at[:, cols(n)], pair_recv.at[n]) for k, n in enumerate(heads)])
    both_colours(lambda n, colour: dz_tile(n).start())
    run(vectors_in)
    all_entered()
    run(passed)
    finish_all(first + vectors_in)
    everything = ([(0, len(ORDER))],) * 2
    prod3.compute(([(1, 2)], [(2, 2)]), dz_arrived, True)
    back_product(w3, u2, vec2, 0)
    send_sums(0)
    prod3.compute(([(0, 1), (3, 1)], [(0, 2)]), None, False)
    for copy in passed:
        copy.wait_send()
    pass_sums(0)
    second = run(operand(x1, x1_pair))
    views = list(enumerate((h_a, h_b)))
    own_h = run([load(src, hv.at[span(v, half)], len(ORDER) + 1 + v) for v, src in views])
    pair_h = run([remote(src, hv.at[span(2 + v, half)], h_send.at[v], h_recv.at[v], PAIR) for v, src in views])
    prod3.relay()
    take_sums(0)
    sums_out = run([small(whole.at[0], sums2, 2)])
    norm_grad(u2, vec2, whole.at[0])
    finish_all(second)
    prod2.compute(everything, lambda n: pair_copy(n).wait(), True)
    pl.semaphore_signal(free_sem, inc=1, device_id=(me ^ PAIR,), device_id_type=MESH)
    back_product(w2, u1, vec1, 1)
    send_sums(1)
    finish_all(own_h + pair_h)
    for k in range(2 * len(TWO)):
        hturn[:, span(k, half)] = hv[span(k, half), :].T
    for j, mask in enumerate(ORDER):
        ht[span(j, blk1), :] = hturn[span(me ^ mask, blk1), :]
    pass_sums(1)
    prod3.finish()
    prod2.relay()
    take_sums(1)
    sums_out += run([small(whole.at[1], sums1, 3)])
    pl.semaphore_wait(free_sem, 1)
    norm_grad(u1, vec1, whole.at[1])
    prod1.compute(everything, lambda n: pair_copy(n).wait(), True)
    prod1.relay()
    prod2.finish()
    prod1.finish()
    for product in (prod3, prod2, prod1):
        product.drain()
    finish_all(sums_out)


ANYWHERE = pl.BlockSpec(memory_space=pl.ANY)
SCALARS = pl.BlockSpec(memory_space=pltpu.SMEM)


def params(cid):
    return pltpu.CompilerParams(collective_id=cid, has_side_effects=True, vmem_limit_bytes=VMEM_BYTES)


def backward(rows_total, dz, *rest, cid):
    h_a = rest[5]
    rows, feats = dz.shape
    blk3, blk1 = feats // DEVICES, h_a.shape[1] // DEVICES
    groups = len(ORDER)
    blocks = (blk3, blk3, blk1)

    def per_weight(parts):
        return [pltpu.VMEM((TILES, parts * b, TILE), F32) for b in blocks]

    sums = jax.ShapeDtypeStruct((2 * len(TWO), feats), F32)
    half_sums = (2 * len(TWO), feats // 2)
    return pl.pallas_call(
        functools.partial(backward_kernel, rows_total),
        out_shape=[jax.ShapeDtypeStruct((b, feats), F32) for b in blocks] + [sums, sums],
        in_specs=[ANYWHERE] * (len(rest) + 1),
        out_specs=[ANYWHERE] * (WEIGHTS + 2),
        scratch_shapes=[pltpu.VMEM((VEC_ROWS, feats), F32)] * 2 + [pltpu.VMEM((rows, feats), BF16), pltpu.VMEM((rows, feats), BF16),
                        pltpu.VMEM((2 * rows, groups * blk3), BF16), pltpu.VMEM((2 * rows, h_a.shape[1]), BF16),
                        pltpu.VMEM((h_a.shape[1], 2 * rows), BF16), pltpu.VMEM((groups * blk1, 2 * rows), BF16),
                        pltpu.VMEM((rows, feats), F32),
                        pltpu.VMEM((2, TILE, feats), BF16), pltpu.VMEM((2, rows, TILE), F32)]
        + per_weight(groups) + per_weight(2) + per_weight(1)
        + [pltpu.VMEM(shape, F32) for shape in ((2,) + sums.shape, (2,) + half_sums, (2, DEVICES // 2) + half_sums,
                                                (2,) + sums.shape)]
        + [DMA((len(ORDER),)), DMA((DEVICES,)), DMA((TILES,))]
        + [DMA((TILES,))] * 2 + [DMA((WEIGHTS, TILES))] * 4 + [DMA((2, DEVICES))] * 2 + [DMA((2,))] * 2
        + [DMA((WEIGHTS, TILES))] + [DMA((2,))] * 2 + [pltpu.SemaphoreType.REGULAR],
        compiler_params=params(cid),
        name="backward",
    )(dz, *rest)


def forward_kernel(rows_total, lam, h_a, h_b, w1, w2, w3, gain1, shift1, gain2, shift2,
                   loss, u1, u2, x1, x2, x1_pair, x2_pair, dz, dz_pair, vec1_out, vec2_out,
                   affine, vec1, vec2, vec_sem, hv, ubuf, vbuf, w2buf, w3buf, xbuf, zh, za, zb, corr, mine, slots, vec3, loss_mine, loss_slots,
                   load_sem, store_sem, pair_send, pair_recv, sum_send, sum_recv, za_send, za_recv, zb_send, zb_recv,
                   g_send, g_recv, loss_send, loss_recv, dz_sem, dz_send, dz_recv):
    me = lax.axis_index("data")
    half = hv.shape[0] // 2
    feats = w2buf.shape[0]
    rblk, cblk = za.shape[2], zb.shape[2]
    greet()

    def load(src, dst, k):
        return pltpu.make_async_copy(src, dst, load_sem.at[k])

    w1_view = w3buf.at[pl.ds(0, w1.shape[0])]
    loads = run([load(h_a, hv.at[span(0, half)], 0), load(h_b, hv.at[span(1, half)], 1), load(w1, w1_view, 2)])
    affine_in = run([pltpu.make_async_copy(src, affine.at[k], vec_sem.at[k])
                     for k, src in enumerate((gain1, shift1, gain2, shift2))])
    send_sums, take_sums = exchange(mine, slots, sum_send, sum_recv)
    send_loss, take_loss = exchange(loss_mine, loss_slots, loss_send, loss_recv)

    def each_tile(body):
        def step(n, carry):
            body(n, cols(n))
            return carry
        lax.fori_loop(0, TILES, step, 0)

    def take_vectors(e, v, vec):
        total = take_sums(e) / rows_total
        mean = total[:1]
        vec[pl.ds(MEAN + v, 1), :] = mean
        vec[pl.ds(INV + v, 1), :] = lax.rsqrt(total[1:] - mean * mean + NORM_EPS)

    def layer(e, v, left, weight, out, beside=None):
        part = span(v, half)

        def body(n, carry):
            c = span(n, WIDE)
            value = dot(left[part, :], weight[:, c])
            out[part, c] = value
            column_sums(mine, (e,), 0, c, value, value * value)
            if beside:
                beside(c)
            return carry
        lax.fori_loop(0, feats // WIDE, body, 0)

    def normed_tile(values, v, c, vec):
        return (values[span(v, half), c] - row(vec, MEAN + v, c)) * row(vec, INV + v, c)

    def activate_tile(v, values, vec, c):
        pre = row(vec, GAIN, c) * normed_tile(values, v, c, vec) + row(vec, SHIFT, c)
        xbuf[span(v, half), c] = jnp.maximum(pre, 0.0).astype(BF16)

    def activate(v, values, vec):
        each_tile(lambda n, c: activate_tile(v, values, vec, c))

    def store(src, dst, k):
        return pltpu.make_async_copy(src, dst, store_sem.at[k])

    def keep_rows(dst, pair, index):
        blk = feats // DEVICES
        return run([store(xbuf, dst, 2)] + [
            remote(xbuf.at[:, span(me ^ mask ^ PAIR, blk)], pair.at[:, pl.ds(j * blk, blk)],
                   pair_send.at[index, j], pair_recv.at[index, j], PAIR) for j, mask in enumerate(ORDER)])

    finish_all(loads + affine_in)
    for k, vec in enumerate((vec1, vec2)):
        vec[pl.ds(GAIN, 1), :] = affine[2 * k]
        vec[pl.ds(SHIFT, 1), :] = affine[2 * k + 1]
    load_w2 = load(w2, w2buf, 0)
    load_w2.start()
    for v in TWO:
        layer(v, v, hv, w1_view, ubuf)
    all_entered()
    for v in TWO:
        send_sums(v)
    load_w3 = load(w3, w3buf, 2)
    store_u1 = store(ubuf, u1, 0)
    run([load_w3, store_u1])
    for v in TWO:
        take_vectors(v, v, vec1)
    activate(0, ubuf, vec1)
    load_w2.wait()
    layer(2, 0, xbuf, w2buf, vbuf, functools.partial(activate_tile, 1, ubuf, vec1))
    send_sums(2)
    kept = keep_rows(x1, x1_pair, 0)
    layer(3, 1, xbuf, w2buf, vbuf)
    send_sums(3)
    store_u2 = store(vbuf, u2, 1)
    store_u2.start()
    finish_all([store_u1, load_w3] + kept)
    for v in TWO:
        take_vectors(2 + v, v, vec2)
        activate(v, vbuf, vec2)
        if v:
            kept = keep_rows(x2, x2_pair, 1)
        layer(4 + v, v, xbuf, w3buf, ubuf)
        send_sums(4 + v)

    small_out = run([pltpu.make_async_copy(vec, out, vec_sem.at[k])
                     for k, (vec, out) in enumerate(((vec1, vec1_out), (vec2, vec2_out)))])

    def embed(v):
        take_vectors(4 + v, v, vec3)

        def body(n, c):
            zh[span(v, half), c] = normed_tile(ubuf, v, c, vec3).astype(BF16)
        each_tile(body)

    def row_index(mask):
        dev = me ^ mask
        return dev // 4 * 2 + dev % 2

    def row_block(mask):
        return span(row_index(mask), rblk)

    def col_block(mask):
        return span((me ^ mask) // 2 % 2, cblk)

    quarter = half // 2
    started = []

    def go(copy):
        copy.start()
        started.append(copy)

    def za_direct(mask):
        return remote(zh.at[span(0, half), row_block(mask)], za.at[me], za_send.at[mask], za_recv.at[mask], mask)

    def za_relay(origin):
        slot = za.at[me ^ origin]
        return remote(slot, slot, za_send.at[origin ^ XN], za_recv.at[origin ^ XN], XN)

    def zb_slot(origin, k):
        return zb.at[me ^ origin, span(k, quarter)]

    def zb_direct(mask, k):
        return remote(zh.at[span(2 + k, quarter), col_block(mask)], zb_slot(OWN, k),
                      zb_send.at[mask, k], zb_recv.at[mask, k], mask)

    def zb_relay(origin, mask, k, send):
        return remote(zb_slot(origin, k), zb_slot(origin, k), zb_send.at[send, k], zb_recv.at[origin ^ mask, k], mask)

    def za_arrived(origin):
        slot = za.at[me ^ origin]
        remote(slot, slot, za_send.at[OWN], za_recv.at[origin], PAIR).wait_recv()

    def zb_arrived(origin, ks=TWO):
        for k in ks:
            zb_relay(origin, OWN, k, OWN).wait_recv()

    def accumulate(origin):
        corr[...] = corr[...] + dot(za[me ^ origin], zb[me ^ origin], TURN_LEFT)

    embed(0)
    for mask in (YN, XN, YP, XP, PAIR):
        go(za_direct(mask))
    embed(1)
    for k in TWO:
        for mask in (XN, YN, PAIR):
            go(zb_direct(mask, k))
    corr[...] = dot(zh[span(0, half), row_block(OWN)], zh[span(1, half), col_block(OWN)], TURN_LEFT)
    za_arrived(PAIR)
    zb_arrived(PAIR)
    accumulate(PAIR)
    for origin in (YN, YP):
        za_arrived(origin)
        go(za_relay(origin))
    for k in TWO:
        zb_arrived(XN, (k,))
        go(zb_relay(XN, YN, k, XP))
        go(zb_relay(XN, PAIR, k, YP))
        zb_arrived(YN, (k,))
        go(zb_relay(YN, PAIR, k, DG))
    za_arrived(XN)
    accumulate(XN)
    accumulate(YN)
    za_arrived(XP)
    for origin in (XP, YP):
        zb_arrived(origin)
        accumulate(origin)
    for k in TWO:
        zb_arrived(DG, (k,))
        go(zb_relay(DG, PAIR, k, DP))
    za_arrived(DG)
    accumulate(DG)
    za_arrived(DP)
    zb_arrived(DP)
    accumulate(DP)

    lam_off = lam[0]
    row_start, col_start = row_index(OWN) * rblk, me // 2 % 2 * cblk

    pieces = g_send.shape[1]
    piece = rblk // pieces

    def g_slot(origin, k):
        return w2buf.at[span(row_index(origin) * pieces + k, piece), col_block(origin)]

    def g_copy(origin, mask, k, send):
        return remote(g_slot(origin, k), g_slot(origin, k), g_send.at[send, k], g_recv.at[origin ^ mask, k], mask)

    def g_arrived(origin, ks):
        for k in ks:
            g_copy(origin, OWN, k, OWN).wait_recv()

    def grad_piece(k):
        value = corr[span(k, piece), :] / rows_total
        row_ids = row_start + k * piece + lax.broadcasted_iota(jnp.int32, value.shape, 0)
        col_ids = col_start + lax.broadcasted_iota(jnp.int32, value.shape, 1)
        diag = row_ids == col_ids
        gap = 1.0 - value
        terms = jnp.where(diag, gap * gap, lam_off * value * value)
        grad = jnp.where(diag, -2.0 * gap, 2.0 * lam_off * value) / rows_total
        w2buf[span(row_index(OWN) * pieces + k, piece), col_block(OWN)] = grad.astype(BF16)
        return jnp.sum(terms, axis=0, keepdims=True)

    every = range(pieces)
    even, odd = every[::2], every[1::2]
    loss_row = jnp.zeros((1, cblk), F32)
    for k in every:
        loss_row = loss_row + grad_piece(k)
        go(g_copy(OWN, *((YN, k, XN) if k in odd else (XN, k, PAIR))))
    for k, j in zip(odd, even):
        go(g_copy(OWN, XN, k, PAIR))
        go(g_copy(OWN, YN, j, XN))

    def contribute(origin, k, count):
        part = span(row_index(origin) * (pieces // count) + k // count, count * piece)
        block = w2buf[part, col_block(origin)]
        first = dot(zh[span(1, half), col_block(origin)], block, TURN_RIGHT)
        where_a, where_b = (span(0, half), part), (span(1, half), col_block(origin))
        vbuf[where_a] = vbuf[where_a] + first if origin & XN else first
        second = dot(zh[span(0, half), part], block)
        vbuf[where_b] = second if origin in (OWN, XN) and not k else vbuf[where_b] + second

    for k in every:
        go(g_copy(OWN, PAIR, k, XP))
    loss_mine[0] = jnp.broadcast_to(jnp.sum(loss_row, axis=1, keepdims=True), loss_mine.shape[1:])
    send_loss(0)
    store_u2.wait()
    contribute(OWN, 0, pieces)
    g_arrived(PAIR, every)
    contribute(PAIR, 0, pieces)
    for k, j in zip(even, odd):
        g_arrived(XN, (k,))
        go(g_copy(XN, YN, k, YN))
        go(g_copy(XN, PAIR, k, YP))
        g_arrived(YN, (j,))
        go(g_copy(YN, XN, j, YN))
        go(g_copy(YN, PAIR, j, DG))
    for k, j in zip(odd, even):
        g_arrived(XN, (k,))
        go(g_copy(XN, PAIR, k, YP))
        g_arrived(YN, (j,))
        go(g_copy(YN, PAIR, j, DG))
    contribute(YN, 0, pieces)
    contribute(XN, 0, pieces)
    for origin in (YP, XP):
        g_arrived(origin, every)
        contribute(origin, 0, pieces)
    def dz_columns(v, late):
        first = me // 2 % 2 if v else me // 4
        return span(1 - first if late else first, cblk)

    def dz_sum_copy(v, late, mask):
        e, c = DG + v, dz_columns(v, late)
        k = DEVICES + v if late else e
        return remote(mine.at[e, :, c], slots.at[e, me, :, c], sum_send.at[k, mask], sum_recv.at[k, mask], mask)

    def dz_sums(late):
        for v in TWO:
            def body(t, carry, v=v):
                start = dz_columns(v, late).start + t * TILE
                c = pl.ds(pl.multiple_of(start, TILE), TILE)
                grad = vbuf[span(v, half), c]
                column_sums(mine, (DG + v,), 0, c, grad, grad * normed_tile(ubuf, v, c, vec3))
                return carry
            lax.fori_loop(0, cblk // TILE, body, 0)
            run([dz_sum_copy(v, late, mask) for mask in FAR_FIRST])

    dz_sums(False)
    for k in even:
        now = (k, k + 1)
        for j in now:
            g_arrived(DG, (j,))
            go(g_copy(DG, PAIR, j, DP))
        contribute(DG, k, len(now))
        g_arrived(DP, now)
        contribute(DP, k, len(now))

    dz_sums(True)
    finish_all(kept)
    loss_mine[0] = take_loss(0)
    small_out += run([pltpu.make_async_copy(loss_mine.at[0], loss, vec_sem.at[2])])
    for v in TWO:
        slots[DG + v, me] = mine[DG + v]
    for v in TWO:
        finish_all([dz_sum_copy(v, late, mask) for late in (False, True) for mask in FAR_FIRST])
        mine[DG + v] = functools.reduce(jnp.add, [slots[DG + v, k] for k in range(DEVICES)]) / rows_total

    def dz_copy(n):
        return pltpu.make_async_copy(xbuf.at[:, cols(n)], dz.at[:, cols(n)], dz_sem.at[n])

    def dz_tile(n):
        c = cols(n)
        for v in TWO:
            sums = mine[DG + v, :, c]
            grad = row(vec3, INV + v, c) * (
                vbuf[span(v, half), c] - (sums[:1] + normed_tile(ubuf, v, c, vec3) * sums[1:]))
            xbuf[span(v, half), c] = grad.astype(BF16)
        dz_copy(n).start()

    heads = (0, TILES // 2)
    for k, n in enumerate(heads):
        dz_tile(n)
        go(remote(xbuf.at[:, cols(n)], dz_pair.at[:, cols(k)], dz_send.at[k], dz_recv.at[k], PAIR))

    def dz_body(i, carry):
        for n in heads:
            dz_tile(n + i)
        return carry
    lax.fori_loop(1, TILES // 2, dz_body, 0)
    for copy in started:
        copy.wait_send()
    for copy in started[-len(heads):]:
        copy.wait_recv()
    finish_all(small_out)
    each_tile(lambda n, c: dz_copy(n).wait())


def forward(rows_total, lam, h_a, h_b, w1, w2, w3, *vectors, cid):
    half, depth = h_a.shape
    feats = w2.shape[0]
    full, pair, vec = (2 * half, feats), (2 * half, feats // 2), (VEC_ROWS, feats)
    small = (DEVICES, 128)
    outs = [(small, F32), (full, F32), (full, F32), (full, BF16), (full, BF16), (pair, BF16), (pair, BF16), (full, BF16), ((2 * half, 2 * TILE), BF16),
            (vec, F32), (vec, F32)]
    scratch = [((2 * half, depth), BF16), (full, F32), (full, F32), ((feats, feats), BF16), ((feats, feats), BF16),
               (full, BF16), (full, BF16), ((DEVICES, half, feats // 4), BF16), ((DEVICES, half, feats // 2), BF16),
               ((feats // 4, feats // 2), F32), ((DEVICES, 2, feats), F32), ((DEVICES, DEVICES, 2, feats), F32),
               (vec, F32), ((1,) + small, F32), ((1, DEVICES) + small, F32)]
    return pl.pallas_call(
        functools.partial(forward_kernel, rows_total),
        out_shape=[jax.ShapeDtypeStruct(*out) for out in outs],
        in_specs=[SCALARS] + [ANYWHERE] * (5 + len(vectors)),
        out_specs=[ANYWHERE] * len(outs),
        scratch_shapes=[pltpu.VMEM((len(vectors), 1, feats), F32)] + [pltpu.VMEM(vec, F32)] * 2
        + [DMA((len(vectors),))] + [pltpu.VMEM(*item) for item in scratch]
        + [DMA((WEIGHTS,))] * 2 + [DMA((2, len(ORDER)))] * 2 + [DMA((DEVICES + 2, DEVICES))] * 2 + [DMA((DEVICES,))] * 2
        + [DMA((DEVICES, 2))] * 2 + [DMA((DEVICES, 4))] * 2 + [DMA((1, DEVICES))] * 2 + [DMA((TILES,))] + [DMA((2,))] * 2,
        compiler_params=params(cid),
        name="forward",
    )(lam, h_a, h_b, w1, w2, w3, *vectors)


def emit_kernel(gw3, gw2, gw1, sums2, sums1, loss, loss_out, out3, out2, out1, gain1, shift1, gain2, shift2,
                buf, sums, vecs, loss_in, in_sem, out_sem, sum_sem, vec_sem, loss_sem):
    step = gw1.shape[0]
    pieces = [(src, dst, k) for src, dst in ((gw3, out3), (gw2, out2), (gw1, out1)) for k in range(src.shape[0] // step)]
    ins = run([pltpu.make_async_copy(src.at[span(k, step)], buf.at[i], in_sem.at[i])
               for i, (src, dst, k) in enumerate(pieces)])
    sums_in = run([pltpu.make_async_copy(src, sums.at[i], sum_sem.at[i]) for i, src in enumerate((sums1, sums2))])
    outs = [pltpu.make_async_copy(buf.at[i], dst.at[span(k, step)], out_sem.at[i])
            for i, (src, dst, k) in enumerate(pieces)]
    loss_copy = pltpu.make_async_copy(loss, loss_in, loss_sem)
    loss_copy.start()
    half = len(ins) // 2
    for before, after in zip(ins[:half], outs):
        before.wait()
        after.start()
    finish_all(sums_in)
    for i in TWO:
        both = sums[i, :2, :] + sums[i, 2:, :]
        vecs[2 * i] = both[1:]
        vecs[2 * i + 1] = both[:1]
    vecs_out = run([pltpu.make_async_copy(vecs.at[i], dst, vec_sem.at[i])
                    for i, dst in enumerate((gain1, shift1, gain2, shift2))])
    for before, after in zip(ins[half:], outs[half:]):
        before.wait()
        after.start()
    loss_copy.wait()
    loss_out[0, 0] = loss_in[0, 0]
    finish_all(outs + vecs_out)


def emit(gw3, gw2, gw1, sums2, sums1, loss):
    weights = (gw3, gw2, gw1)
    step, feats = gw1.shape
    count = sum(g.shape[0] for g in weights) // step
    vectors = [jax.ShapeDtypeStruct((1, feats), F32)] * 4
    return pl.pallas_call(
        emit_kernel,
        out_shape=[jax.ShapeDtypeStruct((1, 1), F32)] + [jax.ShapeDtypeStruct(g.shape, F32) for g in weights] + vectors,
        in_specs=[ANYWHERE] * (WEIGHTS + WEIGHTS),
        out_specs=[SCALARS] + [ANYWHERE] * (WEIGHTS + len(vectors)),
        scratch_shapes=[pltpu.VMEM((count, step, feats), F32), pltpu.VMEM((2,) + sums1.shape, F32),
                        pltpu.VMEM((len(vectors), 1, feats), F32), pltpu.SMEM(loss.shape, F32)]
        + [DMA((count,))] * 2 + [DMA((2,)), DMA((len(vectors),)), DMA],
        name="emit",
    )(*weights, sums2, sums1, loss)


def solution(mesh):
    shards = mesh.shape["data"]

    def local_step(h_a, h_b, w_one, w_two, w_three, gain_one, shift_one, gain_two, shift_two, lam_off):
        total_rows = h_a.shape[0] * shards
        loss, u1, u2, x1, x2, x1_pair, x2_pair, dz, dz_pair, vec1, vec2 = forward(
            total_rows, lam_off.reshape(1), h_a, h_b, w_one, w_two, w_three,
            *[v[None] for v in (gain_one, shift_one, gain_two, shift_two)], cid=0)
        grads = backward(total_rows, dz, dz_pair, x2, x2_pair, x1, x1_pair, h_a, h_b, w_three, w_two, u2, u1, vec2, vec1,
                         cid=1)
        loss, grad_w_three, grad_w_two, grad_w_one, *rest = emit(*grads, loss)
        return (loss.reshape(()), grad_w_one, grad_w_two, grad_w_three, *[v[0] for v in rest])

    row_spec = P("data", None)
    whole_mat = P(None, None)
    whole_vec = P(None)
    return jax.shard_map(
        local_step, mesh=mesh,
        in_specs=(row_spec, row_spec, whole_mat, whole_mat, whole_mat,
                  whole_vec, whole_vec, whole_vec, whole_vec, P()),
        out_specs=(P(), row_spec, row_spec, row_spec, whole_vec, whole_vec, whole_vec, whole_vec),
        check_vma=False)
```

```python
import functools

import jax
import jax.numpy as jnp
from jax import lax
from jax.experimental import pallas as pl
from jax.experimental.pallas import tpu as pltpu
from jax.sharding import PartitionSpec as P

NORM_EPS = 1e-5
MESH = pl.DeviceIdType.MESH
DEVICES = 8
OWN, PAIR, XN, XP, YN, YP, DG, DP = range(DEVICES)
FAR_FIRST = (DG, DP, XN, XP, YN, YP, PAIR)
ORDER = (OWN, XN, DG, YN)
TWO = range(2)
TILE = 256
TILES = 8
WIDE = 512
WEIGHTS = 3
GAIN, SHIFT, INV, MEAN, VEC_ROWS = 0, 1, 2, 4, 6
VMEM_BYTES = 67043328
TURN_LEFT = (((0,), (0,)), ((), ()))
TURN_RIGHT = (((1,), (1,)), ((), ()))
F32, BF16 = jnp.float32, jnp.bfloat16
DMA = pltpu.SemaphoreType.DMA


def dot(left, right, dims=None):
    if dims is None:
        return jnp.dot(left, right, preferred_element_type=F32)
    return lax.dot_general(left, right, dims, preferred_element_type=F32)


def span(index, size):
    return pl.ds(pl.multiple_of(index * size, size), size)


def cols(n):
    return span(n, TILE)


def row(ref, r, c):
    return ref[r:r + 1, c]


def remote(src, dst, send, recv, mask):
    return pltpu.make_async_remote_copy(src_ref=src, dst_ref=dst, send_sem=send, recv_sem=recv,
                                        device_id=(lax.axis_index("data") ^ mask,), device_id_type=MESH)


def greet():
    for mask in FAR_FIRST:
        pl.semaphore_signal(pltpu.get_barrier_semaphore(), inc=1, device_id=(lax.axis_index("data") ^ mask,),
                            device_id_type=MESH)


def all_entered():
    pl.semaphore_wait(pltpu.get_barrier_semaphore(), len(FAR_FIRST))


def column_sums(ref, lead, r, c, first, second):
    ref[lead + (slice(r, r + 1), c)] = jnp.sum(first, axis=0, keepdims=True)
    ref[lead + (slice(r + 1, r + 2), c)] = jnp.sum(second, axis=0, keepdims=True)


def exchange(mine, slots, send, recv):
    me = lax.axis_index("data")

    def copy(e, mask):
        return remote(mine.at[e], slots.at[e, me], send.at[e, mask], recv.at[e, mask], mask)

    def start(e):
        for mask in FAR_FIRST:
            copy(e, mask).start()
        slots[e, me] = mine[e]

    def take(e):
        for mask in FAR_FIRST:
            copy(e, mask).wait()
        return functools.reduce(jnp.add, [slots[e, k] for k in range(DEVICES)])
    return start, take


def exchange_halves(mine, mate, chips, whole, send, recv):
    me = lax.axis_index("data")
    width = mate.shape[-1]
    core, chip = me % 2, me // 2
    others = (DG, XN, YN)

    def pair_copy(e):
        return remote(mine.at[e, :, span(1 - core, width)], mate.at[e], send.at[e, OWN], recv.at[e, OWN], PAIR)

    def chip_copy(e, mask):
        return remote(chips.at[e, chip], chips.at[e, chip], send.at[e, mask], recv.at[e, mask], mask)

    def share(e):
        half = whole.at[e, :, span(core, width)]
        return remote(half, half, send.at[e, PAIR], recv.at[e, PAIR], PAIR)

    def start(e):
        pair_copy(e).start()

    def middle(e):
        pair_copy(e).wait()
        chips[e, chip] = mine[e, :, span(core, width)] + mate[e]
        for mask in others:
            chip_copy(e, mask).start()

    def take(e):
        for mask in others:
            chip_copy(e, mask).wait()
        whole[e, :, span(core, width)] = functools.reduce(jnp.add, [chips[e, k] for k in range(DEVICES // 2)])
        share(e).start()
        share(e).wait()
    return start, middle, take


def run(copies):
    for copy in copies:
        copy.start()
    return copies


def finish_all(copies):
    for copy in copies:
        copy.wait()


def backward_kernel(rows_total, dz, dz_pair, x2, x2_pair, x1, x1_pair, h_a, h_b, w3, w2, u2, u1, vec2_hbm, vec1_hbm,
                    gw3, gw2, gw1, sums2, sums1,
                    vec2, vec1, d, pd, xt, hv, hturn, ht, dpre, wbuf, nbuf, acc3, acc2, acc1, near3, near2, near1, far3, far2, far1,
                    mine, mate, chips, whole, vec_sem, load_sem, tile_sem, pair_send, pair_recv, hop_send, hop_recv, far_send, far_recv,
                    sum_send, sum_recv, h_send, h_recv, out_sem, w_sem, n_sem, free_sem):
    me = lax.axis_index("data")
    rows = d.shape[0]
    half = rows // 2
    greet()

    def small(src, dst, k):
        return pltpu.make_async_copy(src, dst, vec_sem.at[k])

    vectors_in = [small(vec2_hbm, vec2, 0), small(vec1_hbm, vec1, 1)]
    send_sums, pass_sums, take_sums = exchange_halves(mine, mate, chips, whole, sum_send, sum_recv)

    def pair_copy(n, src=d):
        return remote(src.at[:, cols(n)], pd.at[:, cols(n)], pair_send.at[n], pair_recv.at[n], PAIR)

    def both_colours(body):
        def step(i, carry):
            for colour in TWO:
                body(colour * (TILES // 2) + i, colour)
            return carry
        lax.fori_loop(0, TILES // 2, step, 0)

    class Product:
        def __init__(self, w, lhs, acc, near, far, out):
            self.w, self.lhs, self.acc, self.near, self.far, self.out = w, lhs, acc, near, far, out
            self.blk = out.shape[0]

        def block(self, j, count=1):
            return pl.ds(j * self.blk, count * self.blk)

        def first_hop(self, n, colour):
            return remote(self.acc.at[n, self.block(1 + colour, 2)], self.near.at[n],
                          hop_send.at[self.w, n], hop_recv.at[self.w, n], YN if colour else XN)

        def second_hop(self, n, colour):
            return remote(self.acc.at[n, self.block(1 if colour else 3)], self.far.at[n],
                          far_send.at[self.w, n], far_recv.at[self.w, n], XN if colour else YN)

        def out_copy(self, n):
            return pltpu.make_async_copy(self.acc.at[n, self.block(0)], self.out.at[:, cols(n)], out_sem.at[self.w, n])

        def fill(self, n, part):
            self.acc[n, part] = self.lhs(0, part, d[:, cols(n)]) + self.lhs(1, part, pd[:, cols(n)])

        def compute(self, parts, arrive, send):
            def body(n, colour):
                if arrive:
                    arrive(n)
                for j, count in parts[colour]:
                    self.fill(n, self.block(j, count))
                if send:
                    self.first_hop(n, colour).start()
            both_colours(body)

        def relay(self):
            def body(n, colour):
                onward, own = self.block(1 if colour else 3), self.block(0)
                self.first_hop(n, colour).wait_recv()
                self.acc[n, onward] = self.acc[n, onward] + self.near[n, self.block(1 - colour)]
                self.second_hop(n, colour).start()
                self.acc[n, own] = self.acc[n, own] + self.near[n, self.block(colour)]
            both_colours(body)

        def finish(self):
            def body(n, colour):
                own = self.block(0)
                self.second_hop(n, colour).wait_recv()
                self.acc[n, own] = self.acc[n, own] + self.far[n]
                self.out_copy(n).start()
            both_colours(body)

        def drain(self):
            def body(n, colour):
                self.first_hop(n, colour).wait_send()
                self.second_hop(n, colour).wait_send()
                self.out_copy(n).wait()
            both_colours(body)

    def w_tile(src, i):
        return pltpu.make_async_copy(src.at[cols(i)], wbuf.at[i % 2], w_sem.at[i % 2])

    def n_tile(src, i):
        return pltpu.make_async_copy(src.at[:, cols(i)], nbuf.at[i % 2], n_sem.at[i % 2])

    def tiles(streams, body):
        run([s(0) for s in streams])

        def step(i, carry):
            @pl.when(i < TILES - 1)
            def _():
                run([s(i + 1) for s in streams])
            finish_all([s(i) for s in streams])
            body(i, cols(i))
            return carry
        lax.fori_loop(0, TILES, step, 0)

    def normed_tile(i, c, v, vec):
        return (nbuf[i % 2, span(v, half), :] - row(vec, MEAN + v, c)) * row(vec, INV + v, c)

    def back_product(w_src, n_src, vec, which):
        def body(i, c):
            for v in TWO:
                grad = dot(d[span(v, half), :], wbuf[i % 2], TURN_RIGHT)
                normed = normed_tile(i, c, v, vec)
                grad = jnp.where(row(vec, GAIN, c) * normed + row(vec, SHIFT, c) > 0, grad, 0.0)
                dpre[span(v, half), c] = grad
                column_sums(mine, (which,), 2 * v, c, grad, grad * normed)
        tiles([functools.partial(w_tile, w_src), functools.partial(n_tile, n_src)], body)

    def norm_grad(n_src, vec, sums):
        def body(i, c):
            for v in TWO:
                part = span(v, half)
                mean, slope = row(sums, 2 * v, c) / rows_total, row(sums, 2 * v + 1, c) / rows_total
                grad = row(vec, GAIN, c) * row(vec, INV + v, c) * (
                    dpre[part, c] - (mean + normed_tile(i, c, v, vec) * slope))
                d[part, c] = grad.astype(BF16)
            pair_copy(i).start()
        tiles([functools.partial(n_tile, n_src)], body)

    def load(src, dst, k):
        return pltpu.make_async_copy(src, dst, load_sem.at[k])

    def dz_tile(n):
        return pltpu.make_async_copy(dz.at[:, cols(n)], d.at[:, cols(n)], tile_sem.at[n])

    heads = (0, TILES // 2)
    passed = [pair_copy(n, dz) for i in range(1, TILES // 2) for n in (i, TILES // 2 + i)]

    def dz_arrived(n):
        dz_tile(n).wait()
        pair_copy(n).wait_recv()

    blk3, blk1 = gw3.shape[0], gw1.shape[0]

    def operand(src, pair):
        return [load(pair, xt.at[span(1, rows)], len(ORDER))] + [
            load(src.at[:, span(me ^ mask, blk3)], xt.at[span(0, rows), pl.ds(j * blk3, blk3)], j)
            for j, mask in enumerate(ORDER)]

    def lhs_x(k, part, right):
        return dot(xt[span(k, rows), part], right, TURN_LEFT)

    def lhs_h(k, part, right):
        return dot(ht[part, span(k, rows)], right)

    prod3 = Product(0, lhs_x, acc3, near3, far3, gw3)
    prod2 = Product(1, lhs_x, acc2, near2, far2, gw2)
    prod1 = Product(2, lhs_h, acc1, near1, far1, gw1)
    first = run(operand(x2, x2_pair))
    run([pltpu.make_async_copy(dz_pair.at[:, cols(k)], pd.at[:, cols(n)], pair_recv.at[n]) for k, n in enumerate(heads)])
    both_colours(lambda n, colour: dz_tile(n).start())
    run(vectors_in)
    all_entered()
    run(passed)
    finish_all(first + vectors_in)
    everything = ([(0, len(ORDER))],) * 2
    prod3.compute(([(1, 2)], [(2, 2)]), dz_arrived, True)
    back_product(w3, u2, vec2, 0)
    send_sums(0)
    prod3.compute(([(0, 1), (3, 1)], [(0, 2)]), None, False)
    for copy in passed:
        copy.wait_send()
    pass_sums(0)
    second = run(operand(x1, x1_pair))
    views = list(enumerate((h_a, h_b)))
    own_h = run([load(src, hv.at[span(v, half)], len(ORDER) + 1 + v) for v, src in views])
    pair_h = run([remote(src, hv.at[span(2 + v, half)], h_send.at[v], h_recv.at[v], PAIR) for v, src in views])
    prod3.relay()
    take_sums(0)
    sums_out = run([small(whole.at[0], sums2, 2)])
    norm_grad(u2, vec2, whole.at[0])
    finish_all(second)
    prod2.compute(everything, lambda n: pair_copy(n).wait(), True)
    pl.semaphore_signal(free_sem, inc=1, device_id=(me ^ PAIR,), device_id_type=MESH)
    back_product(w2, u1, vec1, 1)
    send_sums(1)
    finish_all(own_h + pair_h)
    for k in range(2 * len(TWO)):
        hturn[:, span(k, half)] = hv[span(k, half), :].T
    for j, mask in enumerate(ORDER):
        ht[span(j, blk1), :] = hturn[span(me ^ mask, blk1), :]
    pass_sums(1)
    prod3.finish()
    prod2.relay()
    take_sums(1)
    sums_out += run([small(whole.at[1], sums1, 3)])
    pl.semaphore_wait(free_sem, 1)
    norm_grad(u1, vec1, whole.at[1])
    prod1.compute(everything, lambda n: pair_copy(n).wait(), True)
    prod1.relay()
    prod2.finish()
    prod1.finish()
    for product in (prod3, prod2, prod1):
        product.drain()
    finish_all(sums_out)


ANYWHERE = pl.BlockSpec(memory_space=pl.ANY)
SCALARS = pl.BlockSpec(memory_space=pltpu.SMEM)


def params(cid):
    return pltpu.CompilerParams(collective_id=cid, has_side_effects=True, vmem_limit_bytes=VMEM_BYTES)


def backward(rows_total, dz, *rest, cid):
    h_a = rest[5]
    rows, feats = dz.shape
    blk3, blk1 = feats // DEVICES, h_a.shape[1] // DEVICES
    groups = len(ORDER)
    blocks = (blk3, blk3, blk1)

    def per_weight(parts):
        return [pltpu.VMEM((TILES, parts * b, TILE), F32) for b in blocks]

    sums = jax.ShapeDtypeStruct((2 * len(TWO), feats), F32)
    half_sums = (2 * len(TWO), feats // 2)
    return pl.pallas_call(
        functools.partial(backward_kernel, rows_total),
        out_shape=[jax.ShapeDtypeStruct((b, feats), F32) for b in blocks] + [sums, sums],
        in_specs=[ANYWHERE] * (len(rest) + 1),
        out_specs=[ANYWHERE] * (WEIGHTS + 2),
        scratch_shapes=[pltpu.VMEM((VEC_ROWS, feats), F32)] * 2 + [pltpu.VMEM((rows, feats), BF16), pltpu.VMEM((rows, feats), BF16),
                        pltpu.VMEM((2 * rows, groups * blk3), BF16), pltpu.VMEM((2 * rows, h_a.shape[1]), BF16),
                        pltpu.VMEM((h_a.shape[1], 2 * rows), BF16), pltpu.VMEM((groups * blk1, 2 * rows), BF16),
                        pltpu.VMEM((rows, feats), F32),
                        pltpu.VMEM((2, TILE, feats), BF16), pltpu.VMEM((2, rows, TILE), F32)]
        + per_weight(groups) + per_weight(2) + per_weight(1)
        + [pltpu.VMEM(shape, F32) for shape in ((2,) + sums.shape, (2,) + half_sums, (2, DEVICES // 2) + half_sums,
                                                (2,) + sums.shape)]
        + [DMA((len(ORDER),)), DMA((DEVICES,)), DMA((TILES,))]
        + [DMA((TILES,))] * 2 + [DMA((WEIGHTS, TILES))] * 4 + [DMA((2, DEVICES))] * 2 + [DMA((2,))] * 2
        + [DMA((WEIGHTS, TILES))] + [DMA((2,))] * 2 + [pltpu.SemaphoreType.REGULAR],
        compiler_params=params(cid),
        name="backward",
    )(dz, *rest)


def forward_kernel(rows_total, lam, h_a, h_b, w1, w2, w3, gain1, shift1, gain2, shift2,
                   loss, u1, u2, x1, x2, x1_pair, x2_pair, dz, dz_pair, vec1_out, vec2_out,
                   affine, vec1, vec2, vec_sem, hv, ubuf, vbuf, w2buf, w3buf, xbuf, zh, za, zb, corr, mine, slots, vec3, loss_mine, loss_slots,
                   load_sem, store_sem, pair_send, pair_recv, sum_send, sum_recv, za_send, za_recv, zb_send, zb_recv,
                   g_send, g_recv, loss_send, loss_recv, dz_sem, dz_send, dz_recv):
    me = lax.axis_index("data")
    half = hv.shape[0] // 2
    feats = w2buf.shape[0]
    rblk, cblk = za.shape[2], zb.shape[2]
    greet()

    def load(src, dst, k):
        return pltpu.make_async_copy(src, dst, load_sem.at[k])

    w1_view = w3buf.at[pl.ds(0, w1.shape[0])]
    loads = run([load(h_a, hv.at[span(0, half)], 0), load(h_b, hv.at[span(1, half)], 1), load(w1, w1_view, 2)])
    affine_in = run([pltpu.make_async_copy(src, affine.at[k], vec_sem.at[k])
                     for k, src in enumerate((gain1, shift1, gain2, shift2))])
    all_entered()
    send_sums, take_sums = exchange(mine, slots, sum_send, sum_recv)
    send_loss, take_loss = exchange(loss_mine, loss_slots, loss_send, loss_recv)

    def each_tile(body):
        def step(n, carry):
            body(n, cols(n))
            return carry
        lax.fori_loop(0, TILES, step, 0)

    def take_vectors(e, v, vec):
        total = take_sums(e) / rows_total
        mean = total[:1]
        vec[pl.ds(MEAN + v, 1), :] = mean
        vec[pl.ds(INV + v, 1), :] = lax.rsqrt(total[1:] - mean * mean + NORM_EPS)

    def layer(e, v, left, weight, out, beside=None, tiles=None):
        part = span(v, half)

        def body(n, carry):
            c = span(n, WIDE)
            value = dot(left[part, :], weight[:, c])
            out[part, c] = value
            column_sums(mine, (e,), 0, c, value, value * value)
            if beside:
                beside(c)
            return carry
        lax.fori_loop(*(tiles or (0, feats // WIDE)), body, 0)
        if not tiles or tiles[1] == feats // WIDE:
            send_sums(e)

    def normed_tile(values, v, c, vec):
        return (values[span(v, half), c] - row(vec, MEAN + v, c)) * row(vec, INV + v, c)

    def activate_tile(v, values, vec, c):
        pre = row(vec, GAIN, c) * normed_tile(values, v, c, vec) + row(vec, SHIFT, c)
        xbuf[span(v, half), c] = jnp.maximum(pre, 0.0).astype(BF16)

    def activate(v, values, vec):
        each_tile(lambda n, c: activate_tile(v, values, vec, c))

    def store(src, dst, k):
        return pltpu.make_async_copy(src, dst, store_sem.at[k])

    def keep_rows(dst, pair, index):
        blk = feats // DEVICES
        return run([store(xbuf, dst, 2)] + [
            remote(xbuf.at[:, span(me ^ mask ^ PAIR, blk)], pair.at[:, pl.ds(j * blk, blk)],
                   pair_send.at[index, j], pair_recv.at[index, j], PAIR) for j, mask in enumerate(ORDER)])

    finish_all(loads + affine_in)
    for k, vec in enumerate((vec1, vec2)):
        vec[pl.ds(GAIN, 1), :] = affine[2 * k]
        vec[pl.ds(SHIFT, 1), :] = affine[2 * k + 1]
    load_w2 = load(w2, w2buf, 0)
    load_w2.start()
    for v in TWO:
        layer(v, v, hv, w1_view, ubuf)
    load_w3 = load(w3, w3buf, 2)
    store_u1 = store(ubuf, u1, 0)
    run([load_w3, store_u1])
    for v in TWO:
        take_vectors(v, v, vec1)
    activate(0, ubuf, vec1)
    load_w2.wait()
    layer(2, 0, xbuf, w2buf, vbuf, functools.partial(activate_tile, 1, ubuf, vec1))
    kept = keep_rows(x1, x1_pair, 0)
    layer(3, 1, xbuf, w2buf, vbuf)
    store_u2 = store(vbuf, u2, 1)
    store_u2.start()
    finish_all([store_u1, load_w3] + kept)
    take_vectors(2, 0, vec2)
    activate(0, vbuf, vec2)
    count = feats // WIDE
    middle = count // 2
    layer(4, 0, xbuf, w3buf, ubuf, None, (0, middle))
    take_vectors(3, 1, vec2)

    def activate_two(c):
        for k in TWO:
            activate_tile(1, vbuf, vec2, pl.ds(pl.multiple_of((c.start - middle * WIDE) * 2 + k * WIDE, WIDE), WIDE))
    layer(4, 0, xbuf, w3buf, ubuf, activate_two, (middle, count))
    kept = keep_rows(x2, x2_pair, 1)
    layer(5, 1, xbuf, w3buf, ubuf, None, (0, count - 1))
    small_out = run([pltpu.make_async_copy(vec, out, vec_sem.at[k])
                     for k, (vec, out) in enumerate(((vec1, vec1_out), (vec2, vec2_out)))])

    def embed_tile(v, c):
        zh[span(v, half), c] = normed_tile(ubuf, v, c, vec3).astype(BF16)

    def row_index(mask):
        dev = me ^ mask
        return dev // 4 * 2 + dev % 2

    def row_block(mask):
        return span(row_index(mask), rblk)

    def col_block(mask):
        return span((me ^ mask) // 2 % 2, cblk)

    quarter = half // 2
    started = []

    def go(copy):
        copy.start()
        started.append(copy)

    def za_direct(mask):
        return remote(zh.at[span(0, half), row_block(mask)], za.at[me], za_send.at[mask], za_recv.at[mask], mask)

    def za_relay(origin):
        slot = za.at[me ^ origin]
        return remote(slot, slot, za_send.at[origin ^ XN], za_recv.at[origin ^ XN], XN)

    def zb_slot(origin, k):
        return zb.at[me ^ origin, span(k, quarter)]

    def zb_direct(mask, k):
        return remote(zh.at[span(2 + k, quarter), col_block(mask)], zb_slot(OWN, k),
                      zb_send.at[mask, k], zb_recv.at[mask, k], mask)

    def zb_relay(origin, mask, k, send):
        return remote(zb_slot(origin, k), zb_slot(origin, k), zb_send.at[send, k], zb_recv.at[origin ^ mask, k], mask)

    def za_arrived(origin):
        slot = za.at[me ^ origin]
        remote(slot, slot, za_send.at[OWN], za_recv.at[origin], PAIR).wait_recv()

    def zb_arrived(origin, ks=TWO):
        for k in ks:
            zb_relay(origin, OWN, k, OWN).wait_recv()

    def accumulate(origin):
        corr[...] = corr[...] + dot(za[me ^ origin], zb[me ^ origin], TURN_LEFT)

    take_vectors(4, 0, vec3)
    layer(5, 1, xbuf, w3buf, ubuf, lambda c: [embed_tile(0, span(n, WIDE)) for n in range(count)], (count - 1, count))
    for mask in (YN, XN, YP, XP, PAIR):
        go(za_direct(mask))
    take_vectors(5, 1, vec3)
    each_tile(lambda n, c: embed_tile(1, c))
    for k in TWO:
        for mask in (XN, YN, PAIR):
            go(zb_direct(mask, k))
    corr[...] = dot(zh[span(0, half), row_block(OWN)], zh[span(1, half), col_block(OWN)], TURN_LEFT)
    za_arrived(PAIR)
    zb_arrived(PAIR)
    accumulate(PAIR)
    for origin in (YN, YP):
        za_arrived(origin)
        go(za_relay(origin))
    for k in TWO:
        zb_arrived(XN, (k,))
        go(zb_relay(XN, YN, k, XP))
        go(zb_relay(XN, PAIR, k, YP))
        zb_arrived(YN, (k,))
        go(zb_relay(YN, PAIR, k, DG))
    za_arrived(XN)
    accumulate(XN)
    accumulate(YN)
    za_arrived(XP)
    for origin in (XP, YP):
        zb_arrived(origin)
        accumulate(origin)
    for k in TWO:
        zb_arrived(DG, (k,))
        go(zb_relay(DG, PAIR, k, DP))
    za_arrived(DG)
    accumulate(DG)
    za_arrived(DP)
    zb_arrived(DP)
    accumulate(DP)

    lam_off = lam[0]
    row_start, col_start = row_index(OWN) * rblk, me // 2 % 2 * cblk

    pieces = g_send.shape[1]
    piece = rblk // pieces

    def g_slot(origin, k):
        return w2buf.at[span(row_index(origin) * pieces + k, piece), col_block(origin)]

    def g_copy(origin, mask, k, send):
        return remote(g_slot(origin, k), g_slot(origin, k), g_send.at[send, k], g_recv.at[origin ^ mask, k], mask)

    def g_arrived(origin, ks):
        for k in ks:
            g_copy(origin, OWN, k, OWN).wait_recv()

    def grad_piece(k):
        value = corr[span(k, piece), :] / rows_total
        row_ids = row_start + k * piece + lax.broadcasted_iota(jnp.int32, value.shape, 0)
        col_ids = col_start + lax.broadcasted_iota(jnp.int32, value.shape, 1)
        diag = row_ids == col_ids
        gap = 1.0 - value
        terms = jnp.where(diag, gap * gap, lam_off * value * value)
        grad = jnp.where(diag, -2.0 * gap, 2.0 * lam_off * value) / rows_total
        w2buf[span(row_index(OWN) * pieces + k, piece), col_block(OWN)] = grad.astype(BF16)
        return jnp.sum(terms, axis=0, keepdims=True)

    every = range(pieces)
    even, odd = every[::2], every[1::2]
    loss_row = jnp.zeros((1, cblk), F32)
    for k in every:
        loss_row = loss_row + grad_piece(k)
        go(g_copy(OWN, *((YN, k, XN) if k in odd else (XN, k, PAIR))))
    for k, j in zip(odd, even):
        go(g_copy(OWN, XN, k, PAIR))
        go(g_copy(OWN, YN, j, XN))

    def contribute(origin, k, count):
        part = span(row_index(origin) * (pieces // count) + k // count, count * piece)
        block = w2buf[part, col_block(origin)]
        first = dot(zh[span(1, half), col_block(origin)], block, TURN_RIGHT)
        where_a, where_b = (span(0, half), part), (span(1, half), col_block(origin))
        vbuf[where_a] = vbuf[where_a] + first if origin & XN else first
        second = dot(zh[span(0, half), part], block)
        vbuf[where_b] = second if origin in (OWN, XN) and not k else vbuf[where_b] + second

    for k in every:
        go(g_copy(OWN, PAIR, k, XP))
    loss_mine[0] = jnp.broadcast_to(jnp.sum(loss_row, axis=1, keepdims=True), loss_mine.shape[1:])
    send_loss(0)
    store_u2.wait()
    contribute(OWN, 0, pieces)
    g_arrived(PAIR, every)
    contribute(PAIR, 0, pieces)
    for k, j in zip(even, odd):
        g_arrived(XN, (k,))
        go(g_copy(XN, YN, k, YN))
        go(g_copy(XN, PAIR, k, YP))
        g_arrived(YN, (j,))
        go(g_copy(YN, XN, j, YN))
        go(g_copy(YN, PAIR, j, DG))
    for k, j in zip(odd, even):
        g_arrived(XN, (k,))
        go(g_copy(XN, PAIR, k, YP))
        g_arrived(YN, (j,))
        go(g_copy(YN, PAIR, j, DG))
    contribute(YN, 0, pieces)
    contribute(XN, 0, pieces)
    for origin in (YP, XP):
        g_arrived(origin, every)
        contribute(origin, 0, pieces)
    def dz_columns(v, late):
        first = me // 2 % 2 if v else me // 4
        return span(1 - first if late else first, cblk)

    def dz_sum_copy(v, late, mask):
        e, c = DG + v, dz_columns(v, late)
        k = DEVICES + v if late else e
        return remote(mine.at[e, :, c], slots.at[e, me, :, c], sum_send.at[k, mask], sum_recv.at[k, mask], mask)

    def dz_sums(late):
        for v in TWO:
            def body(t, carry, v=v):
                start = dz_columns(v, late).start + t * TILE
                c = pl.ds(pl.multiple_of(start, TILE), TILE)
                grad = vbuf[span(v, half), c]
                column_sums(mine, (DG + v,), 0, c, grad, grad * normed_tile(ubuf, v, c, vec3))
                return carry
            lax.fori_loop(0, cblk // TILE, body, 0)
            run([dz_sum_copy(v, late, mask) for mask in FAR_FIRST])

    dz_sums(False)
    for k in even:
        now = (k, k + 1)
        for j in now:
            g_arrived(DG, (j,))
            go(g_copy(DG, PAIR, j, DP))
        contribute(DG, k, len(now))
        g_arrived(DP, now)
        contribute(DP, k, len(now))

    dz_sums(True)
    finish_all(kept)
    loss_mine[0] = take_loss(0)
    small_out += run([pltpu.make_async_copy(loss_mine.at[0], loss, vec_sem.at[2])])
    for v in TWO:
        slots[DG + v, me] = mine[DG + v]
    for v in TWO:
        finish_all([dz_sum_copy(v, late, mask) for late in (False, True) for mask in FAR_FIRST])
        mine[DG + v] = functools.reduce(jnp.add, [slots[DG + v, k] for k in range(DEVICES)]) / rows_total

    def dz_copy(n):
        return pltpu.make_async_copy(xbuf.at[:, cols(n)], dz.at[:, cols(n)], dz_sem.at[n])

    def dz_tile(n):
        c = cols(n)
        for v in TWO:
            sums = mine[DG + v, :, c]
            grad = row(vec3, INV + v, c) * (
                vbuf[span(v, half), c] - (sums[:1] + normed_tile(ubuf, v, c, vec3) * sums[1:]))
            xbuf[span(v, half), c] = grad.astype(BF16)
        dz_copy(n).start()

    heads = (0, TILES // 2)
    for k, n in enumerate(heads):
        dz_tile(n)
        go(remote(xbuf.at[:, cols(n)], dz_pair.at[:, cols(k)], dz_send.at[k], dz_recv.at[k], PAIR))

    def dz_body(i, carry):
        for n in heads:
            dz_tile(n + i)
        return carry
    lax.fori_loop(1, TILES // 2, dz_body, 0)
    for copy in started:
        copy.wait_send()
    for copy in started[-len(heads):]:
        copy.wait_recv()
    finish_all(small_out)
    each_tile(lambda n, c: dz_copy(n).wait())


def forward(rows_total, lam, h_a, h_b, w1, w2, w3, *vectors, cid):
    half, depth = h_a.shape
    feats = w2.shape[0]
    full, pair, vec = (2 * half, feats), (2 * half, feats // 2), (VEC_ROWS, feats)
    small = (DEVICES, 128)
    outs = [(small, F32), (full, F32), (full, F32), (full, BF16), (full, BF16), (pair, BF16), (pair, BF16), (full, BF16), ((2 * half, 2 * TILE), BF16),
            (vec, F32), (vec, F32)]
    scratch = [((2 * half, depth), BF16), (full, F32), (full, F32), ((feats, feats), BF16), ((feats, feats), BF16),
               (full, BF16), (full, BF16), ((DEVICES, half, feats // 4), BF16), ((DEVICES, half, feats // 2), BF16),
               ((feats // 4, feats // 2), F32), ((DEVICES, 2, feats), F32), ((DEVICES, DEVICES, 2, feats), F32),
               (vec, F32), ((1,) + small, F32), ((1, DEVICES) + small, F32)]
    return pl.pallas_call(
        functools.partial(forward_kernel, rows_total),
        out_shape=[jax.ShapeDtypeStruct(*out) for out in outs],
        in_specs=[SCALARS] + [ANYWHERE] * (5 + len(vectors)),
        out_specs=[ANYWHERE] * len(outs),
        scratch_shapes=[pltpu.VMEM((len(vectors), 1, feats), F32)] + [pltpu.VMEM(vec, F32)] * 2
        + [DMA((len(vectors),))] + [pltpu.VMEM(*item) for item in scratch]
        + [DMA((WEIGHTS,))] * 2 + [DMA((2, len(ORDER)))] * 2 + [DMA((DEVICES + 2, DEVICES))] * 2 + [DMA((DEVICES,))] * 2
        + [DMA((DEVICES, 2))] * 2 + [DMA((DEVICES, 4))] * 2 + [DMA((1, DEVICES))] * 2 + [DMA((TILES,))] + [DMA((2,))] * 2,
        compiler_params=params(cid),
        name="forward",
    )(lam, h_a, h_b, w1, w2, w3, *vectors)


def emit_kernel(gw3, gw2, gw1, sums2, sums1, loss, loss_out, out3, out2, out1, gain1, shift1, gain2, shift2,
                buf, sums, vecs, loss_in, in_sem, out_sem, sum_sem, vec_sem, loss_sem):
    step = gw1.shape[0]
    pieces = [(src, dst, k) for src, dst in ((gw3, out3), (gw2, out2), (gw1, out1)) for k in range(src.shape[0] // step)]
    ins = run([pltpu.make_async_copy(src.at[span(k, step)], buf.at[i], in_sem.at[i])
               for i, (src, dst, k) in enumerate(pieces)])
    sums_in = run([pltpu.make_async_copy(src, sums.at[i], sum_sem.at[i]) for i, src in enumerate((sums1, sums2))])
    outs = [pltpu.make_async_copy(buf.at[i], dst.at[span(k, step)], out_sem.at[i])
            for i, (src, dst, k) in enumerate(pieces)]
    loss_copy = pltpu.make_async_copy(loss, loss_in, loss_sem)
    loss_copy.start()
    half = len(ins) // 2
    for before, after in zip(ins[:half], outs):
        before.wait()
        after.start()
    finish_all(sums_in)
    for i in TWO:
        both = sums[i, :2, :] + sums[i, 2:, :]
        vecs[2 * i] = both[1:]
        vecs[2 * i + 1] = both[:1]
    vecs_out = run([pltpu.make_async_copy(vecs.at[i], dst, vec_sem.at[i])
                    for i, dst in enumerate((gain1, shift1, gain2, shift2))])
    for before, after in zip(ins[half:], outs[half:]):
        before.wait()
        after.start()
    loss_copy.wait()
    loss_out[0, 0] = loss_in[0, 0]
    finish_all(outs + vecs_out)


def emit(gw3, gw2, gw1, sums2, sums1, loss):
    weights = (gw3, gw2, gw1)
    step, feats = gw1.shape
    count = sum(g.shape[0] for g in weights) // step
    vectors = [jax.ShapeDtypeStruct((1, feats), F32)] * 4
    return pl.pallas_call(
        emit_kernel,
        out_shape=[jax.ShapeDtypeStruct((1, 1), F32)] + [jax.ShapeDtypeStruct(g.shape, F32) for g in weights] + vectors,
        in_specs=[ANYWHERE] * (WEIGHTS + WEIGHTS),
        out_specs=[SCALARS] + [ANYWHERE] * (WEIGHTS + len(vectors)),
        scratch_shapes=[pltpu.VMEM((count, step, feats), F32), pltpu.VMEM((2,) + sums1.shape, F32),
                        pltpu.VMEM((len(vectors), 1, feats), F32), pltpu.SMEM(loss.shape, F32)]
        + [DMA((count,))] * 2 + [DMA((2,)), DMA((len(vectors),)), DMA],
        name="emit",
    )(*weights, sums2, sums1, loss)


def solution(mesh):
    shards = mesh.shape["data"]

    def local_step(h_a, h_b, w_one, w_two, w_three, gain_one, shift_one, gain_two, shift_two, lam_off):
        total_rows = h_a.shape[0] * shards
        loss, u1, u2, x1, x2, x1_pair, x2_pair, dz, dz_pair, vec1, vec2 = forward(
            total_rows, lam_off.reshape(1), h_a, h_b, w_one, w_two, w_three,
            *[v[None] for v in (gain_one, shift_one, gain_two, shift_two)], cid=0)
        grads = backward(total_rows, dz, dz_pair, x2, x2_pair, x1, x1_pair, h_a, h_b, w_three, w_two, u2, u1, vec2, vec1,
                         cid=1)
        loss, grad_w_three, grad_w_two, grad_w_one, *rest = emit(*grads, loss)
        return (loss.reshape(()), grad_w_one, grad_w_two, grad_w_three, *[v[0] for v in rest])

    row_spec = P("data", None)
    whole_mat = P(None, None)
    whole_vec = P(None)
    return jax.shard_map(
        local_step, mesh=mesh,
        in_specs=(row_spec, row_spec, whole_mat, whole_mat, whole_mat,
                  whole_vec, whole_vec, whole_vec, whole_vec, P()),
        out_specs=(P(), row_spec, row_spec, row_spec, whole_vec, whole_vec, whole_vec, whole_vec),
        check_vma=False)
```
